8 devices in a mesh: rep: 1 (over z), row: 2 (over y), col: 2 (over x), core: 2 (over core).
Axes of the slice: x: 2, y: 2, z: 1, core: 2. Of those that a mesh axis runs over, the one named last changes fastest.
Arguments:
- x: bfloat16 [2, 768, 384], P(None, ('rep', 'row', 'col', 'core'))
- route_idx: int32 [2, 768, 4], P(None, ('rep', 'row', 'col', 'core'))
- gates: float32 [2, 768, 4], P(None, ('rep', 'row', 'col', 'core'))
- w_gate: bfloat16 [32, 384, 384], P(('rep', 'row', 'col', 'core'))
- w_up: bfloat16 [32, 384, 384], P(('rep', 'row', 'col', 'core'))
- w_down: bfloat16 [32, 384, 384], P(('rep', 'row', 'col', 'core'))
- grad_y: bfloat16 [2, 768, 384], P(None, ('rep', 'row', 'col', 'core'))
Outputs:
- output 1: bfloat16 [2, 768, 384], P(None, ('rep', 'row', 'col', 'core'))
- output 2: bfloat16 [2, 768, 384], P(None, ('rep', 'row', 'col', 'core'))
- output 3: float32 [2, 768, 4], P(None, ('rep', 'row', 'col', 'core'))
- output 4: float32 [32, 384, 384], P(('rep', 'row', 'col', 'core'))
- output 5: float32 [32, 384, 384], P(('rep', 'row', 'col', 'core'))
- output 6: float32 [32, 384, 384], P(('rep', 'row', 'col', 'core'))
All inputs are finite; a program needn't handle non-finite values.
Results may differ from the reference program's by a relative error of at most 0.00857745.
Values are sent between devices in bfloat16 or wider.
A program may use at most 1 GiB of HBM per device.

```python
import jax
import jax.numpy as jnp
from jax import lax

D_MODEL = 384
D_FF = 384
EXPERTS = 32
TOP_K = 4
TOK_DEV = 96
N_ROWS = 2
N_COLS = 2
N_CORES = 2

GROUP_SIZE = N_ROWS * N_COLS * N_CORES
TOKENS = GROUP_SIZE * TOK_DEV
CAPACITY = TOK_DEV // 2
CHIP_EXP = EXPERTS // (N_ROWS * N_COLS)
N_HOT = min(CHIP_EXP, TOP_K // 2)
N_COLD = EXPERTS - N_HOT
LOAD_MAX = GROUP_SIZE * CAPACITY


def draw_hot_chips(base_key):
    key_list = jax.random.split(base_key, 4)
    row_first = jax.random.randint(key_list[0], (), 0, N_ROWS)
    col_first = jax.random.randint(key_list[1], (), 0, N_COLS)
    row_second = (row_first + jax.random.randint(key_list[2], (), 1, N_ROWS)) % N_ROWS
    col_second = (col_first + jax.random.randint(key_list[3], (), 1, N_COLS)) % N_COLS
    return row_first * N_COLS + col_first, row_second * N_COLS + col_second


def draw_routing(base_key, hot_chip):
    key_list = jax.random.split(base_key, 4)
    slot_ids = jnp.arange(TOP_K)
    hot_ids = hot_chip * CHIP_EXP + jnp.arange(N_HOT) * (CHIP_EXP // N_HOT)
    sel_keys = jax.random.split(key_list[0], GROUP_SIZE * N_HOT)
    perm_rank = jax.vmap(lambda sub_key: jax.random.permutation(sub_key, TOK_DEV))(sel_keys)
    hot_mask = (perm_rank < CAPACITY).astype(jnp.int32).reshape(GROUP_SIZE, N_HOT, TOK_DEV)
    hot_mask = jnp.transpose(hot_mask, (0, 2, 1))
    hot_count = jnp.sum(hot_mask, axis=2)
    hot_rank = jnp.cumsum(hot_mask, axis=2) - hot_mask
    hot_pick = hot_mask[:, :, :, None] * (hot_rank[:, :, :, None] == slot_ids).astype(jnp.int32)
    hot_route = jnp.sum(hot_pick * hot_ids[None, None, :, None], axis=2)
    is_hot = jnp.zeros((EXPERTS,), jnp.int32).at[hot_ids].set(1)
    cold_sorted = jnp.argsort(is_hot * EXPERTS + jnp.arange(EXPERTS))[:N_COLD]
    cold_keys = jax.random.split(key_list[1], GROUP_SIZE)
    cold_perm = jax.vmap(lambda sub_key: jax.random.permutation(sub_key, cold_sorted))(cold_keys)
    win_start = jax.random.randint(key_list[2], (GROUP_SIZE, 1, 1), 0, N_COLD)
    cold_offset = slot_ids[None, None, :] - hot_count[:, :, None]
    cold_pos = (win_start + jnp.arange(TOK_DEV)[None, :, None] * TOP_K + cold_offset) % N_COLD
    cold_route = jnp.take_along_axis(cold_perm, cold_pos.reshape(GROUP_SIZE, TOK_DEV * TOP_K), axis=1)
    route_ids = jnp.where(cold_offset < 0, hot_route, cold_route.reshape(GROUP_SIZE, TOK_DEV, TOP_K))
    slot_rot = jax.random.randint(key_list[3], (GROUP_SIZE, TOK_DEV, 1), 0, TOP_K)
    route_ids = jnp.take_along_axis(route_ids, (slot_ids - slot_rot) % TOP_K, axis=2)
    return route_ids.reshape(TOKENS, TOP_K).astype(jnp.int32)


def setup_inputs(seed: int = 0, part: int = 0) -> dict:
    base_key = jax.random.fold_in(jax.random.key(seed), part)
    key_list = jax.random.split(base_key, 9)
    hot_first, hot_second = draw_hot_chips(key_list[0])
    route_idx = jnp.stack([draw_routing(key_list[1], hot_first), draw_routing(key_list[2], hot_second)])
    x = jax.random.normal(key_list[3], (2, TOKENS, D_MODEL), jnp.float32).astype(jnp.bfloat16)
    raw_gates = jax.random.uniform(key_list[4], (2, TOKENS, TOP_K), jnp.float32, 1.0, 2.0)
    gates = raw_gates / jnp.sum(raw_gates, axis=2, keepdims=True)
    w_gate = (jax.random.normal(key_list[5], (EXPERTS, D_MODEL, D_FF), jnp.float32) * D_MODEL ** -0.5).astype(jnp.bfloat16)
    w_up = (jax.random.normal(key_list[6], (EXPERTS, D_MODEL, D_FF), jnp.float32) * D_MODEL ** -0.5).astype(jnp.bfloat16)
    w_down = (jax.random.normal(key_list[7], (EXPERTS, D_FF, D_MODEL), jnp.float32) * D_FF ** -0.5).astype(jnp.bfloat16)
    grad_y = jax.random.normal(key_list[8], (2, TOKENS, D_MODEL), jnp.float32).astype(jnp.bfloat16)
    return {"x": x, "route_idx": route_idx, "gates": gates, "w_gate": w_gate, "w_up": w_up, "w_down": w_down, "grad_y": grad_y}


def swiglu_rows(x_rows, d_out, w_gate_e, w_up_e, w_down_e):
    gate_pre = jnp.dot(x_rows, w_gate_e, preferred_element_type=jnp.float32).astype(jnp.bfloat16)
    up_pre = jnp.dot(x_rows, w_up_e, preferred_element_type=jnp.float32).astype(jnp.bfloat16)
    gate_f = gate_pre.astype(jnp.float32)
    up_f = up_pre.astype(jnp.float32)
    sigmoid_g = jax.nn.sigmoid(gate_f)
    hidden = (gate_f * sigmoid_g * up_f).astype(jnp.bfloat16)
    exp_out = jnp.dot(hidden, w_down_e, preferred_element_type=jnp.float32).astype(jnp.bfloat16)
    d_act = jnp.dot(d_out, w_down_e.T, preferred_element_type=jnp.float32)
    d_up = (d_act * gate_f * sigmoid_g).astype(jnp.bfloat16)
    d_gate = (d_act * up_f * sigmoid_g * (1.0 + gate_f * (1.0 - sigmoid_g))).astype(jnp.bfloat16)
    d_in = (jnp.dot(d_gate, w_gate_e.T, preferred_element_type=jnp.float32) + jnp.dot(d_up, w_up_e.T, preferred_element_type=jnp.float32)).astype(jnp.bfloat16)
    g_gate = jnp.dot(x_rows.T, d_gate, preferred_element_type=jnp.float32)
    g_up = jnp.dot(x_rows.T, d_up, preferred_element_type=jnp.float32)
    g_down = jnp.dot(hidden.T, d_out, preferred_element_type=jnp.float32)
    return exp_out, d_in, g_gate, g_up, g_down


def microbatch(x, route_ids, gates, grad_y, w_gate, w_up, w_down):
    token_ids = jnp.arange(TOKENS)
    member = jnp.zeros((TOKENS, EXPERTS), jnp.int32).at[token_ids[:, None], route_ids].set(1)
    slot_rank = jnp.cumsum(member, axis=0) - member
    slot_pos = jnp.take_along_axis(slot_rank, route_ids, axis=1)
    slot_owner = jnp.full((EXPERTS * LOAD_MAX,), TOKENS * TOP_K, jnp.int32)
    slot_owner = slot_owner.at[(route_ids * LOAD_MAX + slot_pos).reshape(-1)].set(jnp.arange(TOKENS * TOP_K))
    slot_owner = slot_owner.reshape(EXPERTS, LOAD_MAX)
    x_pad = jnp.concatenate([x, jnp.zeros((1, D_MODEL), x.dtype)])
    dy_pad = jnp.concatenate([grad_y, jnp.zeros((1, D_MODEL), grad_y.dtype)])
    gate_pad = jnp.concatenate([gates.reshape(-1), jnp.zeros((1,), jnp.float32)])

    def one_expert(accums, per_expert):
        y_acc, dx_acc, dg_acc = accums
        slot_ids, w_gate_e, w_up_e, w_down_e = per_expert
        tok_rows = slot_ids // TOP_K
        row_gate = gate_pad[slot_ids]
        x_rows = x_pad[tok_rows]
        dy_rows = dy_pad[tok_rows].astype(jnp.float32)
        d_out = (row_gate[:, None] * dy_rows).astype(jnp.bfloat16)
        exp_out, d_in, g_gate, g_up, g_down = swiglu_rows(x_rows, d_out, w_gate_e, w_up_e, w_down_e)
        out_f = exp_out.astype(jnp.float32)
        y_acc = y_acc.at[tok_rows].add(row_gate[:, None] * out_f)
        dx_acc = dx_acc.at[tok_rows].add(d_in.astype(jnp.float32))
        dg_acc = dg_acc.at[slot_ids].add(jnp.sum(dy_rows * out_f, axis=1))
        return (y_acc, dx_acc, dg_acc), (g_gate, g_up, g_down)

    init_acc = (jnp.zeros((TOKENS + 1, D_MODEL), jnp.float32), jnp.zeros((TOKENS + 1, D_MODEL), jnp.float32), jnp.zeros((TOKENS * TOP_K + 1,), jnp.float32))
    final_acc, grads = lax.scan(one_expert, init_acc, (slot_owner, w_gate, w_up, w_down))
    y_acc, dx_acc, dg_acc = final_acc
    y_out = y_acc[:TOKENS].astype(jnp.bfloat16)
    dx_out = dx_acc[:TOKENS].astype(jnp.bfloat16)
    dg_out = dg_acc[:TOKENS * TOP_K].reshape(TOKENS, TOP_K)
    return y_out, dx_out, dg_out, grads[0], grads[1], grads[2]


def reference(x, route_idx, gates, w_gate, w_up, w_down, grad_y):
    mb_first = microbatch(x[0], route_idx[0], gates[0], grad_y[0], w_gate, w_up, w_down)
    mb_second = microbatch(x[1], route_idx[1], gates[1], grad_y[1], w_gate, w_up, w_down)
    return (jnp.stack([mb_first[0], mb_second[0]]), jnp.stack([mb_first[1], mb_second[1]]), jnp.stack([mb_first[2], mb_second[2]]), mb_first[3] + mb_second[3], mb_first[4] + mb_second[4], mb_first[5] + mb_second[5])
```

```python
import functools

import jax
import jax.numpy as jnp
from jax import lax
from jax.experimental import pallas as pl
from jax.experimental.pallas import tpu as pltpu
from jax.sharding import PartitionSpec as P

ALL_AXES = ("rep", "row", "col", "core")
MESH = pl.DeviceIdType.MESH
BF = jnp.bfloat16
F32 = jnp.float32
SLAB = 16
NBLK = 8
NEXP = 4
TOPK = 4


def coords():
    return (lax.axis_index("rep"), lax.axis_index("row"), lax.axis_index("col"), lax.axis_index("core"))


def peer(mask):
    rep, row, col, core = coords()
    flip = lambda pos, bit: 1 - pos if mask & bit else pos
    return (rep, flip(row, 4), flip(col, 2), flip(core, 1))


def number(mask=0):
    _, row, col, core = peer(mask)
    return row * 4 + col * 2 + core


def enter():
    barrier = pltpu.get_barrier_semaphore()
    for mask in range(1, NBLK):
        pl.semaphore_signal(barrier, inc=1, device_id=peer(mask), device_id_type=MESH)
    pl.semaphore_wait(barrier, NBLK - 1)


def remote(src, dst, send_sem, recv_sem, mask):
    return pltpu.make_async_remote_copy(src_ref=src, dst_ref=dst, send_sem=send_sem, recv_sem=recv_sem, device_id=peer(mask), device_id_type=MESH)


def gather_kernel(x_ref, dy_ref, route_ref, gate_ref, xg_ref, dyg_ref, rt_ref, mine, send_sem, recv_sem, rt_send, rt_recv):
    enter()
    me, at_x, at_y, at_d = number(0), number(2), number(4), number(6)
    outs = (xg_ref, dyg_ref)
    ins = (x_ref, dy_ref)
    PART = 6

    def copy(mb, kind):
        ss, rs = send_sem.at[mb, kind], recv_sem.at[mb, kind]
        if kind in (0, 1):
            return remote(ins[kind].at[mb], outs[kind].at[mb, me], ss, rs, 2)
        if kind == 2:
            return remote(dyg_ref.at[mb, at_y], dyg_ref.at[mb, at_y], ss, rs, 2)
        if kind in (3, 4):
            return remote(ins[kind - 3].at[mb], outs[kind - 3].at[mb, me], ss, rs, 4)
        if kind == 5:
            return remote(xg_ref.at[mb, at_x], xg_ref.at[mb, at_x], ss, rs, 4)
        which, origin = (kind - PART) % 2, (kind - PART) // 2
        if origin == 0:
            return remote(ins[which].at[mb], outs[which].at[mb, me], ss, rs, 1)
        slot = (at_x, at_y, at_d)[origin - 1]
        return remote(outs[which].at[mb, slot], outs[which].at[mb, slot], ss, rs, 1)

    for mb in range(2):
        for kind in (0, 3, 1, 4, 6, 7):
            copy(mb, kind).start()
    tok = x_ref.shape[1]
    eye = lax.broadcasted_iota(jnp.int32, (tok, tok), 0) == lax.broadcasted_iota(jnp.int32, (tok, tok), 1)
    for mb in range(2):
        routes, gates = route_ref[mb].astype(F32), gate_ref[mb]
        rows = [jnp.sum(jnp.where(eye, arr[:, j : j + 1], 0.0), axis=0, keepdims=True) for arr in (routes, gates) for j in range(TOPK)]
        mine[pl.ds(mb * 8, 8), :] = jnp.concatenate(rows, axis=0)
    rt_ref[me] = mine[...]
    for mask in range(1, NBLK):
        remote(mine, rt_ref.at[me], rt_send.at[mask], rt_recv.at[mask], mask).start()
    for mb in range(2):
        xg_ref[mb, me] = x_ref[mb]
        dyg_ref[mb, me] = dy_ref[mb]
    for mb in range(2):
        copy(mb, 0).wait_recv()
        copy(mb, 5).start()
        copy(mb, 8).start()
        copy(mb, 3).wait_recv()
        copy(mb, 10).start()
        copy(mb, 1).wait_recv()
        copy(mb, 9).start()
        copy(mb, 4).wait_recv()
        copy(mb, 2).start()
        copy(mb, 11).start()
    for mb in range(2):
        copy(mb, 5).wait_recv()
        copy(mb, 12).start()
        copy(mb, 2).wait_recv()
        copy(mb, 13).start()
    for mask in range(1, NBLK):
        remote(mine, rt_ref.at[me], rt_send.at[mask], rt_recv.at[mask], mask).wait()
    for mb in range(2):
        for kind in range(PART, 14):
            copy(mb, kind).wait_recv()
        for kind in range(14):
            copy(mb, kind).wait_send()


def gather_all(x, grad_y, route_idx, gates):
    _, tok, dim = x.shape
    vmem = pl.BlockSpec(memory_space=pltpu.VMEM)
    return pl.pallas_call(
        gather_kernel,
        out_shape=(
            jax.ShapeDtypeStruct((2, NBLK, tok, dim), BF),
            jax.ShapeDtypeStruct((2, NBLK, tok, dim), BF),
            jax.ShapeDtypeStruct((NBLK, 16, tok), F32),
        ),
        in_specs=[vmem] * 4,
        out_specs=(vmem,) * 3,
        scratch_shapes=[
            pltpu.VMEM((16, tok), F32),
            pltpu.SemaphoreType.DMA((2, 14)),
            pltpu.SemaphoreType.DMA((2, 14)),
            pltpu.SemaphoreType.DMA((NBLK,)),
            pltpu.SemaphoreType.DMA((NBLK,)),
        ],
        compiler_params=pltpu.CompilerParams(collective_id=0, has_side_effects=True, vmem_limit_bytes=16 << 20),
        name="gather_tokens",
    )(x, grad_y, route_idx, gates)


def tdot(lhs, rhs):
    return lax.dot_general(lhs, rhs, (((0,), (0,)), ((), ())), preferred_element_type=F32)


def ndot(lhs, rhs):
    return lax.dot_general(lhs, rhs, (((1,), (1,)), ((), ())), preferred_element_type=F32)


def dot(lhs, rhs):
    return jnp.dot(lhs, rhs, preferred_element_type=F32)


def expert_kernel(xg_ref, dyg_ref, rt_ref, wg_hbm, wu_hbm, wd_hbm, part_ref, dg_ref, gg_hbm, gu_hbm, gd_hbm,
                  wgu, wd, ggu, gd, rank, grow, disp0, disp12, xr, qr, dyr, gcol, z0, z12, p0, p12, dc0, dc12, more, in_sem, out_sem):
    tok, dim = xg_ref.shape[2], xg_ref.shape[3]
    ff = wd.shape[1]
    loads = []
    for l in range(NEXP):
        loads.append((
            pltpu.make_async_copy(wg_hbm.at[l], wgu.at[l, :, pl.ds(0, ff)], in_sem.at[l, 0]),
            pltpu.make_async_copy(wu_hbm.at[l], wgu.at[l, :, pl.ds(ff, ff)], in_sem.at[l, 1]),
            pltpu.make_async_copy(wd_hbm.at[l], wd.at[l], in_sem.at[l, 2]),
        ))
        for load in loads[-1]:
            load.start()
    first = (number() * NEXP).astype(F32)

    members = []
    for mb in range(2):
        routes, gates = rt_ref[:, mb * 8 : mb * 8 + 4, :], rt_ref[:, mb * 8 + 4 : mb * 8 + 8, :]
        for l in range(NEXP):
            hit = routes == first + l
            members.append(jnp.sum(jnp.where(hit, 1.0, 0.0), axis=1))
            grow[mb, l] = jnp.sum(jnp.where(hit, gates, 0.0), axis=1)
    member = jnp.concatenate(members, axis=0)
    before = lax.broadcasted_iota(jnp.int32, (tok, tok), 0) < lax.broadcasted_iota(jnp.int32, (tok, tok), 1)
    ranks = jnp.where(member > 0, dot(member.astype(BF), jnp.where(before, 1.0, 0.0).astype(BF)), -1.0)
    for mb in range(2):
        for l in range(NEXP):
            here = ranks[(mb * NEXP + l) * NBLK : (mb * NEXP + l + 1) * NBLK]
            rank[mb, l] = here
            more[mb * NEXP + l] = (jnp.max(here) >= SLAB - 0.5).astype(jnp.int32)
    any_more = [functools.reduce(jnp.maximum, [more[mb * NEXP + l] for l in range(NEXP)]) for mb in range(2)]
    slab_iota = lax.broadcasted_iota(jnp.int32, (SLAB, tok), 0).astype(F32)

    def dispatch(mb, b, slabs, disp):
        hot, gs = [], []
        for s in slabs:
            for l in range(NEXP):
                hot.append(jnp.where(rank[mb, l, pl.ds(b, 1), :] == slab_iota + s * SLAB, 1.0, 0.0))
                gs.append(jnp.broadcast_to(grow[mb, l, pl.ds(b, 1), :], (SLAB, tok)))
        hot = jnp.concatenate(hot, axis=0)
        gate = jnp.sum(hot * jnp.concatenate(gs, axis=0), axis=1, keepdims=True)
        hot = hot.astype(BF)
        disp[mb, b] = hot
        xs = dot(hot, xg_ref[mb, b]).astype(BF)
        dys = dot(hot, dyg_ref[mb, b])
        qs = (gate * dys).astype(BF)
        dys = dys.astype(BF)
        rows = pl.ds(pl.multiple_of(b * SLAB, SLAB), SLAB)
        for i, s in enumerate(slabs):
            pair, half = (0, mb) if s == 0 else (1 + mb, s - 1)
            for l in range(NEXP):
                cut = slice((i * NEXP + l) * SLAB, (i * NEXP + l + 1) * SLAB)
                xr[pair, l, half, rows, :] = xs[cut]
                dyr[pair, l, half, rows, :] = dys[cut]
                qr[pair, l, half, rows, :] = qs[cut]
                gcol[pair, l, half, rows, :] = gate[cut]

    for mb in range(2):
        @pl.loop(0, NBLK)
        def _(b):
            dispatch(mb, b, (0,), disp0)

        @pl.when(any_more[mb] > 0)
        def _():
            @pl.loop(0, NBLK)
            def _(b):
                dispatch(mb, b, (1, 2), disp12)

    rows = 2 * NBLK * SLAB

    def experts(pair, l, fresh):
        xs, qs = xr[pair, l].reshape(rows, dim), qr[pair, l].reshape(rows, dim)
        both = dot(xs, wgu[l]).astype(BF).astype(F32)
        u, v = both[:, :ff], both[:, ff:]
        s = jax.nn.sigmoid(u)
        hidden = (u * s * v).astype(BF)
        out = dot(hidden, wd[l]).astype(BF).astype(F32)
        back = ndot(qs, wd[l])
        d_up = (back * u * s).astype(BF)
        d_gate = (back * v * s * (1.0 + u * (1.0 - s))).astype(BF)
        d_both = jnp.concatenate([d_gate, d_up], axis=1)
        d_in = ndot(d_both, wgu[l]).astype(BF)
        if fresh:
            gd[l] = tdot(hidden, qs)
            ggu[l] = tdot(xs, d_both)
        else:
            gd[l] = gd[l] + tdot(hidden, qs)
            ggu[l] = ggu[l] + tdot(xs, d_both)
        dots = jnp.sum(dyr[pair, l].reshape(rows, dim).astype(F32) * out, axis=1, keepdims=True)
        z = gcol[pair, l].reshape(rows, 1) * out
        hi = z.astype(BF)
        rest = z - hi.astype(F32)
        mid = rest.astype(BF)
        low = (rest - mid.astype(F32)).astype(BF)
        return (hi, mid, low), d_in, dots

    def store0(l, zs, d_in, dots):
        for mb in range(2):
            for b in range(NBLK):
                cut = slice((mb * NBLK + b) * SLAB, (mb * NBLK + b + 1) * SLAB)
                at = pl.multiple_of(l * SLAB, SLAB)
                for i, part in enumerate(zs):
                    z0[mb, b, pl.ds(i * NEXP * SLAB + at, SLAB), :] = part[cut]
                p0[mb, b, pl.ds(at, SLAB), :] = d_in[cut]
                dc0[mb, b, pl.ds(at, SLAB), :] = dots[cut]

    def store12(mb, l, zs, d_in, dots):
        for s in range(2):
            for b in range(NBLK):
                cut = slice((s * NBLK + b) * SLAB, (s * NBLK + b + 1) * SLAB)
                at = pl.multiple_of((s * NEXP + l) * SLAB, SLAB)
                for i, part in enumerate(zs):
                    z12[mb, b, pl.ds(2 * i * NEXP * SLAB + at, SLAB), :] = part[cut]
                p12[mb, b, pl.ds(at, SLAB), :] = d_in[cut]
                dc12[mb, b, pl.ds(at, SLAB), :] = dots[cut]

    def stores(l):
        return (
            pltpu.make_async_copy(ggu.at[l, :, pl.ds(0, ff)], gg_hbm.at[l], out_sem.at[l, 0]),
            pltpu.make_async_copy(ggu.at[l, :, pl.ds(ff, ff)], gu_hbm.at[l], out_sem.at[l, 1]),
            pltpu.make_async_copy(gd.at[l], gd_hbm.at[l], out_sem.at[l, 2]),
        )

    for l in range(NEXP):
        for load in loads[l]:
            load.wait()

    @pl.loop(0, NEXP)
    def _(l):
        store0(l, *experts(0, l, True))

        @pl.loop(0, 2)
        def _(mb):
            flag = more[mb * NEXP + l]

            @pl.when(flag > 0)
            def _():
                store12(mb, l, *experts(1 + mb, l, False))

            @pl.when(flag == 0)
            def _():
                for s in range(2):
                    at = pl.multiple_of((s * NEXP + l) * SLAB, SLAB)
                    for i in range(3):
                        z12[mb, :, pl.ds(2 * i * NEXP * SLAB + at, SLAB), :] = jnp.zeros((NBLK, SLAB, dim), BF)
                    p12[mb, :, pl.ds(at, SLAB), :] = jnp.zeros((NBLK, SLAB, dim), BF)
                    dc12[mb, :, pl.ds(at, SLAB), :] = jnp.zeros((NBLK, SLAB, 1), F32)

        for store in stores(l):
            store.start()

    def by_slot(mb, b, hot, dots):
        spread = hot.astype(F32) * dots
        groups = spread.shape[0] // (NEXP * SLAB)
        routes = rt_ref[b, pl.ds(mb * 8, TOPK), :]
        total = jnp.zeros((TOPK, tok), F32)
        for l in range(NEXP):
            line = sum(jnp.sum(spread[(g * NEXP + l) * SLAB : (g * NEXP + l + 1) * SLAB], axis=0, keepdims=True) for g in range(groups))
            total = total + jnp.where(routes == first + l, line, 0.0)
        return total

    for mb in range(2):
        @pl.loop(0, NBLK)
        def _(b):
            hot = disp0[mb, b]
            part_ref[0, mb, b] = tdot(jnp.concatenate([hot] * 3, axis=0), z0[mb, b])
            part_ref[1, mb, b] = tdot(hot, p0[mb, b])
            dg_ref[b, pl.ds(mb * TOPK, TOPK), :] = by_slot(mb, b, hot, dc0[mb, b])

        @pl.when(any_more[mb] > 0)
        def _():
            @pl.loop(0, NBLK)
            def _(b):
                hot = disp12[mb, b]
                part_ref[0, mb, b] += tdot(jnp.concatenate([hot] * 3, axis=0), z12[mb, b])
                part_ref[1, mb, b] += tdot(hot, p12[mb, b])
                dg_ref[b, pl.ds(mb * TOPK, TOPK), :] += by_slot(mb, b, hot, dc12[mb, b])

    for l in range(NEXP):
        for store in stores(l):
            store.wait()


def run_experts(xg, dyg, rt, w_gate, w_up, w_down):
    _, _, tok, dim = xg.shape
    ff = w_gate.shape[2]
    vmem, hbm = pl.BlockSpec(memory_space=pltpu.VMEM), pl.BlockSpec(memory_space=pl.ANY)
    half = NBLK * SLAB
    one, two = NEXP * SLAB, 2 * NEXP * SLAB
    return pl.pallas_call(
        expert_kernel,
        out_shape=(
            jax.ShapeDtypeStruct((2, 2, NBLK, tok, dim), F32),
            jax.ShapeDtypeStruct((NBLK, 2 * TOPK, tok), F32),
            jax.ShapeDtypeStruct(w_gate.shape, F32),
            jax.ShapeDtypeStruct(w_up.shape, F32),
            jax.ShapeDtypeStruct(w_down.shape, F32),
        ),
        in_specs=[vmem] * 3 + [hbm] * 3,
        out_specs=(vmem, vmem, hbm, hbm, hbm),
        scratch_shapes=[
            pltpu.VMEM((NEXP, dim, 2 * ff), BF),
            pltpu.VMEM((NEXP, ff, dim), BF),
            pltpu.VMEM((NEXP, dim, 2 * ff), F32),
            pltpu.VMEM((NEXP, ff, dim), F32),
            pltpu.VMEM((2, NEXP, NBLK, tok), F32),
            pltpu.VMEM((2, NEXP, NBLK, tok), F32),
            pltpu.VMEM((2, NBLK, one, tok), BF),
            pltpu.VMEM((2, NBLK, two, tok), BF),
            pltpu.VMEM((3, NEXP, 2, half, dim), BF),
            pltpu.VMEM((3, NEXP, 2, half, dim), BF),
            pltpu.VMEM((3, NEXP, 2, half, dim), BF),
            pltpu.VMEM((3, NEXP, 2, half, 1), F32),
            pltpu.VMEM((2, NBLK, 3 * one, dim), BF),
            pltpu.VMEM((2, NBLK, 3 * two, dim), BF),
            pltpu.VMEM((2, NBLK, one, dim), BF),
            pltpu.VMEM((2, NBLK, two, dim), BF),
            pltpu.VMEM((2, NBLK, one, 1), F32),
            pltpu.VMEM((2, NBLK, two, 1), F32),
            pltpu.SMEM((2 * NEXP,), jnp.int32),
            pltpu.SemaphoreType.DMA((NEXP, 3)),
            pltpu.SemaphoreType.DMA((NEXP, 3)),
        ],
        compiler_params=pltpu.CompilerParams(vmem_limit_bytes=52 << 20),
        name="experts",
    )(xg, dyg, rt, w_gate, w_up, w_down)


def combine_kernel(part_ref, dg_ref, y_ref, dx_ref, gg_ref, near, chip_sum, first_in, second_in, out, dg_in,
                   near_send, near_recv, first_send, first_recv, second_send, second_recv, out_send, out_recv, dg_send, dg_recv):
    enter()
    _, row, col, core = coords()
    me = number()
    tok = dg_ref.shape[2]

    def blocks(mask):
        return number(mask) - core

    def to_partner(mb, mask):
        at = pl.ds(blocks(mask), 2)
        i = mask // 2
        return remote(part_ref.at[1 - core, mb, at], near.at[mb, i], near_send.at[mb, i], near_recv.at[mb, i], 1)

    def add_chip(mb, mask):
        to_partner(mb, mask).wait_recv()
        i = mask // 2
        chip_sum[mb, i] = part_ref[core, mb, pl.ds(blocks(mask), 2)] + near[mb, i]

    FIRST, SECOND = (2, 4), (4, 2)

    def first(mb, which):
        mask = (6, FIRST[mb])[which]
        return remote(chip_sum.at[mb, mask // 2], first_in.at[mb, which], first_send.at[mb, which], first_recv.at[mb, which], FIRST[mb])

    def second(mb, h):
        return remote(chip_sum.at[mb, SECOND[mb] // 2, h], second_in.at[mb, h], second_send.at[mb, h], second_recv.at[mb, h], SECOND[mb])

    def dg_copy(mask):
        return remote(dg_ref.at[number(mask)], dg_in.at[me], dg_send.at[mask], dg_recv.at[mask], mask)

    for which in range(4):
        for mb in range(2):
            to_partner(mb, (6, FIRST[mb], SECOND[mb], 0)[which]).start()
    for mask in range(1, NBLK):
        dg_copy(mask).start()
    for which in range(2):
        for mb in range(2):
            add_chip(mb, (6, FIRST[mb])[which])
            first(mb, which).start()
    for mb in range(2):
        add_chip(mb, SECOND[mb])
    for mb in range(2):
        first(mb, 0).wait_recv()
        for h in range(2):
            chip_sum[mb, SECOND[mb] // 2, h] += first_in[mb, 0, h]
            second(mb, h).start()
    dg_in[me] = dg_ref[me]
    for mb in range(2):
        add_chip(mb, 0)
    for mask in range(1, NBLK):
        dg_copy(mask).wait()
    grads = jnp.sum(dg_in[...], axis=0)
    eye = lax.broadcasted_iota(jnp.int32, (tok, tok), 0) == lax.broadcasted_iota(jnp.int32, (tok, tok), 1)
    for mb in range(2):
        cols = [jnp.sum(jnp.where(eye, grads[mb * TOPK + j : mb * TOPK + j + 1, :], 0.0), axis=1, keepdims=True) for j in range(TOPK)]
        gg_ref[mb] = jnp.concatenate(cols, axis=1)
    for mb in range(2):
        first(mb, 1).wait_recv()
        chip_sum[mb, 0] += first_in[mb, 1]

    def handover(mb):
        return remote(out.at[2, mb], out.at[core, mb], out_send.at[mb], out_recv.at[mb], 1)

    for h in range(2):
        for mb in range(2):
            second(mb, h).wait_recv()
            done = (chip_sum[mb, 0, h] + second_in[mb, h]).astype(BF)

            @pl.when(core == h)
            def _():
                out[core, mb] = done

            @pl.when(core != h)
            def _():
                out[2, mb] = done
    for mb in range(2):
        handover(mb).start()
    for mb in range(2):
        handover(mb).wait()
    y_ref[...] = out[0]
    dx_ref[...] = out[1]
    for mb in range(2):
        for i in range(4):
            to_partner(mb, 2 * i).wait_send()
        for i in range(2):
            first(mb, i).wait_send()
            second(mb, i).wait_send()


def combine(part, dg):
    _, _, _, tok, dim = part.shape
    vmem = pl.BlockSpec(memory_space=pltpu.VMEM)
    sem = pltpu.SemaphoreType.DMA
    return pl.pallas_call(
        combine_kernel,
        out_shape=(
            jax.ShapeDtypeStruct((2, tok, dim), BF),
            jax.ShapeDtypeStruct((2, tok, dim), BF),
            jax.ShapeDtypeStruct((2, tok, TOPK), F32),
        ),
        in_specs=[vmem] * 2,
        out_specs=(vmem,) * 3,
        scratch_shapes=[
            pltpu.VMEM((2, 4, 2, tok, dim), F32),
            pltpu.VMEM((2, 4, 2, tok, dim), F32),
            pltpu.VMEM((2, 2, 2, tok, dim), F32),
            pltpu.VMEM((2, 2, tok, dim), F32),
            pltpu.VMEM((3, 2, tok, dim), BF),
            pltpu.VMEM((NBLK, 2 * TOPK, tok), F32),
            sem((2, 4)), sem((2, 4)), sem((2, 2)), sem((2, 2)), sem((2, 2)), sem((2, 2)), sem((2,)), sem((2,)), sem((NBLK,)), sem((NBLK,)),
        ],
        compiler_params=pltpu.CompilerParams(collective_id=1, has_side_effects=True, vmem_limit_bytes=32 << 20),
        name="combine_tokens",
    )(part, dg)


def solution(mesh):
    tok_spec = P(None, ALL_AXES, None)
    w_spec = P(ALL_AXES, None, None)

    def moe_layer(x, route_idx, gates, w_gate, w_up, w_down, grad_y):
        xg, dyg, rt = gather_all(x, grad_y, route_idx, gates)
        part, dg, g_gate, g_up, g_down = run_experts(xg, dyg, rt, w_gate, w_up, w_down)
        y, dx, g_gates = combine(part, dg)
        return y, dx, g_gates, g_gate, g_up, g_down

    return jax.shard_map(moe_layer, mesh=mesh, in_specs=(tok_spec, tok_spec, tok_spec, w_spec, w_spec, w_spec, tok_spec), out_specs=(tok_spec, tok_spec, tok_spec, w_spec, w_spec, w_spec), check_vma=False)
```

```python
import functools

import jax
import jax.numpy as jnp
from jax import lax
from jax.experimental import pallas as pl
from jax.experimental.pallas import tpu as pltpu
from jax.sharding import PartitionSpec as P

ALL_AXES = ("rep", "row", "col", "core")
MESH = pl.DeviceIdType.MESH
BF = jnp.bfloat16
F32 = jnp.float32
SLAB = 16
NBLK = 8
NEXP = 4
TOPK = 4


def coords():
    return (lax.axis_index("rep"), lax.axis_index("row"), lax.axis_index("col"), lax.axis_index("core"))


def peer(mask):
    rep, row, col, core = coords()
    flip = lambda pos, bit: 1 - pos if mask & bit else pos
    return (rep, flip(row, 4), flip(col, 2), flip(core, 1))


def number(mask=0):
    _, row, col, core = peer(mask)
    return row * 4 + col * 2 + core


def enter():
    barrier = pltpu.get_barrier_semaphore()
    for mask in range(1, NBLK):
        pl.semaphore_signal(barrier, inc=1, device_id=peer(mask), device_id_type=MESH)
    pl.semaphore_wait(barrier, NBLK - 1)


def remote(src, dst, send_sem, recv_sem, mask):
    return pltpu.make_async_remote_copy(src_ref=src, dst_ref=dst, send_sem=send_sem, recv_sem=recv_sem, device_id=peer(mask), device_id_type=MESH)


def gather_kernel(x_hbm, dy_hbm, route_hbm, gate_hbm, xg_ref, dyg_ref, rt_ref, route_ref, gate_ref, mine, tab_sem, own_sem, send_sem, recv_sem, rt_send, rt_recv):
    me, at_x, at_y, at_d = number(0), number(2), number(4), number(6)
    outs = (xg_ref, dyg_ref)
    PART = 6
    own = [[pltpu.make_async_copy(src.at[mb], dst.at[mb, me], own_sem.at[mb, i]) for i, (src, dst) in enumerate(((x_hbm, xg_ref), (dy_hbm, dyg_ref)))] for mb in range(2)]
    tables = [pltpu.make_async_copy(src, dst, tab_sem.at[i]) for i, (src, dst) in enumerate(((route_hbm, route_ref), (gate_hbm, gate_ref)))]
    for load in tables + own[0] + own[1]:
        load.start()
    for load in tables:
        load.wait()
    for mb in range(2):
        mine[pl.ds(mb * 8, TOPK), :] = route_ref[mb].astype(F32)
        mine[pl.ds(mb * 8 + TOPK, TOPK), :] = gate_ref[mb]
    rt_ref[me] = mine[...]
    enter()

    def copy(mb, kind):
        if kind < PART:
            which, slot, mask = ((0, me, 2), (1, me, 2), (1, at_y, 2), (0, me, 4), (1, me, 4), (0, at_x, 4))[kind]
        else:
            which, slot, mask = (kind - PART) % 2, (me, at_x, at_y, at_d)[(kind - PART) // 2], 1
        ref = outs[which].at[mb, slot]
        return remote(ref, ref, send_sem.at[mb, kind], recv_sem.at[mb, kind], mask)

    for mb in range(2):
        for kinds, load in zip(((0, 3, 6), (1, 4, 7)), own[mb]):
            load.wait()
            for kind in kinds:
                copy(mb, kind).start()
    for mask in range(1, NBLK):
        remote(mine, rt_ref.at[me], rt_send.at[mask], rt_recv.at[mask], mask).start()
    for mb in range(2):
        copy(mb, 0).wait_recv()
        copy(mb, 5).start()
        copy(mb, 8).start()
        copy(mb, 3).wait_recv()
        copy(mb, 10).start()
        copy(mb, 1).wait_recv()
        copy(mb, 9).start()
        copy(mb, 4).wait_recv()
        copy(mb, 2).start()
        copy(mb, 11).start()
    for mb in range(2):
        copy(mb, 5).wait_recv()
        copy(mb, 12).start()
        copy(mb, 2).wait_recv()
        copy(mb, 13).start()
    for mask in range(1, NBLK):
        remote(mine, rt_ref.at[me], rt_send.at[mask], rt_recv.at[mask], mask).wait()
    for mb in range(2):
        for kind in range(PART, 14):
            copy(mb, kind).wait_recv()
        for kind in range(14):
            copy(mb, kind).wait_send()


def gather_all(x, grad_y, route_rows, gate_rows):
    _, tok, dim = x.shape
    vmem, hbm = pl.BlockSpec(memory_space=pltpu.VMEM), pl.BlockSpec(memory_space=pltpu.HBM)
    return pl.pallas_call(
        gather_kernel,
        out_shape=(
            jax.ShapeDtypeStruct((2, NBLK, tok, dim), BF),
            jax.ShapeDtypeStruct((2, NBLK, tok, dim), BF),
            jax.ShapeDtypeStruct((NBLK, 16, tok), F32),
        ),
        in_specs=[hbm] * 4,
        out_specs=(vmem,) * 3,
        scratch_shapes=[
            pltpu.VMEM((2, TOPK, tok), jnp.int32),
            pltpu.VMEM((2, TOPK, tok), F32),
            pltpu.VMEM((16, tok), F32),
            pltpu.SemaphoreType.DMA((2,)),
            pltpu.SemaphoreType.DMA((2, 2)),
            pltpu.SemaphoreType.DMA((2, 14)),
            pltpu.SemaphoreType.DMA((2, 14)),
            pltpu.SemaphoreType.DMA((NBLK,)),
            pltpu.SemaphoreType.DMA((NBLK,)),
        ],
        compiler_params=pltpu.CompilerParams(collective_id=0, has_side_effects=True, vmem_limit_bytes=8 << 20),
        name="gather_tokens",
    )(x, grad_y, route_rows, gate_rows)


def tdot(lhs, rhs):
    return lax.dot_general(lhs, rhs, (((0,), (0,)), ((), ())), preferred_element_type=F32)


def ndot(lhs, rhs):
    return lax.dot_general(lhs, rhs, (((1,), (1,)), ((), ())), preferred_element_type=F32)


def dot(lhs, rhs):
    return jnp.dot(lhs, rhs, preferred_element_type=F32)


def expert_kernel(xg_ref, dyg_ref, rt_ref, wg_hbm, wu_hbm, wd_hbm, part_ref, dg_ref, gg_hbm, gu_hbm, gd_hbm,
                  wgu, wd, ggu, gd, rank, grow, disp0, disp12, xr, qr, dyr, gcol, z0, z12, p0, p12, dc0, dc12, more, in_sem, out_sem):
    tok, dim = xg_ref.shape[2], xg_ref.shape[3]
    ff = wd.shape[1]
    loads = []
    for l in range(NEXP):
        loads.append((
            pltpu.make_async_copy(wg_hbm.at[l], wgu.at[l, :, pl.ds(0, ff)], in_sem.at[l, 0]),
            pltpu.make_async_copy(wu_hbm.at[l], wgu.at[l, :, pl.ds(ff, ff)], in_sem.at[l, 1]),
            pltpu.make_async_copy(wd_hbm.at[l], wd.at[l], in_sem.at[l, 2]),
        ))
        for load in loads[-1]:
            load.start()
    first = (number() * NEXP).astype(F32)

    members = []
    for mb in range(2):
        routes, gates = rt_ref[:, mb * 8 : mb * 8 + 4, :], rt_ref[:, mb * 8 + 4 : mb * 8 + 8, :]
        for l in range(NEXP):
            hit = routes == first + l
            members.append(jnp.sum(jnp.where(hit, 1.0, 0.0), axis=1))
            grow[mb, l] = jnp.sum(jnp.where(hit, gates, 0.0), axis=1)
    member = jnp.concatenate(members, axis=0)
    before = lax.broadcasted_iota(jnp.int32, (tok, tok), 0) < lax.broadcasted_iota(jnp.int32, (tok, tok), 1)
    ranks = jnp.where(member > 0, dot(member.astype(BF), jnp.where(before, 1.0, 0.0).astype(BF)), -1.0)
    for mb in range(2):
        for l in range(NEXP):
            here = ranks[(mb * NEXP + l) * NBLK : (mb * NEXP + l + 1) * NBLK]
            rank[mb, l] = here
            more[mb * NEXP + l] = (jnp.max(here) >= SLAB - 0.5).astype(jnp.int32)
    any_more = [functools.reduce(jnp.maximum, [more[mb * NEXP + l] for l in range(NEXP)]) for mb in range(2)]
    slab_iota = lax.broadcasted_iota(jnp.int32, (SLAB, tok), 0).astype(F32)

    def dispatch(mb, b, slabs, disp):
        hot, gs = [], []
        for s in slabs:
            for l in range(NEXP):
                hot.append(jnp.where(rank[mb, l, pl.ds(b, 1), :] == slab_iota + s * SLAB, 1.0, 0.0))
                gs.append(jnp.broadcast_to(grow[mb, l, pl.ds(b, 1), :], (SLAB, tok)))
        hot = jnp.concatenate(hot, axis=0)
        gate = jnp.sum(hot * jnp.concatenate(gs, axis=0), axis=1, keepdims=True)
        hot = hot.astype(BF)
        disp[mb, b] = hot
        xs = dot(hot, xg_ref[mb, b]).astype(BF)
        dys = dot(hot, dyg_ref[mb, b])
        qs = (gate * dys).astype(BF)
        dys = dys.astype(BF)
        rows = pl.ds(pl.multiple_of(b * SLAB, SLAB), SLAB)
        for i, s in enumerate(slabs):
            pair, half = (0, mb) if s == 0 else (1 + mb, s - 1)
            for l in range(NEXP):
                cut = slice((i * NEXP + l) * SLAB, (i * NEXP + l + 1) * SLAB)
                xr[pair, l, half, rows, :] = xs[cut]
                dyr[pair, l, half, rows, :] = dys[cut]
                qr[pair, l, half, rows, :] = qs[cut]
                gcol[pair, l, half, rows, :] = gate[cut]

    for mb in range(2):
        @pl.loop(0, NBLK)
        def _(b):
            dispatch(mb, b, (0,), disp0)

        @pl.when(any_more[mb] > 0)
        def _():
            @pl.loop(0, NBLK)
            def _(b):
                dispatch(mb, b, (1, 2), disp12)

    rows = 2 * NBLK * SLAB

    def experts(pair, l, fresh):
        xs, qs = xr[pair, l].reshape(rows, dim), qr[pair, l].reshape(rows, dim)
        both = dot(xs, wgu[l]).astype(BF).astype(F32)
        u, v = both[:, :ff], both[:, ff:]
        s = jax.nn.sigmoid(u)
        hidden = (u * s * v).astype(BF)
        out = dot(hidden, wd[l]).astype(BF).astype(F32)
        back = ndot(qs, wd[l])
        d_up = (back * u * s).astype(BF)
        d_gate = (back * v * s * (1.0 + u * (1.0 - s))).astype(BF)
        d_both = jnp.concatenate([d_gate, d_up], axis=1)
        d_in = ndot(d_both, wgu[l]).astype(BF)
        if fresh:
            gd[l] = tdot(hidden, qs)
            ggu[l] = tdot(xs, d_both)
        else:
            gd[l] = gd[l] + tdot(hidden, qs)
            ggu[l] = ggu[l] + tdot(xs, d_both)
        dots = jnp.sum(dyr[pair, l].reshape(rows, dim).astype(F32) * out, axis=1, keepdims=True)
        z = gcol[pair, l].reshape(rows, 1) * out
        hi = z.astype(BF)
        rest = z - hi.astype(F32)
        mid = rest.astype(BF)
        low = (rest - mid.astype(F32)).astype(BF)
        return (hi, mid, low), d_in, dots

    def store0(l, zs, d_in, dots):
        for mb in range(2):
            for b in range(NBLK):
                cut = slice((mb * NBLK + b) * SLAB, (mb * NBLK + b + 1) * SLAB)
                at = pl.multiple_of(l * SLAB, SLAB)
                for i, part in enumerate(zs):
                    z0[mb, b, pl.ds(i * NEXP * SLAB + at, SLAB), :] = part[cut]
                p0[mb, b, pl.ds(at, SLAB), :] = d_in[cut]
                dc0[mb, b, pl.ds(at, SLAB), :] = dots[cut]

    def store12(mb, l, zs, d_in, dots):
        for s in range(2):
            for b in range(NBLK):
                cut = slice((s * NBLK + b) * SLAB, (s * NBLK + b + 1) * SLAB)
                at = pl.multiple_of((s * NEXP + l) * SLAB, SLAB)
                for i, part in enumerate(zs):
                    z12[mb, b, pl.ds(2 * i * NEXP * SLAB + at, SLAB), :] = part[cut]
                p12[mb, b, pl.ds(at, SLAB), :] = d_in[cut]
                dc12[mb, b, pl.ds(at, SLAB), :] = dots[cut]

    def stores(l):
        return (
            pltpu.make_async_copy(ggu.at[l, :, pl.ds(0, ff)], gg_hbm.at[l], out_sem.at[l, 0]),
            pltpu.make_async_copy(ggu.at[l, :, pl.ds(ff, ff)], gu_hbm.at[l], out_sem.at[l, 1]),
            pltpu.make_async_copy(gd.at[l], gd_hbm.at[l], out_sem.at[l, 2]),
        )

    for l in range(NEXP):
        for load in loads[l]:
            load.wait()

    @pl.loop(0, NEXP)
    def _(l):
        store0(l, *experts(0, l, True))

        @pl.loop(0, 2)
        def _(mb):
            flag = more[mb * NEXP + l]

            @pl.when(flag > 0)
            def _():
                store12(mb, l, *experts(1 + mb, l, False))

            @pl.when(flag == 0)
            def _():
                for s in range(2):
                    at = pl.multiple_of((s * NEXP + l) * SLAB, SLAB)
                    for i in range(3):
                        z12[mb, :, pl.ds(2 * i * NEXP * SLAB + at, SLAB), :] = jnp.zeros((NBLK, SLAB, dim), BF)
                    p12[mb, :, pl.ds(at, SLAB), :] = jnp.zeros((NBLK, SLAB, dim), BF)
                    dc12[mb, :, pl.ds(at, SLAB), :] = jnp.zeros((NBLK, SLAB, 1), F32)

        for store in stores(l):
            store.start()

    def by_slot(mb, b, hot, dots):
        spread = hot.astype(F32) * dots
        groups = spread.shape[0] // (NEXP * SLAB)
        routes = rt_ref[b, pl.ds(mb * 8, TOPK), :]
        total = jnp.zeros((TOPK, tok), F32)
        for l in range(NEXP):
            line = sum(jnp.sum(spread[(g * NEXP + l) * SLAB : (g * NEXP + l + 1) * SLAB], axis=0, keepdims=True) for g in range(groups))
            total = total + jnp.where(routes == first + l, line, 0.0)
        return total

    for mb in range(2):
        @pl.loop(0, NBLK)
        def _(b):
            hot = disp0[mb, b]
            part_ref[0, mb, b] = tdot(jnp.concatenate([hot] * 3, axis=0), z0[mb, b])
            part_ref[1, mb, b] = tdot(hot, p0[mb, b])
            dg_ref[b, pl.ds(mb * TOPK, TOPK), :] = by_slot(mb, b, hot, dc0[mb, b])

        @pl.when(any_more[mb] > 0)
        def _():
            @pl.loop(0, NBLK)
            def _(b):
                hot = disp12[mb, b]
                part_ref[0, mb, b] += tdot(jnp.concatenate([hot] * 3, axis=0), z12[mb, b])
                part_ref[1, mb, b] += tdot(hot, p12[mb, b])
                dg_ref[b, pl.ds(mb * TOPK, TOPK), :] += by_slot(mb, b, hot, dc12[mb, b])

    for l in range(NEXP):
        for store in stores(l):
            store.wait()


def run_experts(xg, dyg, rt, w_gate, w_up, w_down):
    _, _, tok, dim = xg.shape
    ff = w_gate.shape[2]
    vmem, hbm = pl.BlockSpec(memory_space=pltpu.VMEM), pl.BlockSpec(memory_space=pl.ANY)
    half = NBLK * SLAB
    one, two = NEXP * SLAB, 2 * NEXP * SLAB
    return pl.pallas_call(
        expert_kernel,
        out_shape=(
            jax.ShapeDtypeStruct((2, 2, NBLK, tok, dim), F32),
            jax.ShapeDtypeStruct((NBLK, 2 * TOPK, tok), F32),
            jax.ShapeDtypeStruct(w_gate.shape, F32),
            jax.ShapeDtypeStruct(w_up.shape, F32),
            jax.ShapeDtypeStruct(w_down.shape, F32),
        ),
        in_specs=[vmem] * 3 + [hbm] * 3,
        out_specs=(vmem, vmem, hbm, hbm, hbm),
        scratch_shapes=[
            pltpu.VMEM((NEXP, dim, 2 * ff), BF),
            pltpu.VMEM((NEXP, ff, dim), BF),
            pltpu.VMEM((NEXP, dim, 2 * ff), F32),
            pltpu.VMEM((NEXP, ff, dim), F32),
            pltpu.VMEM((2, NEXP, NBLK, tok), F32),
            pltpu.VMEM((2, NEXP, NBLK, tok), F32),
            pltpu.VMEM((2, NBLK, one, tok), BF),
            pltpu.VMEM((2, NBLK, two, tok), BF),
            pltpu.VMEM((3, NEXP, 2, half, dim), BF),
            pltpu.VMEM((3, NEXP, 2, half, dim), BF),
            pltpu.VMEM((3, NEXP, 2, half, dim), BF),
            pltpu.VMEM((3, NEXP, 2, half, 1), F32),
            pltpu.VMEM((2, NBLK, 3 * one, dim), BF),
            pltpu.VMEM((2, NBLK, 3 * two, dim), BF),
            pltpu.VMEM((2, NBLK, one, dim), BF),
            pltpu.VMEM((2, NBLK, two, dim), BF),
            pltpu.VMEM((2, NBLK, one, 1), F32),
            pltpu.VMEM((2, NBLK, two, 1), F32),
            pltpu.SMEM((2 * NEXP,), jnp.int32),
            pltpu.SemaphoreType.DMA((NEXP, 3)),
            pltpu.SemaphoreType.DMA((NEXP, 3)),
        ],
        compiler_params=pltpu.CompilerParams(vmem_limit_bytes=40 << 20),
        name="experts",
    )(xg, dyg, rt, w_gate, w_up, w_down)


def combine_kernel(part_ref, dg_ref, y_ref, dx_ref, gg_ref, near, chip_sum, first_in, second_in, out, dg_in,
                   near_send, near_recv, first_send, first_recv, second_send, second_recv, out_send, out_recv, dg_send, dg_recv):
    enter()
    _, row, col, core = coords()
    me = number()

    def blocks(mask):
        return number(mask) - core

    def to_partner(mb, mask):
        at = pl.ds(blocks(mask), 2)
        i = mask // 2
        return remote(part_ref.at[1 - core, mb, at], near.at[mb, i], near_send.at[mb, i], near_recv.at[mb, i], 1)

    def add_chip(mb, mask):
        to_partner(mb, mask).wait_recv()
        i = mask // 2
        chip_sum[mb, i] = part_ref[core, mb, pl.ds(blocks(mask), 2)] + near[mb, i]

    FIRST, SECOND = (2, 4), (4, 2)

    def first(mb, which):
        mask = (6, FIRST[mb])[which]
        return remote(chip_sum.at[mb, mask // 2], first_in.at[mb, which], first_send.at[mb, which], first_recv.at[mb, which], FIRST[mb])

    def second(mb, h):
        return remote(chip_sum.at[mb, SECOND[mb] // 2, h], second_in.at[mb, h], second_send.at[mb, h], second_recv.at[mb, h], SECOND[mb])

    def dg_copy(mask):
        return remote(dg_ref.at[number(mask)], dg_in.at[me], dg_send.at[mask], dg_recv.at[mask], mask)

    for which in range(4):
        for mb in range(2):
            to_partner(mb, (6, FIRST[mb], SECOND[mb], 0)[which]).start()
    for mask in range(1, NBLK):
        dg_copy(mask).start()
    for which in range(2):
        for mb in range(2):
            add_chip(mb, (6, FIRST[mb])[which])
            first(mb, which).start()
    for mb in range(2):
        add_chip(mb, SECOND[mb])
    for mb in range(2):
        first(mb, 0).wait_recv()
        for h in range(2):
            chip_sum[mb, SECOND[mb] // 2, h] += first_in[mb, 0, h]
            second(mb, h).start()
    dg_in[me] = dg_ref[me]
    for mb in range(2):
        add_chip(mb, 0)
    for mask in range(1, NBLK):
        dg_copy(mask).wait()
    grads = jnp.sum(dg_in[...], axis=0)
    for mb in range(2):
        gg_ref[mb] = grads[mb * TOPK : (mb + 1) * TOPK]
    for mb in range(2):
        first(mb, 1).wait_recv()
        chip_sum[mb, 0] += first_in[mb, 1]

    def handover(mb):
        return remote(out.at[2, mb], out.at[core, mb], out_send.at[mb], out_recv.at[mb], 1)

    for h in range(2):
        for mb in range(2):
            second(mb, h).wait_recv()
            done = (chip_sum[mb, 0, h] + second_in[mb, h]).astype(BF)

            @pl.when(core == h)
            def _():
                out[core, mb] = done

            @pl.when(core != h)
            def _():
                out[2, mb] = done
    for mb in range(2):
        handover(mb).start()
    for mb in range(2):
        handover(mb).wait()
    y_ref[...] = out[0]
    dx_ref[...] = out[1]
    for mb in range(2):
        for i in range(4):
            to_partner(mb, 2 * i).wait_send()
        for i in range(2):
            first(mb, i).wait_send()
            second(mb, i).wait_send()


def combine(part, dg):
    _, _, _, tok, dim = part.shape
    vmem = pl.BlockSpec(memory_space=pltpu.VMEM)
    sem = pltpu.SemaphoreType.DMA
    return pl.pallas_call(
        combine_kernel,
        out_shape=(
            jax.ShapeDtypeStruct((2, tok, dim), BF),
            jax.ShapeDtypeStruct((2, tok, dim), BF),
            jax.ShapeDtypeStruct((2, TOPK, tok), F32),
        ),
        in_specs=[vmem] * 2,
        out_specs=(vmem,) * 3,
        scratch_shapes=[
            pltpu.VMEM((2, 4, 2, tok, dim), F32),
            pltpu.VMEM((2, 4, 2, tok, dim), F32),
            pltpu.VMEM((2, 2, 2, tok, dim), F32),
            pltpu.VMEM((2, 2, tok, dim), F32),
            pltpu.VMEM((3, 2, tok, dim), BF),
            pltpu.VMEM((NBLK, 2 * TOPK, tok), F32),
            sem((2, 4)), sem((2, 4)), sem((2, 2)), sem((2, 2)), sem((2, 2)), sem((2, 2)), sem((2,)), sem((2,)), sem((NBLK,)), sem((NBLK,)),
        ],
        compiler_params=pltpu.CompilerParams(collective_id=1, has_side_effects=True, vmem_limit_bytes=16 << 20),
        name="combine_tokens",
    )(part, dg)


def solution(mesh):
    tok_spec = P(None, ALL_AXES, None)
    w_spec = P(ALL_AXES, None, None)

    def moe_layer(x, route_idx, gates, w_gate, w_up, w_down, grad_y):
        stay = lambda arr: pltpu.with_memory_space_constraint(arr, pltpu.HBM)
        x, grad_y, w_gate, w_up, w_down = (stay(arr) for arr in (x, grad_y, w_gate, w_up, w_down))
        flat = lambda arr: jnp.transpose(arr, (0, 2, 1))
        xg, dyg, rt = gather_all(x, grad_y, stay(flat(route_idx)), stay(flat(gates)))
        part, dg, g_gate, g_up, g_down = run_experts(xg, dyg, rt, w_gate, w_up, w_down)
        y, dx, g_gates = combine(part, dg)
        return y, dx, flat(g_gates), g_gate, g_up, g_down

    return jax.shard_map(moe_layer, mesh=mesh, in_specs=(tok_spec, tok_spec, tok_spec, w_spec, w_spec, w_spec, tok_spec), out_specs=(tok_spec, tok_spec, tok_spec, w_spec, w_spec, w_spec), check_vma=False)
```

```python
import functools

import jax
import jax.numpy as jnp
from jax import lax
from jax.experimental import pallas as pl
from jax.experimental.pallas import tpu as pltpu
from jax.sharding import PartitionSpec as P

ALL_AXES = ("rep", "row", "col", "core")
MESH = pl.DeviceIdType.MESH
BF = jnp.bfloat16
F32 = jnp.float32
NBLK = 8
QUAD = 4
NEXP = 4
TOPK = 4
NEAR, FAR = 0, 1
Y, DX = 0, 1


def coords():
    return (lax.axis_index("rep"), lax.axis_index("row"), lax.axis_index("col"), lax.axis_index("core"))


def peer(mask):
    rep, row, col, core = coords()
    flip = lambda pos, bit: 1 - pos if mask & bit else pos
    return (rep, flip(row, 4), flip(col, 2), flip(core, 1))


def number(mask=0):
    _, row, col, core = peer(mask)
    return row * 4 + col * 2 + core


def quad(mask=0):
    _, _, col, core = peer(mask)
    return col * 2 + core


def enter():
    barrier = pltpu.get_barrier_semaphore()
    for mask in range(1, NBLK):
        pl.semaphore_signal(barrier, inc=1, device_id=peer(mask), device_id_type=MESH)
    pl.semaphore_wait(barrier, NBLK - 1)


def remote(src, dst, send_sem, recv_sem, mask):
    return pltpu.make_async_remote_copy(src_ref=src, dst_ref=dst, send_sem=send_sem, recv_sem=recv_sem, device_id=peer(mask), device_id_type=MESH)


def tdot(lhs, rhs):
    return lax.dot_general(lhs, rhs, (((0,), (0,)), ((), ())), preferred_element_type=F32)


def ndot(lhs, rhs):
    return lax.dot_general(lhs, rhs, (((1,), (1,)), ((), ())), preferred_element_type=F32)


def dot(lhs, rhs):
    return jnp.dot(lhs, rhs, preferred_element_type=F32)


def layer_kernel(x_hbm, dy_hbm, route_hbm, gate_hbm, wg_hbm, wu_hbm, wd_hbm,
                 y_ref, dx_ref, gates_ref, gg_ref, gu_ref, gd_ref,
                 xg, dyg, rt, route_tab, gate_tab, mine, wgu, wd, rank, grow, disp, gblk, gcol, xr, qr, uv, hid, outs, zbuf, pbuf, dg,
                 part, near_in, chip_sum, first_in, second_in, dg_in,
                 tab_sem, own_sem, w_sem, g_send, g_recv, rt_send, rt_recv, d_send, d_recv, f_send, f_recv, s_send, s_recv, dg_send, dg_recv):
    tok, dim = xg.shape[2], xg.shape[3]
    ff = wd.shape[1]
    cap = tok // 2
    half = tok // 2
    _, row, col, core = coords()
    me, at_x, at_y, at_d = number(0), number(2), number(4), number(6)
    tokens = (xg, dyg)
    PART = 6

    tables = [pltpu.make_async_copy(src, dst, tab_sem.at[i]) for i, (src, dst) in enumerate(((route_hbm, route_tab), (gate_hbm, gate_tab)))]
    own = [[pltpu.make_async_copy(src.at[mb], dst.at[mb, me], own_sem.at[mb, i]) for i, (src, dst) in enumerate(((x_hbm, xg), (dy_hbm, dyg)))] for mb in range(2)]
    weights = []
    for l in range(NEXP):
        weights += [
            pltpu.make_async_copy(wg_hbm.at[l], wgu.at[l, :, pl.ds(0, ff)], w_sem.at[l, 0]),
            pltpu.make_async_copy(wu_hbm.at[l], wgu.at[l, :, pl.ds(ff, ff)], w_sem.at[l, 1]),
            pltpu.make_async_copy(wd_hbm.at[l], wd.at[l], w_sem.at[l, 2]),
        ]
    for load in own[0] + tables + own[1] + weights:
        load.start()
    for load in tables:
        load.wait()
    for mb in range(2):
        mine[pl.ds(mb * 8, TOPK), :] = route_tab[mb].astype(F32)
        mine[pl.ds(mb * 8 + TOPK, TOPK), :] = gate_tab[mb]
    rt[me] = mine[...]
    enter()

    def tok_copy(mb, kind):
        if kind < PART:
            which, slot, mask = ((0, me, 2), (1, me, 2), (1, at_y, 2), (0, me, 4), (1, me, 4), (0, at_x, 4))[kind]
        else:
            which, slot, mask = (kind - PART) % 2, (me, at_x, at_y, at_d)[(kind - PART) // 2], 1
        ref = tokens[which].at[mb, slot]
        return remote(ref, ref, g_send.at[mb, kind], g_recv.at[mb, kind], mask)

    def send_own(mb, which):
        own[mb][which].wait()
        for kind in (which, 3 + which, PART + which):
            tok_copy(mb, kind).start()

    def relay(mb, kind, *then):
        tok_copy(mb, kind).wait_recv()
        for nxt in then:
            tok_copy(mb, nxt).start()

    def rt_copy(mask):
        return remote(mine, rt.at[me], rt_send.at[mask], rt_recv.at[mask], mask)

    FIRST, SECOND = (2, 4), (4, 2)

    def to_partner(q, mb, mask):
        r, i = q * 2 + mb, mask // 2
        src = part.at[r, FAR if mask & 4 else NEAR, quad(mask | 1)]
        return remote(src, near_in.at[r, i], d_send.at[r, i], d_recv.at[r, i], 1)

    def partner_start(q, mb, far):
        for mask in ((6, 4) if far else (2, 0)):
            to_partner(q, mb, mask).start()

    def chip_add(q, mb, mask):
        r, i = q * 2 + mb, mask // 2
        to_partner(q, mb, mask).wait_recv()
        chip_sum[r, i] = part[r, FAR if mask & 4 else NEAR, quad(mask)] + near_in[r, i]

    def first(q, mb, h, which):
        r, mask = q * 2 + mb, (6, FIRST[h])[which]
        src = chip_sum.at[r, mask // 2, pl.ds(h * half, half)]
        return remote(src, first_in.at[r, h, which], f_send.at[r, h, which], f_recv.at[r, h, which], FIRST[h])

    def second(q, mb, h):
        r = q * 2 + mb
        src = chip_sum.at[r, SECOND[h] // 2, pl.ds(h * half, half)]
        return remote(src, second_in.at[r, h], s_send.at[r, h], s_recv.at[r, h], SECOND[h])

    def far_send(q, mb):
        chip_add(q, mb, 6)
        first(q, mb, 0, 0).start()
        first(q, mb, 1, 0).start()
        chip_add(q, mb, 4)
        first(q, mb, 1, 1).start()

    def near_send(q, mb):
        chip_add(q, mb, 2)
        first(q, mb, 0, 1).start()
        chip_add(q, mb, 0)

    def second_send(q, mb):
        for h in range(2):
            first(q, mb, h, 0).wait_recv()
            chip_sum[q * 2 + mb, SECOND[h] // 2, pl.ds(h * half, half), :] += first_in[q * 2 + mb, h, 0]
            second(q, mb, h).start()

    def finish(q, mb):
        r = q * 2 + mb
        for h in range(2):
            first(q, mb, h, 1).wait_recv()
            second(q, mb, h).wait_recv()
            rows = pl.ds(h * half, half)
            (y_ref, dx_ref)[q][mb, rows, :] = (chip_sum[r, 0, rows, :] + first_in[r, h, 1] + second_in[r, h]).astype(BF)

    first_id = (me * NEXP).astype(F32)
    slot_iota = lax.broadcasted_iota(jnp.int32, (cap, tok), 0).astype(F32)

    def block_of(far, b):
        return (1 - row if far else row) * QUAD + b

    def make_ranks():
        members = []
        for mb in range(2):
            routes, gates = rt[:, mb * 8 : mb * 8 + 4, :], rt[:, mb * 8 + 4 : mb * 8 + 8, :]
            for l in range(NEXP):
                hit = routes == first_id + l
                members.append(jnp.sum(jnp.where(hit, 1.0, 0.0), axis=1))
                grow[mb, l] = jnp.sum(jnp.where(hit, gates, 0.0), axis=1)
        member = jnp.concatenate(members, axis=0)
        before = lax.broadcasted_iota(jnp.int32, (tok, tok), 0) < lax.broadcasted_iota(jnp.int32, (tok, tok), 1)
        ranks = jnp.where(member > 0, dot(member.astype(BF), jnp.where(before, 1.0, 0.0).astype(BF)), -1.0)
        for mb in range(2):
            for l in range(NEXP):
                rank[mb, l] = ranks[(mb * NEXP + l) * NBLK : (mb * NEXP + l + 1) * NBLK]

    def per_block(body):
        @pl.loop(0, QUAD)
        def _(b):
            body(b)

    def dispatch_x(mb, far):
        u = mb * 2 + far

        def body(b):
            blk = block_of(far, b)
            hot = jnp.concatenate([jnp.where(rank[mb, l, pl.ds(blk, 1), :] == slot_iota, 1.0, 0.0) for l in range(NEXP)], axis=0)
            gs = jnp.concatenate([jnp.broadcast_to(grow[mb, l, pl.ds(blk, 1), :], (cap, tok)) for l in range(NEXP)], axis=0)
            gate = jnp.sum(hot * gs, axis=1, keepdims=True)
            hot = hot.astype(BF)
            disp[u, b] = hot
            gblk[u, b] = gate
            xs = dot(hot, xg[mb, blk]).astype(BF)
            rows = pl.ds(pl.multiple_of(b * cap, cap), cap)
            for l in range(NEXP):
                xr[l, u, rows, :] = xs[l * cap : (l + 1) * cap]
                gcol[l, u, rows, :] = gate[l * cap : (l + 1) * cap]

        per_block(body)

    def forward(mb, far):
        u = mb * 2 + far

        @pl.loop(0, NEXP)
        def _(l):
            both = dot(xr[l, u], wgu[l]).astype(BF)
            uv[l, u] = both
            both = both.astype(F32)
            gate_pre, up_pre = both[:, :ff], both[:, ff:]
            hidden = (gate_pre * jax.nn.sigmoid(gate_pre) * up_pre).astype(BF)
            hid[l, u] = hidden
            out = dot(hidden, wd[l]).astype(BF)
            outs[l, u] = out
            z = gcol[l, u] * out.astype(F32)
            hi = z.astype(BF)
            rest = z - hi.astype(F32)
            mid = rest.astype(BF)
            low = (rest - mid.astype(F32)).astype(BF)
            at = pl.multiple_of(l * cap, cap)
            for b in range(QUAD):
                for i, piece in enumerate((hi, mid, low)):
                    zbuf[b, pl.ds(i * NEXP * cap + at, cap), :] = piece[b * cap : (b + 1) * cap]

        def body(b):
            part[Y * 2 + mb, far, b] = tdot(jnp.concatenate([disp[u, b]] * 3, axis=0), zbuf[b])

        per_block(body)

    def dispatch_dy(mb, far):
        u = mb * 2 + far

        def body(b):
            blk = block_of(far, b)
            hot = disp[u, b]
            dys = dot(hot, dyg[mb, blk])
            qs = (gblk[u, b] * dys).astype(BF)
            rows = pl.ds(pl.multiple_of(b * cap, cap), cap)
            hot_f = hot.astype(F32)
            routes = rt[blk, pl.ds(mb * 8, TOPK), :]
            total = jnp.zeros((TOPK, tok), F32)
            for l in range(NEXP):
                cut = slice(l * cap, (l + 1) * cap)
                qr[l, u, rows, :] = qs[cut]
                dots = jnp.sum(dys[cut] * outs[l, u, rows, :].astype(F32), axis=1, keepdims=True)
                line = jnp.sum(hot_f[cut] * dots, axis=0, keepdims=True)
                total = total + jnp.where(routes == first_id + l, line, 0.0)
            dg[blk, pl.ds(mb * TOPK, TOPK), :] = total

        per_block(body)

    def backward(mb, far):
        u = mb * 2 + far

        @pl.loop(0, NEXP)
        def _(l):
            both = uv[l, u].astype(F32)
            gate_pre, up_pre = both[:, :ff], both[:, ff:]
            sig = jax.nn.sigmoid(gate_pre)
            back = ndot(qr[l, u], wd[l])
            d_up = (back * gate_pre * sig).astype(BF)
            d_gate = (back * up_pre * sig * (1.0 + gate_pre * (1.0 - sig))).astype(BF)
            d_both = jnp.concatenate([d_gate, d_up], axis=1)
            uv[l, u] = d_both
            d_in = ndot(d_both, wgu[l]).astype(BF)
            at = pl.multiple_of(l * cap, cap)
            for b in range(QUAD):
                pbuf[b, pl.ds(at, cap), :] = d_in[b * cap : (b + 1) * cap]

        def body(b):
            part[DX * 2 + mb, far, b] = tdot(disp[u, b], pbuf[b])

        per_block(body)

    def weight_grads(l):
        rows = 2 * 2 * QUAD * cap
        gd_ref[l] = tdot(hid[l].reshape(rows, ff), qr[l].reshape(rows, dim))
        xs, d_both = xr[l].reshape(rows, dim), uv[l].reshape(rows, 2 * ff)
        gg_ref[l] = tdot(xs, d_both[:, :ff])
        gu_ref[l] = tdot(xs, d_both[:, ff:])

    send_own(0, 0)
    for mask in range(1, NBLK):
        rt_copy(mask).start()
    send_own(0, 1)
    for mask in range(1, NBLK):
        rt_copy(mask).wait_recv()
    make_ranks()
    for load in weights:
        load.wait()
    relay(0, 0, 5, 8)
    relay(0, 3, 10)
    send_own(1, 0)
    relay(0, 6)
    relay(0, 8)
    dispatch_x(0, NEAR)
    relay(0, 1, 9)
    relay(0, 4, 2, 11)
    forward(0, NEAR)
    partner_start(Y, 0, NEAR)

    relay(0, 5, 12)
    relay(0, 10)
    send_own(1, 1)
    relay(1, 0, 5, 8)
    relay(1, 3, 10)
    near_send(Y, 0)
    relay(0, 12)
    dispatch_x(0, FAR)
    forward(0, FAR)
    partner_start(Y, 0, FAR)

    relay(0, 2, 13)
    relay(1, 5, 12)
    relay(1, 1, 9)
    relay(1, 4, 2, 11)
    for kind in (6, 8, 10, 12):
        relay(1, kind)
    dispatch_x(1, FAR)
    far_send(Y, 0)
    forward(1, FAR)
    partner_start(Y, 1, FAR)

    relay(1, 2, 13)
    dispatch_x(1, NEAR)
    far_send(Y, 1)
    forward(1, NEAR)
    partner_start(Y, 1, NEAR)

    second_send(Y, 0)
    for kind in (7, 9, 11, 13):
        relay(0, kind)
    dispatch_dy(0, FAR)
    near_send(Y, 1)
    backward(0, FAR)
    partner_start(DX, 0, FAR)

    second_send(Y, 1)
    dispatch_dy(0, NEAR)
    far_send(DX, 0)
    backward(0, NEAR)
    partner_start(DX, 0, NEAR)

    finish(Y, 0)
    for kind in (7, 9, 11, 13):
        relay(1, kind)
    dispatch_dy(1, FAR)
    near_send(DX, 0)
    backward(1, FAR)
    partner_start(DX, 1, FAR)

    finish(Y, 1)
    dispatch_dy(1, NEAR)
    far_send(DX, 1)
    second_send(DX, 0)
    backward(1, NEAR)
    partner_start(DX, 1, NEAR)

    def dg_copy(mask):
        return remote(dg.at[number(mask)], dg_in.at[me], dg_send.at[mask], dg_recv.at[mask], mask)

    for mask in range(1, NBLK):
        dg_copy(mask).start()
    dg_in[me] = dg[me]
    weight_grads(0)
    near_send(DX, 1)
    second_send(DX, 1)
    weight_grads(1)
    finish(DX, 0)
    weight_grads(2)
    weight_grads(3)
    for mask in range(1, NBLK):
        dg_copy(mask).wait()
    grads = jnp.sum(dg_in[...], axis=0)
    for mb in range(2):
        gates_ref[mb] = grads[mb * TOPK : (mb + 1) * TOPK]
    finish(DX, 1)
    for mask in range(1, NBLK):
        rt_copy(mask).wait_send()
    for mb in range(2):
        for kind in range(14):
            tok_copy(mb, kind).wait_send()
        for q in (Y, DX):
            for mask in (0, 2, 4, 6):
                to_partner(q, mb, mask).wait_send()
            for h in range(2):
                second(q, mb, h).wait_send()
                for which in range(2):
                    first(q, mb, h, which).wait_send()


def layer(x, grad_y, route_rows, gate_rows, w_gate, w_up, w_down):
    _, tok, dim = x.shape
    ff = w_gate.shape[2]
    cap = tok // 2
    hbm, vmem = pl.BlockSpec(memory_space=pltpu.HBM), pl.BlockSpec(memory_space=pltpu.VMEM)
    dma = pltpu.SemaphoreType.DMA
    unit = QUAD * cap
    shape = jax.ShapeDtypeStruct
    return pl.pallas_call(
        layer_kernel,
        out_shape=(
            shape((2, tok, dim), BF), shape((2, tok, dim), BF), shape((2, TOPK, tok), F32),
            shape(w_gate.shape, F32), shape(w_up.shape, F32), shape(w_down.shape, F32),
        ),
        in_specs=[hbm] * 7,
        out_specs=(vmem,) * 6,
        scratch_shapes=[
            pltpu.VMEM((2, NBLK, tok, dim), BF),
            pltpu.VMEM((2, NBLK, tok, dim), BF),
            pltpu.VMEM((NBLK, 16, tok), F32),
            pltpu.VMEM((2, TOPK, tok), jnp.int32),
            pltpu.VMEM((2, TOPK, tok), F32),
            pltpu.VMEM((16, tok), F32),
            pltpu.VMEM((NEXP, dim, 2 * ff), BF),
            pltpu.VMEM((NEXP, ff, dim), BF),
            pltpu.VMEM((2, NEXP, NBLK, tok), F32),
            pltpu.VMEM((2, NEXP, NBLK, tok), F32),
            pltpu.VMEM((4, QUAD, NEXP * cap, tok), BF),
            pltpu.VMEM((4, QUAD, NEXP * cap, 1), F32),
            pltpu.VMEM((NEXP, 4, unit, 1), F32),
            pltpu.VMEM((NEXP, 4, unit, dim), BF),
            pltpu.VMEM((NEXP, 4, unit, dim), BF),
            pltpu.VMEM((NEXP, 4, unit, 2 * ff), BF),
            pltpu.VMEM((NEXP, 4, unit, ff), BF),
            pltpu.VMEM((NEXP, 4, unit, dim), BF),
            pltpu.VMEM((QUAD, 3 * NEXP * cap, dim), BF),
            pltpu.VMEM((QUAD, NEXP * cap, dim), BF),
            pltpu.VMEM((NBLK, 2 * TOPK, tok), F32),
            pltpu.VMEM((4, 2, QUAD, tok, dim), F32),
            pltpu.VMEM((4, 4, tok, dim), F32),
            pltpu.VMEM((4, 4, tok, dim), F32),
            pltpu.VMEM((4, 2, 2, tok // 2, dim), F32),
            pltpu.VMEM((4, 2, tok // 2, dim), F32),
            pltpu.VMEM((NBLK, 2 * TOPK, tok), F32),
            dma((2,)), dma((2, 2)), dma((NEXP, 3)), dma((2, 14)), dma((2, 14)), dma((NBLK,)), dma((NBLK,)),
            dma((4, 4)), dma((4, 4)), dma((4, 2, 2)), dma((4, 2, 2)), dma((4, 2)), dma((4, 2)), dma((NBLK,)), dma((NBLK,)),
        ],
        compiler_params=pltpu.CompilerParams(collective_id=0, has_side_effects=True, vmem_limit_bytes=46 << 20),
        name="moe_layer",
    )(x, grad_y, route_rows, gate_rows, w_gate, w_up, w_down)


def flush_kernel(*refs):
    count = (len(refs) - 1) // 2
    sem = refs[-1]
    copies = [pltpu.make_async_copy(refs[i], refs[count + i], sem.at[i]) for i in range(count)]
    for copy in copies:
        copy.start()
    for copy in copies:
        copy.wait()


def flush(arrays):
    hbm, vmem = pl.BlockSpec(memory_space=pltpu.HBM), pl.BlockSpec(memory_space=pltpu.VMEM)
    return pl.pallas_call(
        flush_kernel,
        out_shape=tuple(jax.ShapeDtypeStruct(arr.shape, arr.dtype) for arr in arrays),
        in_specs=[vmem] * len(arrays),
        out_specs=(hbm,) * len(arrays),
        scratch_shapes=[pltpu.SemaphoreType.DMA((len(arrays),))],
        compiler_params=pltpu.CompilerParams(vmem_limit_bytes=12 << 20),
        name="write_out",
    )(*arrays)


def solution(mesh):
    tok_spec = P(None, ALL_AXES, None)
    w_spec = P(ALL_AXES, None, None)

    def moe_layer(x, route_idx, gates, w_gate, w_up, w_down, grad_y):
        stay = lambda arr: pltpu.with_memory_space_constraint(arr, pltpu.HBM)
        flat = lambda arr: jnp.transpose(arr, (0, 2, 1))
        args = [stay(arr) for arr in (x, grad_y, flat(route_idx), flat(gates), w_gate, w_up, w_down)]
        y, dx, g_gates, g_gate, g_up, g_down = flush(layer(*args))
        return y, dx, flat(g_gates), g_gate, g_up, g_down

    return jax.shard_map(moe_layer, mesh=mesh, in_specs=(tok_spec, tok_spec, tok_spec, w_spec, w_spec, w_spec, tok_spec), out_specs=(tok_spec, tok_spec, tok_spec, w_spec, w_spec, w_spec), check_vma=False)
```

```python
import functools

import jax
import jax.numpy as jnp
from jax import lax
from jax.experimental import pallas as pl
from jax.experimental.pallas import tpu as pltpu
from jax.sharding import PartitionSpec as P

ALL_AXES = ("rep", "row", "col", "core")
MESH = pl.DeviceIdType.MESH
BF = jnp.bfloat16
F32 = jnp.float32
NBLK = 8
QUAD = 4
NEXP = 4
TOPK = 4
LANES = 128
NEAR, FAR = 0, 1
Y, DX = 0, 1


def coords():
    return (lax.axis_index("rep"), lax.axis_index("row"), lax.axis_index("col"), lax.axis_index("core"))


def peer(mask):
    rep, row, col, core = coords()
    flip = lambda pos, bit: 1 - pos if mask & bit else pos
    return (rep, flip(row, 4), flip(col, 2), flip(core, 1))


def number(mask=0):
    _, row, col, core = peer(mask)
    return row * 4 + col * 2 + core


def quad(mask=0):
    _, _, col, core = peer(mask)
    return col * 2 + core


def announce():
    barrier = pltpu.get_barrier_semaphore()
    for mask in range(1, NBLK):
        pl.semaphore_signal(barrier, inc=1, device_id=peer(mask), device_id_type=MESH)


def all_entered():
    pl.semaphore_wait(pltpu.get_barrier_semaphore(), NBLK - 1)


def remote(src, dst, send_sem, recv_sem, mask):
    return pltpu.make_async_remote_copy(src_ref=src, dst_ref=dst, send_sem=send_sem, recv_sem=recv_sem, device_id=peer(mask), device_id_type=MESH)


def tdot(lhs, rhs):
    return lax.dot_general(lhs, rhs, (((0,), (0,)), ((), ())), preferred_element_type=F32)


def ndot(lhs, rhs):
    return lax.dot_general(lhs, rhs, (((1,), (1,)), ((), ())), preferred_element_type=F32)


def dot(lhs, rhs):
    return jnp.dot(lhs, rhs, preferred_element_type=F32)


def layer_kernel(x_hbm, dy_hbm, route_hbm, gate_hbm, wg_hbm, wu_hbm, wd_hbm,
                 y_ref, dx_ref, gates_ref, gg_ref, gu_ref, gd_ref,
                 xg, dyg, rt, route_tab, gate_tab, mine, wgu, wd, rank, grow, disp, gblk, gcol, xr, qr, uv, hid, outs, zbuf, pbuf, dg,
                 part, near_in, chip_sum, first_in, second_in, dg_in,
                 tab_sem, own_sem, w_sem, g_send, g_recv, rt_send, rt_recv, d_send, d_recv, f_send, f_recv, s_send, s_recv, dg_send, dg_recv):
    tok, dim = xg.shape[2], xg.shape[3]
    ff = wd.shape[1]
    cap = tok // 2
    half = tok // 2
    _, row, col, core = coords()
    me, at_x, at_y, at_d = number(0), number(2), number(4), number(6)
    tokens = (xg, dyg)
    PART = 6

    announce()
    tables = [pltpu.make_async_copy(src, dst, tab_sem.at[i]) for i, (src, dst) in enumerate(((route_hbm, route_tab), (gate_hbm, gate_tab)))]
    own = [[pltpu.make_async_copy(src.at[mb], dst.at[mb, me], own_sem.at[mb, i]) for i, (src, dst) in enumerate(((x_hbm, xg), (dy_hbm, dyg)))] for mb in range(2)]
    weights = []
    for l in range(NEXP):
        weights += [
            pltpu.make_async_copy(wg_hbm.at[l], wgu.at[l, :, pl.ds(0, ff)], w_sem.at[l, 0]),
            pltpu.make_async_copy(wu_hbm.at[l], wgu.at[l, :, pl.ds(ff, ff)], w_sem.at[l, 1]),
            pltpu.make_async_copy(wd_hbm.at[l], wd.at[l], w_sem.at[l, 2]),
        ]
    for load in tables + own[0] + own[1] + weights:
        load.start()
    for load in tables:
        load.wait()
    for mb in range(2):
        mine[mb] = jnp.zeros(mine.shape[1:], F32)
        mine[mb, pl.ds(0, TOPK), pl.ds(0, tok)] = route_tab[mb].astype(F32)
        mine[mb, pl.ds(TOPK, TOPK), pl.ds(0, tok)] = gate_tab[mb]
        rt[mb, me] = mine[mb]
    all_entered()

    def tok_copy(mb, kind):
        if kind < PART:
            which, slot, mask = ((0, me, 2), (1, me, 2), (1, at_y, 2), (0, me, 4), (1, me, 4), (0, at_x, 4))[kind]
        else:
            which, slot, mask = (kind - PART) % 2, (me, at_x, at_y, at_d)[(kind - PART) // 2], 1
        ref = tokens[which].at[mb, slot]
        return remote(ref, ref, g_send.at[mb, kind], g_recv.at[mb, kind], mask)

    def send_own(mb, *kinds):
        for kind in kinds:
            tok_copy(mb, kind).start()

    def relay(mb, kind, *then):
        tok_copy(mb, kind).wait_recv()
        for nxt in then:
            tok_copy(mb, nxt).start()

    def rt_copy(mb, mask):
        return remote(mine.at[mb], rt.at[mb, me], rt_send.at[mb, mask], rt_recv.at[mb, mask], mask)

    def send_tables(mb):
        for mask in (2, 4, 6, 3, 5, 7, 1):
            rt_copy(mb, mask).start()

    def await_tables(mb):
        for mask in range(1, NBLK):
            rt_copy(mb, mask).wait_recv()

    FIRST, SECOND = (2, 4), (4, 2)

    def to_partner(q, mb, mask):
        r, i = q * 2 + mb, mask // 2
        src = part.at[r, FAR if mask & 4 else NEAR, quad(mask | 1)]
        return remote(src, near_in.at[r, i], d_send.at[r, i], d_recv.at[r, i], 1)

    def partner_start(q, mb, far):
        for mask in ((6, 4) if far else (2, 0)):
            to_partner(q, mb, mask).start()

    def chip_add(q, mb, mask):
        r, i = q * 2 + mb, mask // 2
        to_partner(q, mb, mask).wait_recv()
        chip_sum[r, i] = part[r, FAR if mask & 4 else NEAR, quad(mask)] + near_in[r, i]

    def first(q, mb, h, which):
        r, mask = q * 2 + mb, (6, FIRST[h])[which]
        src = chip_sum.at[r, mask // 2, pl.ds(h * half, half)]
        return remote(src, first_in.at[r, h, which], f_send.at[r, h, which], f_recv.at[r, h, which], FIRST[h])

    def second(q, mb, h):
        r = q * 2 + mb
        src = chip_sum.at[r, SECOND[h] // 2, pl.ds(h * half, half)]
        return remote(src, second_in.at[r, h], s_send.at[r, h], s_recv.at[r, h], SECOND[h])

    def far_send(q, mb):
        chip_add(q, mb, 6)
        first(q, mb, 0, 0).start()
        first(q, mb, 1, 0).start()
        chip_add(q, mb, 4)
        first(q, mb, 1, 1).start()

    def near_send(q, mb):
        chip_add(q, mb, 2)
        first(q, mb, 0, 1).start()
        chip_add(q, mb, 0)

    def second_send(q, mb):
        for h in range(2):
            first(q, mb, h, 0).wait_recv()
            chip_sum[q * 2 + mb, SECOND[h] // 2, pl.ds(h * half, half), :] += first_in[q * 2 + mb, h, 0]
            second(q, mb, h).start()

    def finish(q, mb):
        r = q * 2 + mb
        for h in range(2):
            first(q, mb, h, 1).wait_recv()
            second(q, mb, h).wait_recv()
            rows = pl.ds(h * half, half)
            (y_ref, dx_ref)[q][mb, rows, :] = (chip_sum[r, 0, rows, :] + first_in[r, h, 1] + second_in[r, h]).astype(BF)

    first_id = (me * NEXP).astype(F32)
    slot_iota = lax.broadcasted_iota(jnp.int32, (cap, tok), 0).astype(F32)

    def block_of(far, b):
        return (1 - row if far else row) * QUAD + b

    before = lax.broadcasted_iota(jnp.int32, (tok, tok), 0) < lax.broadcasted_iota(jnp.int32, (tok, tok), 1)

    def make_ranks(mb):
        routes, gates = rt[mb, :, 0:TOPK, 0:tok], rt[mb, :, TOPK : 2 * TOPK, 0:tok]
        members = []
        for l in range(NEXP):
            hit = routes == first_id + l
            members.append(jnp.sum(jnp.where(hit, 1.0, 0.0), axis=1))
            grow[mb, l] = jnp.sum(jnp.where(hit, gates, 0.0), axis=1)
        member = jnp.concatenate(members, axis=0)
        ranks = jnp.where(member > 0, dot(member.astype(BF), jnp.where(before, 1.0, 0.0).astype(BF)), -1.0)
        for l in range(NEXP):
            rank[mb, l] = ranks[l * NBLK : (l + 1) * NBLK]

    def per_block(body):
        for b in range(QUAD):
            body(b)

    def dispatch_x(mb, far):
        u = mb * 2 + far

        def body(b):
            blk = block_of(far, b)
            hot = jnp.concatenate([jnp.where(rank[mb, l, pl.ds(blk, 1), :] == slot_iota, 1.0, 0.0) for l in range(NEXP)], axis=0)
            gs = jnp.concatenate([jnp.broadcast_to(grow[mb, l, pl.ds(blk, 1), :], (cap, tok)) for l in range(NEXP)], axis=0)
            gate = jnp.sum(hot * gs, axis=1, keepdims=True)
            hot = hot.astype(BF)
            disp[u, b] = hot
            gblk[u, b] = gate
            xs = dot(hot, xg[mb, blk]).astype(BF)
            rows = pl.ds(pl.multiple_of(b * cap, cap), cap)
            for l in range(NEXP):
                xr[l, u, rows, :] = xs[l * cap : (l + 1) * cap]
                gcol[l, u, rows, :] = gate[l * cap : (l + 1) * cap]

        per_block(body)

    def forward(mb, far, between=lambda: None):
        u = mb * 2 + far

        @pl.loop(0, NEXP, unroll=NEXP)
        def _(l):
            both = dot(xr[l, u], wgu[l]).astype(BF)
            uv[l, u] = both
            both = both.astype(F32)
            gate_pre, up_pre = both[:, :ff], both[:, ff:]
            hidden = (gate_pre * jax.nn.sigmoid(gate_pre) * up_pre).astype(BF)
            hid[l, u] = hidden
            out = dot(hidden, wd[l]).astype(BF)
            outs[l, u] = out
            z = gcol[l, u] * out.astype(F32)
            hi = z.astype(BF)
            rest = z - hi.astype(F32)
            mid = rest.astype(BF)
            low = (rest - mid.astype(F32)).astype(BF)
            at = pl.multiple_of(l * cap, cap)
            for b in range(QUAD):
                for i, piece in enumerate((hi, mid, low)):
                    zbuf[b, pl.ds(i * NEXP * cap + at, cap), :] = piece[b * cap : (b + 1) * cap]

        between()

        def body(b):
            part[Y * 2 + mb, far, b] = tdot(jnp.concatenate([disp[u, b]] * 3, axis=0), zbuf[b])

        per_block(body)

    def dispatch_dy(mb, far):
        u = mb * 2 + far

        def body(b):
            blk = block_of(far, b)
            hot = disp[u, b]
            dys = dot(hot, dyg[mb, blk])
            qs = (gblk[u, b] * dys).astype(BF)
            rows = pl.ds(pl.multiple_of(b * cap, cap), cap)
            hot_f = hot.astype(F32)
            routes = rt[mb, blk, 0:TOPK, 0:tok]
            total = jnp.zeros((TOPK, tok), F32)
            for l in range(NEXP):
                cut = slice(l * cap, (l + 1) * cap)
                qr[l, u, rows, :] = qs[cut]
                dots = jnp.sum(dys[cut] * outs[l, u, rows, :].astype(F32), axis=1, keepdims=True)
                line = jnp.sum(hot_f[cut] * dots, axis=0, keepdims=True)
                total = total + jnp.where(routes == first_id + l, line, 0.0)
            dg[blk, pl.ds(mb * TOPK, TOPK), pl.ds(0, tok)] = total

        per_block(body)

    def backward(mb, far, between=lambda: None):
        u = mb * 2 + far

        @pl.loop(0, NEXP, unroll=NEXP)
        def _(l):
            both = uv[l, u].astype(F32)
            gate_pre, up_pre = both[:, :ff], both[:, ff:]
            sig = jax.nn.sigmoid(gate_pre)
            back = ndot(qr[l, u], wd[l])
            d_up = (back * gate_pre * sig).astype(BF)
            d_gate = (back * up_pre * sig * (1.0 + gate_pre * (1.0 - sig))).astype(BF)
            d_both = jnp.concatenate([d_gate, d_up], axis=1)
            uv[l, u] = d_both
            d_in = ndot(d_both, wgu[l]).astype(BF)
            at = pl.multiple_of(l * cap, cap)
            for b in range(QUAD):
                pbuf[b, pl.ds(at, cap), :] = d_in[b * cap : (b + 1) * cap]

        between()

        def body(b):
            part[DX * 2 + mb, far, b] = tdot(disp[u, b], pbuf[b])

        per_block(body)

    def weight_grads(l):
        rows = 2 * 2 * QUAD * cap
        gd_ref[l] = tdot(hid[l].reshape(rows, ff), qr[l].reshape(rows, dim))
        xs, d_both = xr[l].reshape(rows, dim), uv[l].reshape(rows, 2 * ff)
        gg_ref[l] = tdot(xs, d_both[:, :ff])
        gu_ref[l] = tdot(xs, d_both[:, ff:])

    def dg_copy(mask):
        return remote(dg.at[number(mask)], dg_in.at[me], dg_send.at[mask], dg_recv.at[mask], mask)

    send_tables(0)
    own[0][0].wait()
    send_own(0, 0, 3, 6)
    own[1][0].wait()
    send_own(1, 0, 3, 6)
    send_tables(1)
    own[0][1].wait()
    send_own(0, 1, 7)
    own[1][1].wait()
    send_own(1, 1, 7)
    await_tables(0)
    make_ranks(0)
    await_tables(1)
    make_ranks(1)
    for load in weights:
        load.wait()
    relay(0, 0, 5, 8)
    relay(0, 3, 10)
    send_own(0, 4)
    relay(0, 6)
    relay(0, 8)
    dispatch_x(0, NEAR)
    relay(1, 0, 5, 8)
    relay(1, 3, 10)
    send_own(1, 4)
    forward(0, NEAR, lambda: relay(0, 1, 9))
    partner_start(Y, 0, NEAR)

    relay(1, 6)
    relay(1, 8)
    dispatch_x(1, NEAR)
    relay(0, 5, 12)
    relay(0, 10)

    def during():
        near_send(Y, 0)
        relay(1, 1, 9)

    forward(1, NEAR, during)
    partner_start(Y, 1, NEAR)

    relay(1, 5, 12)
    relay(1, 10)
    relay(0, 12)
    dispatch_x(0, FAR)
    relay(0, 4, 2, 11)

    def during():
        near_send(Y, 1)
        relay(1, 4, 2, 11)

    forward(0, FAR, during)
    partner_start(Y, 0, FAR)

    relay(1, 12)
    dispatch_x(1, FAR)
    forward(1, FAR, lambda: far_send(Y, 0))
    partner_start(Y, 1, FAR)

    relay(0, 7)
    relay(0, 9)
    dispatch_dy(0, NEAR)
    relay(0, 2, 13)

    def during():
        far_send(Y, 1)
        relay(1, 2, 13)

    backward(0, NEAR, during)
    partner_start(DX, 0, NEAR)

    second_send(Y, 0)
    relay(0, 11)
    relay(0, 13)
    dispatch_dy(0, FAR)
    backward(0, FAR, lambda: near_send(DX, 0))
    partner_start(DX, 0, FAR)

    second_send(Y, 1)
    for kind in (7, 9, 11, 13):
        relay(1, kind)
    dispatch_dy(1, FAR)
    backward(1, FAR, lambda: far_send(DX, 0))
    partner_start(DX, 1, FAR)

    finish(Y, 0)
    dispatch_dy(1, NEAR)
    for mask in range(1, NBLK):
        dg_copy(mask).start()
    dg_in[me] = dg[me]
    backward(1, NEAR, lambda: far_send(DX, 1))
    partner_start(DX, 1, NEAR)

    second_send(DX, 0)
    weight_grads(0)
    near_send(DX, 1)
    second_send(DX, 1)
    finish(Y, 1)
    weight_grads(1)
    finish(DX, 0)
    weight_grads(2)
    weight_grads(3)
    for mask in range(1, NBLK):
        dg_copy(mask).wait()
    grads = jnp.sum(dg_in[...], axis=0)
    for mb in range(2):
        gates_ref[mb] = grads[mb * TOPK : (mb + 1) * TOPK, :tok]
    finish(DX, 1)
    for mb in range(2):
        for mask in range(1, NBLK):
            rt_copy(mb, mask).wait_send()
        for kind in range(14):
            tok_copy(mb, kind).wait_send()
        for q in (Y, DX):
            for mask in (0, 2, 4, 6):
                to_partner(q, mb, mask).wait_send()
            for h in range(2):
                second(q, mb, h).wait_send()
                for which in range(2):
                    first(q, mb, h, which).wait_send()


def layer(x, grad_y, route_rows, gate_rows, w_gate, w_up, w_down):
    _, tok, dim = x.shape
    ff = w_gate.shape[2]
    cap = tok // 2
    hbm, vmem = pl.BlockSpec(memory_space=pltpu.HBM), pl.BlockSpec(memory_space=pltpu.VMEM)
    dma = pltpu.SemaphoreType.DMA
    unit = QUAD * cap
    shape = jax.ShapeDtypeStruct
    return pl.pallas_call(
        layer_kernel,
        out_shape=(
            shape((2, tok, dim), BF), shape((2, tok, dim), BF), shape((2, TOPK, tok), F32),
            shape(w_gate.shape, F32), shape(w_up.shape, F32), shape(w_down.shape, F32),
        ),
        in_specs=[hbm] * 7,
        out_specs=(vmem,) * 6,
        scratch_shapes=[
            pltpu.VMEM((2, NBLK, tok, dim), BF),
            pltpu.VMEM((2, NBLK, tok, dim), BF),
            pltpu.VMEM((2, NBLK, 2 * TOPK, LANES), F32),
            pltpu.VMEM((2, TOPK, tok), jnp.int32),
            pltpu.VMEM((2, TOPK, tok), F32),
            pltpu.VMEM((2, 2 * TOPK, LANES), F32),
            pltpu.VMEM((NEXP, dim, 2 * ff), BF),
            pltpu.VMEM((NEXP, ff, dim), BF),
            pltpu.VMEM((2, NEXP, NBLK, tok), F32),
            pltpu.VMEM((2, NEXP, NBLK, tok), F32),
            pltpu.VMEM((4, QUAD, NEXP * cap, tok), BF),
            pltpu.VMEM((4, QUAD, NEXP * cap, 1), F32),
            pltpu.VMEM((NEXP, 4, unit, 1), F32),
            pltpu.VMEM((NEXP, 4, unit, dim), BF),
            pltpu.VMEM((NEXP, 4, unit, dim), BF),
            pltpu.VMEM((NEXP, 4, unit, 2 * ff), BF),
            pltpu.VMEM((NEXP, 4, unit, ff), BF),
            pltpu.VMEM((NEXP, 4, unit, dim), BF),
            pltpu.VMEM((QUAD, 3 * NEXP * cap, dim), BF),
            pltpu.VMEM((QUAD, NEXP * cap, dim), BF),
            pltpu.VMEM((NBLK, 2 * TOPK, LANES), F32),
            pltpu.VMEM((4, 2, QUAD, tok, dim), F32),
            pltpu.VMEM((4, 4, tok, dim), F32),
            pltpu.VMEM((4, 4, tok, dim), F32),
            pltpu.VMEM((4, 2, 2, tok // 2, dim), F32),
            pltpu.VMEM((4, 2, tok // 2, dim), F32),
            pltpu.VMEM((NBLK, 2 * TOPK, LANES), F32),
            dma((2,)), dma((2, 2)), dma((NEXP, 3)), dma((2, 14)), dma((2, 14)), dma((2, NBLK)), dma((2, NBLK)),
            dma((4, 4)), dma((4, 4)), dma((4, 2, 2)), dma((4, 2, 2)), dma((4, 2)), dma((4, 2)), dma((NBLK,)), dma((NBLK,)),
        ],
        compiler_params=pltpu.CompilerParams(collective_id=0, has_side_effects=True, vmem_limit_bytes=46 << 20),
        name="moe_layer",
    )(x, grad_y, route_rows, gate_rows, w_gate, w_up, w_down)


def flush_kernel(*refs):
    count = (len(refs) - 1) // 2
    sem = refs[-1]
    copies = [pltpu.make_async_copy(refs[i], refs[count + i], sem.at[i]) for i in range(count)]
    for copy in copies:
        copy.start()
    for copy in copies:
        copy.wait()


def flush(arrays):
    hbm, vmem = pl.BlockSpec(memory_space=pltpu.HBM), pl.BlockSpec(memory_space=pltpu.VMEM)
    return pl.pallas_call(
        flush_kernel,
        out_shape=tuple(jax.ShapeDtypeStruct(arr.shape, arr.dtype) for arr in arrays),
        in_specs=[vmem] * len(arrays),
        out_specs=(hbm,) * len(arrays),
        scratch_shapes=[pltpu.SemaphoreType.DMA((len(arrays),))],
        compiler_params=pltpu.CompilerParams(vmem_limit_bytes=12 << 20),
        name="write_out",
    )(*arrays)


def solution(mesh):
    tok_spec = P(None, ALL_AXES, None)
    w_spec = P(ALL_AXES, None, None)

    def moe_layer(x, route_idx, gates, w_gate, w_up, w_down, grad_y):
        stay = lambda arr: pltpu.with_memory_space_constraint(arr, pltpu.HBM)
        flat = lambda arr: jnp.transpose(arr, (0, 2, 1))
        args = [stay(arr) for arr in (x, grad_y, flat(route_idx), flat(gates), w_gate, w_up, w_down)]
        y, dx, g_gates, g_gate, g_up, g_down = flush(layer(*args))
        return y, dx, flat(g_gates), g_gate, g_up, g_down

    return jax.shard_map(moe_layer, mesh=mesh, in_specs=(tok_spec, tok_spec, tok_spec, w_spec, w_spec, w_spec, tok_spec), out_specs=(tok_spec, tok_spec, tok_spec, w_spec, w_spec, w_spec), check_vma=False)
```

```python
import functools

import jax
import jax.numpy as jnp
from jax import lax
from jax.experimental import pallas as pl
from jax.experimental.pallas import tpu as pltpu
from jax.sharding import PartitionSpec as P

ALL_AXES = ("rep", "row", "col", "core")
MESH = pl.DeviceIdType.MESH
BF = jnp.bfloat16
F32 = jnp.float32
NBLK = 8
QUAD = 4
NEXP = 4
TOPK = 4
LANES = 128
OWN, XY0, XY1, DIAG = 0, 1, 2, 3
Y, DX = 0, 1


def coords():
    return (lax.axis_index("rep"), lax.axis_index("row"), lax.axis_index("col"), lax.axis_index("core"))


def peer(mask):
    rep, row, col, core = coords()
    flip = lambda pos, bit: 1 - pos if mask & bit else pos
    return (rep, flip(row, 4), flip(col, 2), flip(core, 1))


def number(mask=0):
    _, row, col, core = peer(mask)
    return row * 4 + col * 2 + core


def announce():
    barrier = pltpu.get_barrier_semaphore()
    for mask in range(1, NBLK):
        pl.semaphore_signal(barrier, inc=1, device_id=peer(mask), device_id_type=MESH)


def all_entered():
    pl.semaphore_wait(pltpu.get_barrier_semaphore(), NBLK - 1)


def remote(src, dst, send_sem, recv_sem, mask):
    return pltpu.make_async_remote_copy(src_ref=src, dst_ref=dst, send_sem=send_sem, recv_sem=recv_sem, device_id=peer(mask), device_id_type=MESH)


def tdot(lhs, rhs):
    return lax.dot_general(lhs, rhs, (((0,), (0,)), ((), ())), preferred_element_type=F32)


def ndot(lhs, rhs):
    return lax.dot_general(lhs, rhs, (((1,), (1,)), ((), ())), preferred_element_type=F32)


def dot(lhs, rhs):
    return jnp.dot(lhs, rhs, preferred_element_type=F32)


CHIPS = {
    OWN: ((0, 0), (1, 0)),
    XY0: ((0, 2), (0, 4)),
    XY1: ((1, 4), (1, 2)),
    DIAG: ((0, 6), (1, 6)),
}
BLOCKS = {unit: tuple((mb, mask, c) for mb, mask in chips for c in range(2)) for unit, chips in CHIPS.items()}


def layer_kernel(x_hbm, dy_hbm, route_hbm, gate_hbm, wg_hbm, wu_hbm, wd_hbm,
                 y_ref, dx_ref, gates_ref, gg_ref, gu_ref, gd_ref,
                 xg, dyg, rt, route_tab, gate_tab, mine, wgu, wd, rank, grow, disp, gblk, gcol, xr, qr, uv, hid, outs, zbuf, pbuf, dg,
                 part, near_in, chip_sum, first_in, second_in, dg_in,
                 tab_sem, own_sem, w_sem, g_send, g_recv, rt_send, rt_recv, d_send, d_recv, f_send, f_recv, s_send, s_recv, dg_send, dg_recv):
    tok, dim = xg.shape[2], xg.shape[3]
    ff = wd.shape[1]
    cap = tok // 2
    _, row, col, core = coords()
    me, at_x, at_y, at_d = number(0), number(2), number(4), number(6)
    tokens = (xg, dyg)
    PART = 6

    announce()
    tables = [pltpu.make_async_copy(src, dst, tab_sem.at[i]) for i, (src, dst) in enumerate(((route_hbm, route_tab), (gate_hbm, gate_tab)))]
    own = [[pltpu.make_async_copy(src.at[mb], dst.at[mb, me], own_sem.at[mb, i]) for i, (src, dst) in enumerate(((x_hbm, xg), (dy_hbm, dyg)))] for mb in range(2)]
    weights = []
    for l in range(NEXP):
        weights += [
            pltpu.make_async_copy(wg_hbm.at[l], wgu.at[l, :, pl.ds(0, ff)], w_sem.at[l, 0]),
            pltpu.make_async_copy(wu_hbm.at[l], wgu.at[l, :, pl.ds(ff, ff)], w_sem.at[l, 1]),
            pltpu.make_async_copy(wd_hbm.at[l], wd.at[l], w_sem.at[l, 2]),
        ]
    for load in tables + own[0] + own[1] + weights:
        load.start()
    for load in tables:
        load.wait()
    mine[...] = jnp.zeros(mine.shape, F32)
    for mb in range(2):
        mine[pl.ds(mb * 2 * TOPK, TOPK), pl.ds(0, tok)] = route_tab[mb].astype(F32)
        mine[pl.ds(mb * 2 * TOPK + TOPK, TOPK), pl.ds(0, tok)] = gate_tab[mb]
    rt[me] = mine[...]
    all_entered()

    def tok_copy(mb, kind):
        if kind < PART:
            slot, mask = (me, 2) if kind in (0, 1) else (me, 4) if kind in (3, 4) else ((at_x, 4), (at_y, 2))[mb]
            which = int(kind in (1, 2, 4))
        else:
            which, slot, mask = (kind - PART) % 2, (me, at_x, at_y, at_d)[(kind - PART) // 2], 1
        ref = tokens[which].at[mb, slot]
        return remote(ref, ref, g_send.at[mb, kind], g_recv.at[mb, kind], mask)

    def send_own(mb, *kinds):
        for kind in kinds:
            tok_copy(mb, kind).start()

    def relay(mb, kind, *then):
        tok_copy(mb, kind).wait_recv()
        for nxt in then:
            tok_copy(mb, nxt).start()

    def rt_copy(mask):
        return remote(mine, rt.at[me], rt_send.at[mask], rt_recv.at[mask], mask)

    FIRST, SECOND = (2, 4), (4, 2)

    def to_partner(q, mb, mask):
        r, i = q * 2 + mb, mask // 2
        return remote(part.at[r, i, 1 - core], near_in.at[r, i], d_send.at[r, i], d_recv.at[r, i], 1)

    def partner_start(q, unit):
        for mb, mask in CHIPS[unit]:
            to_partner(q, mb, mask).start()

    def chip_add(q, mb, mask):
        r, i = q * 2 + mb, mask // 2
        to_partner(q, mb, mask).wait_recv()
        chip_sum[r, i] = part[r, i, core] + near_in[r, i]

    def first(q, mb, which):
        r = q * 2 + mb
        src = chip_sum.at[r, (3, FIRST[mb] // 2)[which]]
        return remote(src, first_in.at[r, which], f_send.at[r, which], f_recv.at[r, which], FIRST[mb])

    def second(q, mb):
        r = q * 2 + mb
        return remote(chip_sum.at[r, SECOND[mb] // 2], second_in.at[r], s_send.at[r], s_recv.at[r], SECOND[mb])

    def leave(q, unit):
        for mb, mask in CHIPS[unit]:
            if mask in (6, FIRST[mb]):
                chip_add(q, mb, mask)
                first(q, mb, 0 if mask == 6 else 1).start()
        for mb, mask in CHIPS[unit]:
            if mask not in (6, FIRST[mb]):
                chip_add(q, mb, mask)

    def second_send(q, mb):
        first(q, mb, 0).wait_recv()
        chip_sum[q * 2 + mb, SECOND[mb] // 2] += first_in[q * 2 + mb, 0]
        second(q, mb).start()

    def finish(q, mb):
        r = q * 2 + mb
        first(q, mb, 1).wait_recv()
        second(q, mb).wait_recv()
        (y_ref, dx_ref)[q][mb] = (chip_sum[r, 0] + first_in[r, 1] + second_in[r]).astype(BF)

    first_id = (me * NEXP).astype(F32)
    slot_iota = lax.broadcasted_iota(jnp.int32, (cap, tok), 0).astype(F32)

    def block_of(mask, c):
        return number(mask) - core + c

    before = lax.broadcasted_iota(jnp.int32, (tok, tok), 0) < lax.broadcasted_iota(jnp.int32, (tok, tok), 1)

    def make_ranks(mask):
        tables = rt[pl.ds(number(mask) - core, 2)]
        members, weights_of = [], []
        for mb in range(2):
            at = mb * 2 * TOPK
            routes, gates = tables[:, at : at + TOPK, :tok], tables[:, at + TOPK : at + 2 * TOPK, :tok]
            for l in range(NEXP):
                hit = routes == first_id + l
                members.append(jnp.sum(jnp.where(hit, 1.0, 0.0), axis=1))
                weights_of.append(jnp.sum(jnp.where(hit, gates, 0.0), axis=1))
        member = jnp.concatenate(members, axis=0)
        rank[mask // 2] = jnp.where(member > 0, dot(member.astype(BF), jnp.where(before, 1.0, 0.0).astype(BF)), -1.0)
        grow[mask // 2] = jnp.concatenate(weights_of, axis=0)

    def dispatch_x(unit):
        for b, (mb, mask, c) in enumerate(BLOCKS[unit]):
            lines = [pl.ds((mb * NEXP + l) * 2 + c, 1) for l in range(NEXP)]
            hot = jnp.concatenate([jnp.where(rank[mask // 2, line, :] == slot_iota, 1.0, 0.0) for line in lines], axis=0)
            gs = jnp.concatenate([jnp.broadcast_to(grow[mask // 2, line, :], (cap, tok)) for line in lines], axis=0)
            gate = jnp.sum(hot * gs, axis=1, keepdims=True)
            hot = hot.astype(BF)
            disp[unit, b] = hot
            gblk[unit, b] = gate
            xs = dot(hot, xg[mb, block_of(mask, c)]).astype(BF)
            rows = pl.ds(b * cap, cap)
            for l in range(NEXP):
                xr[l, unit, rows, :] = xs[l * cap : (l + 1) * cap]
                gcol[l, unit, rows, :] = gate[l * cap : (l + 1) * cap]

    def forward(u, between=lambda: None):
        @pl.loop(0, NEXP, unroll=NEXP)
        def _(l):
            both = dot(xr[l, u], wgu[l]).astype(BF)
            uv[l, u] = both
            both = both.astype(F32)
            gate_pre, up_pre = both[:, :ff], both[:, ff:]
            hidden = (gate_pre * jax.nn.sigmoid(gate_pre) * up_pre).astype(BF)
            hid[l, u] = hidden
            out = dot(hidden, wd[l]).astype(BF)
            outs[l, u] = out
            z = gcol[l, u] * out.astype(F32)
            hi = z.astype(BF)
            rest = z - hi.astype(F32)
            mid = rest.astype(BF)
            low = (rest - mid.astype(F32)).astype(BF)
            at = pl.multiple_of(l * cap, cap)
            for b in range(QUAD):
                for i, piece in enumerate((hi, mid, low)):
                    zbuf[b, pl.ds(i * NEXP * cap + at, cap), :] = piece[b * cap : (b + 1) * cap]

        between()

        for b, (mb, mask, c) in enumerate(BLOCKS[u]):
            part[Y * 2 + mb, mask // 2, c] = tdot(jnp.concatenate([disp[u, b]] * 3, axis=0), zbuf[b])

    def dispatch_dy(unit):
        for b, (mb, mask, c) in enumerate(BLOCKS[unit]):
            blk = block_of(mask, c)
            hot = disp[unit, b]
            dys = dot(hot, dyg[mb, blk])
            qs = (gblk[unit, b] * dys).astype(BF)
            rows = pl.ds(b * cap, cap)
            hot_f = hot.astype(F32)
            routes = rt[blk, mb * 2 * TOPK : mb * 2 * TOPK + TOPK, 0:tok]
            total = jnp.zeros((TOPK, tok), F32)
            for l in range(NEXP):
                cut = slice(l * cap, (l + 1) * cap)
                qr[l, unit, rows, :] = qs[cut]
                dots = jnp.sum(dys[cut] * outs[l, unit, rows, :].astype(F32), axis=1, keepdims=True)
                line = jnp.sum(hot_f[cut] * dots, axis=0, keepdims=True)
                total = total + jnp.where(routes == first_id + l, line, 0.0)
            dg[blk, pl.ds(mb * TOPK, TOPK), pl.ds(0, tok)] = total

    def backward(u, between=lambda: None):
        @pl.loop(0, NEXP, unroll=NEXP)
        def _(l):
            both = uv[l, u].astype(F32)
            gate_pre, up_pre = both[:, :ff], both[:, ff:]
            sig = jax.nn.sigmoid(gate_pre)
            back = ndot(qr[l, u], wd[l])
            d_up = (back * gate_pre * sig).astype(BF)
            d_gate = (back * up_pre * sig * (1.0 + gate_pre * (1.0 - sig))).astype(BF)
            d_both = jnp.concatenate([d_gate, d_up], axis=1)
            uv[l, u] = d_both
            d_in = ndot(d_both, wgu[l]).astype(BF)
            at = pl.multiple_of(l * cap, cap)
            for b in range(QUAD):
                pbuf[b, pl.ds(at, cap), :] = d_in[b * cap : (b + 1) * cap]

        between()

        for b, (mb, mask, c) in enumerate(BLOCKS[u]):
            part[DX * 2 + mb, mask // 2, c] = tdot(disp[u, b], pbuf[b])

    def weight_grads(l):
        rows = 2 * 2 * QUAD * cap
        gd_ref[l] = tdot(hid[l].reshape(rows, ff), qr[l].reshape(rows, dim))
        xs, d_both = xr[l].reshape(rows, dim), uv[l].reshape(rows, 2 * ff)
        gg_ref[l] = tdot(xs, d_both[:, :ff])
        gu_ref[l] = tdot(xs, d_both[:, ff:])

    def dg_copy(mask):
        return remote(dg.at[number(mask)], dg_in.at[me], dg_send.at[mask], dg_recv.at[mask], mask)

    for mask in (1, 2, 4, 3, 5, 6, 7):
        rt_copy(mask).start()
    for mb in range(2):
        own[mb][0].wait()
        send_own(mb, 6, 0, 3)
    own[0][1].wait()
    send_own(0, 7, 1)
    own[1][1].wait()
    send_own(1, 7)
    rt_copy(1).wait_recv()
    make_ranks(0)
    for load in weights:
        load.wait()
    relay(0, 6)
    relay(1, 6)
    dispatch_x(OWN)
    forward(OWN)
    partner_start(Y, OWN)

    relay(0, 0, 5, 8)
    relay(0, 3, 10)
    send_own(1, 4)
    for mask in (2, 3, 4, 5):
        rt_copy(mask).wait_recv()
    make_ranks(2)
    make_ranks(4)
    relay(0, 7)
    relay(1, 7)
    dispatch_dy(OWN)
    relay(1, 3, 5, 10)
    relay(1, 0, 8)
    send_own(1, 1)
    send_own(0, 4)
    relay(0, 8)
    relay(0, 10)
    dispatch_x(XY0)
    forward(XY0, lambda: relay(0, 1, 2, 9))
    partner_start(Y, XY0)

    for mask in (6, 7):
        rt_copy(mask).wait_recv()
    make_ranks(6)
    relay(0, 5, 12)
    relay(1, 8)
    relay(1, 10)
    dispatch_x(XY1)

    def during():
        relay(1, 4, 2, 11)
        relay(1, 5, 12)
        leave(Y, XY0)

    forward(XY1, during)
    partner_start(Y, XY1)

    relay(0, 12)
    relay(1, 12)
    dispatch_x(DIAG)
    relay(0, 4, 11)
    relay(1, 1, 9)

    def during():
        relay(0, 2, 13)
        leave(Y, XY1)

    forward(DIAG, during)
    partner_start(Y, DIAG)

    relay(1, 2, 13)
    leave(Y, OWN)
    relay(0, 9)
    relay(0, 11)
    dispatch_dy(XY0)
    leave(Y, DIAG)
    relay(1, 9)
    relay(1, 11)
    dispatch_dy(XY1)
    relay(0, 13)
    relay(1, 13)
    dispatch_dy(DIAG)
    for mask in range(1, NBLK):
        dg_copy(mask).start()
    dg_in[me] = dg[me]
    backward(DIAG)
    partner_start(DX, DIAG)

    backward(XY0, lambda: leave(DX, DIAG))
    partner_start(DX, XY0)

    def during():
        leave(DX, XY0)
        second_send(Y, 0)
        second_send(Y, 1)

    backward(XY1, during)
    partner_start(DX, XY1)

    def during():
        leave(DX, XY1)
        second_send(DX, 0)
        second_send(DX, 1)

    backward(OWN, during)
    partner_start(DX, OWN)

    weight_grads(0)
    leave(DX, OWN)
    weight_grads(1)
    weight_grads(2)
    weight_grads(3)
    finish(Y, 0)
    finish(Y, 1)
    for mask in range(1, NBLK):
        dg_copy(mask).wait()
    grads = jnp.sum(dg_in[...], axis=0)
    for mb in range(2):
        gates_ref[mb] = grads[mb * TOPK : (mb + 1) * TOPK, :tok]
    finish(DX, 0)
    finish(DX, 1)
    for mask in range(1, NBLK):
        rt_copy(mask).wait_send()
    for mb in range(2):
        for kind in range(14):
            tok_copy(mb, kind).wait_send()
        for q in (Y, DX):
            for mask in (0, 2, 4, 6):
                to_partner(q, mb, mask).wait_send()
            for which in range(2):
                first(q, mb, which).wait_send()
            second(q, mb).wait_send()


def layer(x, grad_y, route_rows, gate_rows, w_gate, w_up, w_down):
    _, tok, dim = x.shape
    ff = w_gate.shape[2]
    cap = tok // 2
    hbm, vmem = pl.BlockSpec(memory_space=pltpu.HBM), pl.BlockSpec(memory_space=pltpu.VMEM)
    dma = pltpu.SemaphoreType.DMA
    unit = QUAD * cap
    shape = jax.ShapeDtypeStruct
    return pl.pallas_call(
        layer_kernel,
        out_shape=(
            shape((2, tok, dim), BF), shape((2, tok, dim), BF), shape((2, TOPK, tok), F32),
            shape(w_gate.shape, F32), shape(w_up.shape, F32), shape(w_down.shape, F32),
        ),
        in_specs=[hbm] * 7,
        out_specs=(vmem,) * 6,
        scratch_shapes=[
            pltpu.VMEM((2, NBLK, tok, dim), BF),
            pltpu.VMEM((2, NBLK, tok, dim), BF),
            pltpu.VMEM((NBLK, 4 * TOPK, LANES), F32),
            pltpu.VMEM((2, TOPK, tok), jnp.int32),
            pltpu.VMEM((2, TOPK, tok), F32),
            pltpu.VMEM((4 * TOPK, LANES), F32),
            pltpu.VMEM((NEXP, dim, 2 * ff), BF),
            pltpu.VMEM((NEXP, ff, dim), BF),
            pltpu.VMEM((4, 4 * NEXP, tok), F32),
            pltpu.VMEM((4, 4 * NEXP, tok), F32),
            pltpu.VMEM((4, QUAD, NEXP * cap, tok), BF),
            pltpu.VMEM((4, QUAD, NEXP * cap, 1), F32),
            pltpu.VMEM((NEXP, 4, unit, 1), F32),
            pltpu.VMEM((NEXP, 4, unit, dim), BF),
            pltpu.VMEM((NEXP, 4, unit, dim), BF),
            pltpu.VMEM((NEXP, 4, unit, 2 * ff), BF),
            pltpu.VMEM((NEXP, 4, unit, ff), BF),
            pltpu.VMEM((NEXP, 4, unit, dim), BF),
            pltpu.VMEM((QUAD, 3 * NEXP * cap, dim), BF),
            pltpu.VMEM((QUAD, NEXP * cap, dim), BF),
            pltpu.VMEM((NBLK, 2 * TOPK, LANES), F32),
            pltpu.VMEM((4, 4, 2, tok, dim), F32),
            pltpu.VMEM((4, 4, tok, dim), F32),
            pltpu.VMEM((4, 4, tok, dim), F32),
            pltpu.VMEM((4, 2, tok, dim), F32),
            pltpu.VMEM((4, tok, dim), F32),
            pltpu.VMEM((NBLK, 2 * TOPK, LANES), F32),
            dma((2,)), dma((2, 2)), dma((NEXP, 3)), dma((2, 14)), dma((2, 14)), dma((NBLK,)), dma((NBLK,)),
            dma((4, 4)), dma((4, 4)), dma((4, 2)), dma((4, 2)), dma((4,)), dma((4,)), dma((NBLK,)), dma((NBLK,)),
        ],
        compiler_params=pltpu.CompilerParams(collective_id=0, has_side_effects=True, vmem_limit_bytes=46 << 20),
        name="moe_layer",
    )(x, grad_y, route_rows, gate_rows, w_gate, w_up, w_down)


def flush_kernel(*refs):
    count = (len(refs) - 1) // 2
    sem = refs[-1]
    copies = [pltpu.make_async_copy(refs[i], refs[count + i], sem.at[i]) for i in range(count)]
    for copy in copies:
        copy.start()
    for copy in copies:
        copy.wait()


def flush(arrays):
    hbm, vmem = pl.BlockSpec(memory_space=pltpu.HBM), pl.BlockSpec(memory_space=pltpu.VMEM)
    return pl.pallas_call(
        flush_kernel,
        out_shape=tuple(jax.ShapeDtypeStruct(arr.shape, arr.dtype) for arr in arrays),
        in_specs=[vmem] * len(arrays),
        out_specs=(hbm,) * len(arrays),
        scratch_shapes=[pltpu.SemaphoreType.DMA((len(arrays),))],
        compiler_params=pltpu.CompilerParams(vmem_limit_bytes=12 << 20),
        name="write_out",
    )(*arrays)


def solution(mesh):
    tok_spec = P(None, ALL_AXES, None)
    w_spec = P(ALL_AXES, None, None)

    def moe_layer(x, route_idx, gates, w_gate, w_up, w_down, grad_y):
        stay = lambda arr: pltpu.with_memory_space_constraint(arr, pltpu.HBM)
        flat = lambda arr: jnp.transpose(arr, (0, 2, 1))
        args = [stay(arr) for arr in (x, grad_y, flat(route_idx), flat(gates), w_gate, w_up, w_down)]
        y, dx, g_gates, g_gate, g_up, g_down = flush(layer(*args))
        return y, dx, flat(g_gates), g_gate, g_up, g_down

    return jax.shard_map(moe_layer, mesh=mesh, in_specs=(tok_spec, tok_spec, tok_spec, w_spec, w_spec, w_spec, tok_spec), out_specs=(tok_spec, tok_spec, tok_spec, w_spec, w_spec, w_spec), check_vma=False)
```

```python
import functools

import jax
import jax.numpy as jnp
from jax import lax
from jax.experimental import pallas as pl
from jax.experimental.pallas import tpu as pltpu
from jax.sharding import PartitionSpec as P

ALL_AXES = ("rep", "row", "col", "core")
MESH = pl.DeviceIdType.MESH
BF = jnp.bfloat16
F32 = jnp.float32
NBLK = 8
QUAD = 4
NEXP = 4
TOPK = 4
LANES = 128
OWN, XY0, XY1, DIAG = 0, 1, 2, 3
Y, DX = 0, 1


def coords():
    return (lax.axis_index("rep"), lax.axis_index("row"), lax.axis_index("col"), lax.axis_index("core"))


def peer(mask):
    rep, row, col, core = coords()
    flip = lambda pos, bit: 1 - pos if mask & bit else pos
    return (rep, flip(row, 4), flip(col, 2), flip(core, 1))


def number(mask=0):
    _, row, col, core = peer(mask)
    return row * 4 + col * 2 + core


def announce():
    barrier = pltpu.get_barrier_semaphore()
    for mask in range(1, NBLK):
        pl.semaphore_signal(barrier, inc=1, device_id=peer(mask), device_id_type=MESH)


def all_entered():
    pl.semaphore_wait(pltpu.get_barrier_semaphore(), NBLK - 1)


def remote(src, dst, send_sem, recv_sem, mask):
    return pltpu.make_async_remote_copy(src_ref=src, dst_ref=dst, send_sem=send_sem, recv_sem=recv_sem, device_id=peer(mask), device_id_type=MESH)


def tdot(lhs, rhs):
    return lax.dot_general(lhs, rhs, (((0,), (0,)), ((), ())), preferred_element_type=F32)


def ndot(lhs, rhs):
    return lax.dot_general(lhs, rhs, (((1,), (1,)), ((), ())), preferred_element_type=F32)


def dot(lhs, rhs):
    return jnp.dot(lhs, rhs, preferred_element_type=F32)


CHIPS = {
    OWN: ((0, 0), (1, 0)),
    XY0: ((0, 2), (0, 4)),
    XY1: ((1, 4), (1, 2)),
    DIAG: ((0, 6), (1, 6)),
}
BLOCKS = {unit: tuple((mb, mask, c) for mb, mask in chips for c in range(2)) for unit, chips in CHIPS.items()}


def layer_kernel(x_hbm, dy_hbm, route_hbm, gate_hbm, wg_hbm, wu_hbm, wd_hbm,
                 y_ref, dx_ref, gates_ref, gg_ref, gu_ref, gd_ref,
                 xg, dyg, rt, route_tab, gate_tab, mine, wgu, wd, rank, grow, disp, gblk, gcol, xr, qr, uv, hid, outs, zbuf, pbuf, dg,
                 part, near_in, chip_sum, first_in, second_in, dg_in,
                 tab_sem, own_sem, w_sem, g_send, g_recv, rt_send, rt_recv, d_send, d_recv, f_send, f_recv, s_send, s_recv, dg_send, dg_recv):
    tok, dim = xg.shape[2], xg.shape[3]
    ff = wd.shape[1]
    cap = tok // 2
    _, row, col, core = coords()
    me, at_x, at_y, at_d = number(0), number(2), number(4), number(6)
    tokens = (xg, dyg)
    PART = 6

    announce()
    tables = [pltpu.make_async_copy(src, dst, tab_sem.at[i]) for i, (src, dst) in enumerate(((route_hbm, route_tab), (gate_hbm, gate_tab)))]
    own = [[pltpu.make_async_copy(src.at[mb], dst.at[mb, me], own_sem.at[mb, i]) for i, (src, dst) in enumerate(((x_hbm, xg), (dy_hbm, dyg)))] for mb in range(2)]
    weights = []
    for l in range(NEXP):
        weights += [
            pltpu.make_async_copy(wg_hbm.at[l], wgu.at[l, :, pl.ds(0, ff)], w_sem.at[l, 0]),
            pltpu.make_async_copy(wu_hbm.at[l], wgu.at[l, :, pl.ds(ff, ff)], w_sem.at[l, 1]),
            pltpu.make_async_copy(wd_hbm.at[l], wd.at[l], w_sem.at[l, 2]),
        ]
    for load in tables + own[0] + own[1] + weights:
        load.start()
    for load in tables:
        load.wait()
    mine[...] = jnp.zeros(mine.shape, F32)
    for mb in range(2):
        mine[pl.ds(mb * 2 * TOPK, TOPK), pl.ds(0, tok)] = route_tab[mb].astype(F32)
        mine[pl.ds(mb * 2 * TOPK + TOPK, TOPK), pl.ds(0, tok)] = gate_tab[mb]
    rt[me] = mine[...]
    all_entered()

    def tok_copy(mb, kind):
        if kind < PART:
            slot, mask = (me, 2) if kind in (0, 1) else (me, 4) if kind in (3, 4) else ((at_x, 4), (at_y, 2))[mb]
            which = int(kind in (1, 2, 4))
        else:
            which, slot, mask = (kind - PART) % 2, (me, at_x, at_y, at_d)[(kind - PART) // 2], 1
        ref = tokens[which].at[mb, slot]
        return remote(ref, ref, g_send.at[mb, kind], g_recv.at[mb, kind], mask)

    def send_own(mb, *kinds):
        for kind in kinds:
            tok_copy(mb, kind).start()

    def relay(mb, kind, *then):
        tok_copy(mb, kind).wait_recv()
        for nxt in then:
            tok_copy(mb, nxt).start()

    def rt_copy(mask):
        return remote(mine, rt.at[me], rt_send.at[mask], rt_recv.at[mask], mask)

    FIRST, SECOND = (2, 4), (4, 2)
    half = tok // 2

    def to_partner(q, mb, mask):
        r, i = q * 2 + mb, mask // 2
        return remote(part.at[r, i, 1 - core], near_in.at[r, i], d_send.at[r, i], d_recv.at[r, i], 1)

    def partner_start(q, unit):
        for mb, mask in CHIPS[unit]:
            to_partner(q, mb, mask).start()

    def chip_add(q, mb, mask):
        r, i = q * 2 + mb, mask // 2
        to_partner(q, mb, mask).wait_recv()
        chip_sum[r, i] = part[r, i, core] + near_in[r, i]

    def rows_of(h):
        return pl.ds(h * half, half)

    def first(q, mb, h, which):
        r = q * 2 + mb
        src = chip_sum.at[r, (3, FIRST[h] // 2)[which], rows_of(h)]
        return remote(src, first_in.at[r, h, which], f_send.at[r, h, which], f_recv.at[r, h, which], FIRST[h])

    def second(q, mb, h):
        r = q * 2 + mb
        return remote(chip_sum.at[r, SECOND[h] // 2, rows_of(h)], second_in.at[r, h], s_send.at[r, h], s_recv.at[r, h], SECOND[h])

    def leave(q, unit):
        for mb, mask in CHIPS[unit]:
            chip_add(q, mb, mask)
            for h in range(2):
                if mask in (6, FIRST[h]):
                    first(q, mb, h, 0 if mask == 6 else 1).start()

    def second_send(q, mb):
        for h in range(2):
            first(q, mb, h, 0).wait_recv()
            chip_sum[q * 2 + mb, SECOND[h] // 2, rows_of(h), :] += first_in[q * 2 + mb, h, 0]
            second(q, mb, h).start()

    def finish(q, mb):
        r = q * 2 + mb
        for h in range(2):
            first(q, mb, h, 1).wait_recv()
            second(q, mb, h).wait_recv()
            done = chip_sum[r, 0, rows_of(h), :] + first_in[r, h, 1] + second_in[r, h]
            (y_ref, dx_ref)[q][mb, rows_of(h), :] = done.astype(BF)

    first_id = (me * NEXP).astype(F32)
    slot_iota = lax.broadcasted_iota(jnp.int32, (cap, tok), 0).astype(F32)

    def block_of(mask, c):
        return number(mask) - core + c

    before = lax.broadcasted_iota(jnp.int32, (tok, tok), 0) < lax.broadcasted_iota(jnp.int32, (tok, tok), 1)

    def make_ranks(mask):
        tables = rt[pl.ds(number(mask) - core, 2)]
        members, weights_of = [], []
        for mb in range(2):
            at = mb * 2 * TOPK
            routes, gates = tables[:, at : at + TOPK, :tok], tables[:, at + TOPK : at + 2 * TOPK, :tok]
            for l in range(NEXP):
                hit = routes == first_id + l
                members.append(jnp.sum(jnp.where(hit, 1.0, 0.0), axis=1))
                weights_of.append(jnp.sum(jnp.where(hit, gates, 0.0), axis=1))
        member = jnp.concatenate(members, axis=0)
        rank[mask // 2] = jnp.where(member > 0, dot(member.astype(BF), jnp.where(before, 1.0, 0.0).astype(BF)), -1.0)
        grow[mask // 2] = jnp.concatenate(weights_of, axis=0)

    def dispatch_x(unit):
        for b, (mb, mask, c) in enumerate(BLOCKS[unit]):
            lines = [pl.ds((mb * NEXP + l) * 2 + c, 1) for l in range(NEXP)]
            hot = jnp.concatenate([jnp.where(rank[mask // 2, line, :] == slot_iota, 1.0, 0.0) for line in lines], axis=0)
            gs = jnp.concatenate([jnp.broadcast_to(grow[mask // 2, line, :], (cap, tok)) for line in lines], axis=0)
            gate = jnp.sum(hot * gs, axis=1, keepdims=True)
            hot = hot.astype(BF)
            disp[unit, b] = hot
            gblk[unit, b] = gate
            xs = dot(hot, xg[mb, block_of(mask, c)]).astype(BF)
            rows = pl.ds(b * cap, cap)
            for l in range(NEXP):
                xr[l, unit, rows, :] = xs[l * cap : (l + 1) * cap]
                gcol[l, unit, rows, :] = gate[l * cap : (l + 1) * cap]

    def forward(u, between=lambda: None):
        def spread(l, out):
            z = gcol[l, u] * out.astype(F32)
            hi = z.astype(BF)
            rest = z - hi.astype(F32)
            mid = rest.astype(BF)
            low = (rest - mid.astype(F32)).astype(BF)
            for b in range(QUAD):
                for i, piece in enumerate((hi, mid, low)):
                    zbuf[b, pl.ds((i * NEXP + l) * cap, cap), :] = piece[b * cap : (b + 1) * cap]

        both, out = dot(xr[0, u], wgu[0]).astype(BF), None
        for l in range(NEXP):
            ahead = dot(xr[l + 1, u], wgu[l + 1]).astype(BF) if l + 1 < NEXP else None
            uv[l, u] = both
            both = both.astype(F32)
            gate_pre, up_pre = both[:, :ff], both[:, ff:]
            hidden = (gate_pre * jax.nn.sigmoid(gate_pre) * up_pre).astype(BF)
            hid[l, u] = hidden
            if out is not None:
                spread(l - 1, out)
            out = dot(hidden, wd[l]).astype(BF)
            outs[l, u] = out
            both = ahead
        spread(NEXP - 1, out)

        between()

        for b, (mb, mask, c) in enumerate(BLOCKS[u]):
            part[Y * 2 + mb, mask // 2, c] = tdot(jnp.concatenate([disp[u, b]] * 3, axis=0), zbuf[b])

    def dispatch_dy(unit):
        for b, (mb, mask, c) in enumerate(BLOCKS[unit]):
            blk = block_of(mask, c)
            hot = disp[unit, b]
            dys = dot(hot, dyg[mb, blk])
            qs = (gblk[unit, b] * dys).astype(BF)
            rows = pl.ds(b * cap, cap)
            hot_f = hot.astype(F32)
            routes = rt[blk, mb * 2 * TOPK : mb * 2 * TOPK + TOPK, 0:tok]
            total = jnp.zeros((TOPK, tok), F32)
            for l in range(NEXP):
                cut = slice(l * cap, (l + 1) * cap)
                qr[l, unit, rows, :] = qs[cut]
                dots = jnp.sum(dys[cut] * outs[l, unit, rows, :].astype(F32), axis=1, keepdims=True)
                line = jnp.sum(hot_f[cut] * dots, axis=0, keepdims=True)
                total = total + jnp.where(routes == first_id + l, line, 0.0)
            dg[blk, pl.ds(mb * TOPK, TOPK), pl.ds(0, tok)] = total

    def backward(u, between=lambda: None):
        back = ndot(qr[0, u], wd[0])
        for l in range(NEXP):
            ahead = ndot(qr[l + 1, u], wd[l + 1]) if l + 1 < NEXP else None
            both = uv[l, u].astype(F32)
            gate_pre, up_pre = both[:, :ff], both[:, ff:]
            sig = jax.nn.sigmoid(gate_pre)
            d_up = (back * gate_pre * sig).astype(BF)
            d_gate = (back * up_pre * sig * (1.0 + gate_pre * (1.0 - sig))).astype(BF)
            d_both = jnp.concatenate([d_gate, d_up], axis=1)
            uv[l, u] = d_both
            d_in = ndot(d_both, wgu[l]).astype(BF)
            for b in range(QUAD):
                pbuf[b, pl.ds(l * cap, cap), :] = d_in[b * cap : (b + 1) * cap]
            back = ahead

        between()

        for b, (mb, mask, c) in enumerate(BLOCKS[u]):
            part[DX * 2 + mb, mask // 2, c] = tdot(disp[u, b], pbuf[b])

    def weight_grads(l):
        rows = 2 * 2 * QUAD * cap
        gd_ref[l] = tdot(hid[l].reshape(rows, ff), qr[l].reshape(rows, dim))
        xs, d_both = xr[l].reshape(rows, dim), uv[l].reshape(rows, 2 * ff)
        grads = tdot(xs, d_both)
        gg_ref[l] = grads[:, :ff]
        gu_ref[l] = grads[:, ff:]

    def dg_copy(mask):
        return remote(dg.at[number(mask)], dg_in.at[me], dg_send.at[mask], dg_recv.at[mask], mask)

    for mask in (1, 2, 4, 3, 5, 6, 7):
        rt_copy(mask).start()
    for mb in range(2):
        own[mb][0].wait()
        send_own(mb, 6, 0, 3)
    own[0][1].wait()
    send_own(0, 7, 1)
    own[1][1].wait()
    send_own(1, 7, 4)
    rt_copy(1).wait_recv()
    make_ranks(0)
    for load in weights:
        load.wait()
    relay(0, 6)
    relay(1, 6)
    dispatch_x(OWN)
    forward(OWN)
    partner_start(Y, OWN)

    relay(0, 0, 5, 8)
    relay(0, 3, 10)
    for mask in (2, 3, 4, 5):
        rt_copy(mask).wait_recv()
    make_ranks(2)
    make_ranks(4)
    relay(0, 7)
    relay(1, 7)
    dispatch_dy(OWN)
    relay(1, 3, 5, 10)
    relay(1, 0, 8)
    send_own(1, 1)
    send_own(0, 4)
    relay(0, 8)
    relay(0, 10)
    dispatch_x(XY0)
    forward(XY0, lambda: relay(0, 1, 2, 9))
    partner_start(Y, XY0)

    for mask in (6, 7):
        rt_copy(mask).wait_recv()
    make_ranks(6)
    relay(1, 4, 2, 11)
    relay(1, 8)
    relay(1, 10)
    dispatch_x(XY1)
    relay(0, 5, 12)

    def during():
        relay(1, 5, 12)
        leave(Y, XY0)

    forward(XY1, during)
    partner_start(Y, XY1)

    relay(0, 12)
    relay(1, 12)
    dispatch_x(DIAG)
    relay(0, 4, 11)
    relay(1, 1, 9)

    def during():
        relay(0, 2, 13)
        leave(Y, XY1)

    forward(DIAG, during)
    partner_start(Y, DIAG)

    relay(1, 2, 13)
    leave(Y, OWN)
    relay(0, 9)
    relay(0, 11)
    dispatch_dy(XY0)
    leave(Y, DIAG)
    relay(1, 9)
    relay(1, 11)
    dispatch_dy(XY1)
    relay(0, 13)
    relay(1, 13)
    dispatch_dy(DIAG)
    for mask in range(1, NBLK):
        dg_copy(mask).start()
    dg_in[me] = dg[me]
    backward(DIAG)
    partner_start(DX, DIAG)

    backward(XY0, lambda: leave(DX, DIAG))
    partner_start(DX, XY0)

    def during():
        leave(DX, XY0)
        second_send(Y, 0)
        second_send(Y, 1)

    backward(XY1, during)
    partner_start(DX, XY1)

    def during():
        leave(DX, XY1)

    backward(OWN, during)
    partner_start(DX, OWN)
    second_send(DX, 0)
    second_send(DX, 1)

    weight_grads(0)
    leave(DX, OWN)
    weight_grads(1)
    weight_grads(2)
    weight_grads(3)
    finish(Y, 0)
    finish(Y, 1)
    for mask in range(1, NBLK):
        dg_copy(mask).wait()
    grads = jnp.sum(dg_in[...], axis=0)
    for mb in range(2):
        gates_ref[mb] = grads[mb * TOPK : (mb + 1) * TOPK, :tok]
    finish(DX, 0)
    finish(DX, 1)
    for mask in range(1, NBLK):
        rt_copy(mask).wait_send()
    for mb in range(2):
        for kind in range(14):
            tok_copy(mb, kind).wait_send()
        for q in (Y, DX):
            for mask in (0, 2, 4, 6):
                to_partner(q, mb, mask).wait_send()
            for h in range(2):
                second(q, mb, h).wait_send()
                for which in range(2):
                    first(q, mb, h, which).wait_send()


def layer(x, grad_y, route_rows, gate_rows, w_gate, w_up, w_down):
    _, tok, dim = x.shape
    ff = w_gate.shape[2]
    cap = tok // 2
    hbm, vmem = pl.BlockSpec(memory_space=pltpu.HBM), pl.BlockSpec(memory_space=pltpu.VMEM)
    dma = pltpu.SemaphoreType.DMA
    unit = QUAD * cap
    shape = jax.ShapeDtypeStruct
    return pl.pallas_call(
        layer_kernel,
        out_shape=(
            shape((2, tok, dim), BF), shape((2, tok, dim), BF), shape((2, TOPK, tok), F32),
            shape(w_gate.shape, F32), shape(w_up.shape, F32), shape(w_down.shape, F32),
        ),
        in_specs=[hbm] * 7,
        out_specs=(vmem,) * 6,
        scratch_shapes=[
            pltpu.VMEM((2, NBLK, tok, dim), BF),
            pltpu.VMEM((2, NBLK, tok, dim), BF),
            pltpu.VMEM((NBLK, 4 * TOPK, LANES), F32),
            pltpu.VMEM((2, TOPK, tok), jnp.int32),
            pltpu.VMEM((2, TOPK, tok), F32),
            pltpu.VMEM((4 * TOPK, LANES), F32),
            pltpu.VMEM((NEXP, dim, 2 * ff), BF),
            pltpu.VMEM((NEXP, ff, dim), BF),
            pltpu.VMEM((4, 4 * NEXP, tok), F32),
            pltpu.VMEM((4, 4 * NEXP, tok), F32),
            pltpu.VMEM((4, QUAD, NEXP * cap, tok), BF),
            pltpu.VMEM((4, QUAD, NEXP * cap, 1), F32),
            pltpu.VMEM((NEXP, 4, unit, 1), F32),
            pltpu.VMEM((NEXP, 4, unit, dim), BF),
            pltpu.VMEM((NEXP, 4, unit, dim), BF),
            pltpu.VMEM((NEXP, 4, unit, 2 * ff), BF),
            pltpu.VMEM((NEXP, 4, unit, ff), BF),
            pltpu.VMEM((NEXP, 4, unit, dim), BF),
            pltpu.VMEM((QUAD, 3 * NEXP * cap, dim), BF),
            pltpu.VMEM((QUAD, NEXP * cap, dim), BF),
            pltpu.VMEM((NBLK, 2 * TOPK, LANES), F32),
            pltpu.VMEM((4, 4, 2, tok, dim), F32),
            pltpu.VMEM((4, 4, tok, dim), F32),
            pltpu.VMEM((4, 4, tok, dim), F32),
            pltpu.VMEM((4, 2, 2, tok // 2, dim), F32),
            pltpu.VMEM((4, 2, tok // 2, dim), F32),
            pltpu.VMEM((NBLK, 2 * TOPK, LANES), F32),
            dma((2,)), dma((2, 2)), dma((NEXP, 3)), dma((2, 14)), dma((2, 14)), dma((NBLK,)), dma((NBLK,)),
            dma((4, 4)), dma((4, 4)), dma((4, 2, 2)), dma((4, 2, 2)), dma((4, 2)), dma((4, 2)), dma((NBLK,)), dma((NBLK,)),
        ],
        compiler_params=pltpu.CompilerParams(collective_id=0, has_side_effects=True, vmem_limit_bytes=46 << 20),
        name="moe_layer",
    )(x, grad_y, route_rows, gate_rows, w_gate, w_up, w_down)


def flush_kernel(*refs):
    count = (len(refs) - 1) // 2
    sem = refs[-1]
    copies = [pltpu.make_async_copy(refs[i], refs[count + i], sem.at[i]) for i in range(count)]
    for copy in copies:
        copy.start()
    for copy in copies:
        copy.wait()


def flush(arrays):
    hbm, vmem = pl.BlockSpec(memory_space=pltpu.HBM), pl.BlockSpec(memory_space=pltpu.VMEM)
    return pl.pallas_call(
        flush_kernel,
        out_shape=tuple(jax.ShapeDtypeStruct(arr.shape, arr.dtype) for arr in arrays),
        in_specs=[vmem] * len(arrays),
        out_specs=(hbm,) * len(arrays),
        scratch_shapes=[pltpu.SemaphoreType.DMA((len(arrays),))],
        compiler_params=pltpu.CompilerParams(vmem_limit_bytes=12 << 20),
        name="write_out",
    )(*arrays)


def solution(mesh):
    tok_spec = P(None, ALL_AXES, None)
    w_spec = P(ALL_AXES, None, None)

    def moe_layer(x, route_idx, gates, w_gate, w_up, w_down, grad_y):
        stay = lambda arr: pltpu.with_memory_space_constraint(arr, pltpu.HBM)
        flat = lambda arr: jnp.transpose(arr, (0, 2, 1))
        args = [stay(arr) for arr in (x, grad_y, flat(route_idx), flat(gates), w_gate, w_up, w_down)]
        y, dx, g_gates, g_gate, g_up, g_down = flush(layer(*args))
        return y, dx, flat(g_gates), g_gate, g_up, g_down

    return jax.shard_map(moe_layer, mesh=mesh, in_specs=(tok_spec, tok_spec, tok_spec, w_spec, w_spec, w_spec, tok_spec), out_specs=(tok_spec, tok_spec, tok_spec, w_spec, w_spec, w_spec), check_vma=False)
```

```python
import functools

import jax
import jax.numpy as jnp
from jax import lax
from jax.experimental import pallas as pl
from jax.experimental.pallas import tpu as pltpu
from jax.sharding import PartitionSpec as P

ALL_AXES = ("rep", "row", "col", "core")
MESH = pl.DeviceIdType.MESH
BF = jnp.bfloat16
F32 = jnp.float32
NBLK = 8
QUAD = 4
NEXP = 4
TOPK = 4
LANES = 128
OWN, XY0, XY1, DIAG = 0, 1, 2, 3
Y, DX = 0, 1


def coords():
    return (lax.axis_index("rep"), lax.axis_index("row"), lax.axis_index("col"), lax.axis_index("core"))


def peer(mask):
    rep, row, col, core = coords()
    flip = lambda pos, bit: 1 - pos if mask & bit else pos
    return (rep, flip(row, 4), flip(col, 2), flip(core, 1))


def number(mask=0):
    _, row, col, core = peer(mask)
    return row * 4 + col * 2 + core


def announce():
    barrier = pltpu.get_barrier_semaphore()
    for mask in range(1, NBLK):
        pl.semaphore_signal(barrier, inc=1, device_id=peer(mask), device_id_type=MESH)


def all_entered():
    pl.semaphore_wait(pltpu.get_barrier_semaphore(), NBLK - 1)


def remote(src, dst, send_sem, recv_sem, mask):
    return pltpu.make_async_remote_copy(src_ref=src, dst_ref=dst, send_sem=send_sem, recv_sem=recv_sem, device_id=peer(mask), device_id_type=MESH)


def tdot(lhs, rhs):
    return lax.dot_general(lhs, rhs, (((0,), (0,)), ((), ())), preferred_element_type=F32)


def ndot(lhs, rhs):
    return lax.dot_general(lhs, rhs, (((1,), (1,)), ((), ())), preferred_element_type=F32)


def dot(lhs, rhs):
    return jnp.dot(lhs, rhs, preferred_element_type=F32)


CHIPS = {
    OWN: ((0, 0), (1, 0)),
    XY0: ((0, 2), (0, 4)),
    XY1: ((1, 4), (1, 2)),
    DIAG: ((0, 6), (1, 6)),
}
BLOCKS = {unit: tuple((mb, mask, c) for mb, mask in chips for c in range(2)) for unit, chips in CHIPS.items()}


PAIRS = (
    ((0, 6), (1, 6)), ((0, 7), (1, 7)), ((0, 8), (0, 10)), ((1, 8), (1, 10)),
    ((0, 9), (0, 11)), ((1, 9), (1, 11)), ((0, 12), (1, 12)), ((0, 13), (1, 13)),
)
PAIR = {item: 12 + i for i, pair in enumerate(PAIRS) for item in pair}


def layer_kernel(x_hbm, dy_hbm, route_hbm, gate_hbm, wg_hbm, wu_hbm, wd_hbm,
                 y_ref, dx_ref, gates_ref, gg_ref, gu_ref, gd_ref,
                 xg, dyg, rt, route_tab, gate_tab, wgu, wd, rank, grow, disp, gblk, gcol, xr, qr, uv, hid, outs, zbuf, pbuf, dg,
                 part, near_in, chip_sum, first_in, second_in, dg_in,
                 tab_sem, own_sem, w_sem, g_send, g_recv, rt_send, rt_recv, d_send, d_recv, f_send, f_recv, s_send, s_recv, dg_send, dg_recv):
    tok, dim = xg.shape[2], xg.shape[3]
    ff = wd.shape[1]
    cap = tok // 2
    _, row, col, core = coords()
    me, at_x, at_y, at_d = number(0), number(2), number(4), number(6)
    tokens = (xg, dyg)
    PART = 6

    announce()
    tables = [pltpu.make_async_copy(src, dst, tab_sem.at[i]) for i, (src, dst) in enumerate(((route_hbm, route_tab), (gate_hbm, gate_tab)))]
    own = [[pltpu.make_async_copy(src.at[mb], dst.at[mb, me], own_sem.at[mb, i]) for i, (src, dst) in enumerate(((x_hbm, xg), (dy_hbm, dyg)))] for mb in range(2)]
    weights = [
        pltpu.make_async_copy(wg_hbm, wgu.at[:, :, pl.ds(0, ff)], w_sem.at[0]),
        pltpu.make_async_copy(wu_hbm, wgu.at[:, :, pl.ds(ff, ff)], w_sem.at[1]),
        pltpu.make_async_copy(wd_hbm, wd, w_sem.at[2]),
    ]
    for load in tables + own[0] + own[1] + weights:
        load.start()
    for load in tables:
        load.wait()
    rt[me] = jnp.zeros(rt.shape[1:], F32)
    for mb in range(2):
        rt[me, pl.ds(mb * 2 * TOPK, TOPK), pl.ds(0, tok)] = route_tab[mb].astype(F32)
        rt[me, pl.ds(mb * 2 * TOPK + TOPK, TOPK), pl.ds(0, tok)] = gate_tab[mb]
    all_entered()

    def tok_copy(mb, kind):
        if kind < PART:
            slot, mask = (me, 2) if kind in (0, 1) else (me, 4) if kind in (3, 4) else ((at_x, 4), (at_y, 2))[mb]
            which = int(kind in (1, 2, 4))
        else:
            which, slot, mask = (kind - PART) % 2, (me, at_x, at_y, at_d)[(kind - PART) // 2], 1
        ref = tokens[which].at[mb, slot]
        arrival = mb * PART + kind if kind < PART else PAIR[mb, kind]
        return remote(ref, ref, g_send.at[which], g_recv.at[arrival], mask)

    def await_pair(mb, kind):
        which = (kind - PART) % 2
        two = tokens[which].at[0, pl.ds(0, 2)]
        remote(two, two, g_send.at[which], g_recv.at[PAIR[mb, kind]], 1).wait_recv()

    def send_own(mb, *kinds):
        for kind in kinds:
            tok_copy(mb, kind).start()

    def relay(mb, kind, *then):
        tok_copy(mb, kind).wait_recv()
        for nxt in then:
            tok_copy(mb, nxt).start()

    def rt_copy(kind):
        slot, mask = ((me, 1), (me, 2), (me, 4), (at_x, 4), (at_x, 1), (at_y, 1), (at_d, 1))[kind]
        return remote(rt.at[slot], rt.at[slot], rt_send.at[0], rt_recv.at[kind], mask)

    def rt_relay(kind, *then):
        rt_copy(kind).wait_recv()
        for nxt in then:
            rt_copy(nxt).start()

    FIRST, SECOND = (2, 4), (4, 2)
    half = tok // 2

    def to_partner(q, unit, mb, mask):
        r, i = q * 2 + mb, mask // 2
        return remote(part.at[r, i, 1 - core], near_in.at[r, i], d_send.at[0], d_recv.at[q, unit], 1)

    def partner_start(q, unit):
        for mb, mask in CHIPS[unit]:
            to_partner(q, unit, mb, mask).start()

    def rows_of(h):
        return pl.ds(h * half, half)

    def first(q, mb, h, which):
        r = q * 2 + mb
        src = chip_sum.at[r, (3, FIRST[h] // 2)[which], rows_of(h)]
        return remote(src, first_in.at[r, which, h], f_send.at[0], f_recv.at[r, which], FIRST[h])

    def second(q, mb, h):
        r = q * 2 + mb
        return remote(chip_sum.at[r, SECOND[h] // 2, rows_of(h)], second_in.at[r, h], s_send.at[0], s_recv.at[r], SECOND[h])

    def await_both(ref, sem):
        remote(ref, ref, s_send.at[0], sem, 2).wait_recv()

    def leave(q, unit):
        two = near_in.at[0, pl.ds(0, 2)]
        remote(two, two, d_send.at[0], d_recv.at[q, unit], 1).wait_recv()
        for mb, mask in CHIPS[unit]:
            r, i = q * 2 + mb, mask // 2
            chip_sum[r, i] = part[r, i, core] + near_in[r, i]
            for h in range(2):
                if mask in (6, FIRST[h]):
                    first(q, mb, h, 0 if mask == 6 else 1).start()

    def second_send(q, mb):
        r = q * 2 + mb
        await_both(first_in.at[r, 0], f_recv.at[r, 0])
        for h in range(2):
            chip_sum[r, SECOND[h] // 2, rows_of(h), :] += first_in[r, 0, h]
            second(q, mb, h).start()

    def finish(q, mb):
        r = q * 2 + mb
        await_both(first_in.at[r, 1], f_recv.at[r, 1])
        await_both(second_in.at[r], s_recv.at[r])
        for h in range(2):
            done = chip_sum[r, 0, rows_of(h), :] + first_in[r, 1, h] + second_in[r, h]
            (y_ref, dx_ref)[q][mb, rows_of(h), :] = done.astype(BF)

    first_id = (me * NEXP).astype(F32)
    slot_iota = lax.broadcasted_iota(jnp.int32, (cap, tok), 0).astype(F32)

    def block_of(mask, c):
        return number(mask) - core + c

    before = lax.broadcasted_iota(jnp.int32, (tok, tok), 0) < lax.broadcasted_iota(jnp.int32, (tok, tok), 1)

    def make_ranks(mask):
        tables = rt[pl.ds(number(mask) - core, 2)]
        members, weights_of = [], []
        for mb in range(2):
            at = mb * 2 * TOPK
            routes, gates = tables[:, at : at + TOPK, :tok], tables[:, at + TOPK : at + 2 * TOPK, :tok]
            for l in range(NEXP):
                hit = routes == first_id + l
                members.append(jnp.sum(jnp.where(hit, 1.0, 0.0), axis=1))
                weights_of.append(jnp.sum(jnp.where(hit, gates, 0.0), axis=1))
        member = jnp.concatenate(members, axis=0)
        rank[mask // 2] = jnp.where(member > 0, dot(member.astype(BF), jnp.where(before, 1.0, 0.0).astype(BF)), -1.0)
        grow[mask // 2] = jnp.concatenate(weights_of, axis=0)

    def dispatch_x(unit):
        for b, (mb, mask, c) in enumerate(BLOCKS[unit]):
            lines = [pl.ds((mb * NEXP + l) * 2 + c, 1) for l in range(NEXP)]
            hot = jnp.concatenate([jnp.where(rank[mask // 2, line, :] == slot_iota, 1.0, 0.0) for line in lines], axis=0)
            gs = jnp.concatenate([jnp.broadcast_to(grow[mask // 2, line, :], (cap, tok)) for line in lines], axis=0)
            gate = jnp.sum(hot * gs, axis=1, keepdims=True)
            hot = hot.astype(BF)
            disp[unit, b] = hot
            gblk[unit, b] = gate
            xs = dot(hot, xg[mb, block_of(mask, c)]).astype(BF)
            rows = pl.ds(b * cap, cap)
            for l in range(NEXP):
                xr[l, unit, rows, :] = xs[l * cap : (l + 1) * cap]
                gcol[l, unit, rows, :] = gate[l * cap : (l + 1) * cap]

    def forward(u, between=lambda: None, early=lambda: None):
        def spread(l, out):
            z = gcol[l, u] * out.astype(F32)
            hi = z.astype(BF)
            rest = z - hi.astype(F32)
            mid = rest.astype(BF)
            low = (rest - mid.astype(F32)).astype(BF)
            for b in range(QUAD):
                for i, piece in enumerate((hi, mid, low)):
                    zbuf[b, pl.ds((i * NEXP + l) * cap, cap), :] = piece[b * cap : (b + 1) * cap]

        both, out = dot(xr[0, u], wgu[0]).astype(BF), None
        for l in range(NEXP):
            ahead = dot(xr[l + 1, u], wgu[l + 1]).astype(BF) if l + 1 < NEXP else None
            uv[l, u] = both
            both = both.astype(F32)
            gate_pre, up_pre = both[:, :ff], both[:, ff:]
            hidden = (gate_pre * jax.nn.sigmoid(gate_pre) * up_pre).astype(BF)
            hid[l, u] = hidden
            if out is not None:
                spread(l - 1, out)
            out = dot(hidden, wd[l]).astype(BF)
            outs[l, u] = out
            both = ahead
            if l == 2:
                early()
        spread(NEXP - 1, out)

        between()

        for b, (mb, mask, c) in enumerate(BLOCKS[u]):
            part[Y * 2 + mb, mask // 2, c] = tdot(jnp.concatenate([disp[u, b]] * 3, axis=0), zbuf[b])

    def dispatch_dy(unit):
        for b, (mb, mask, c) in enumerate(BLOCKS[unit]):
            blk = block_of(mask, c)
            hot = disp[unit, b]
            dys = dot(hot, dyg[mb, blk])
            qs = (gblk[unit, b] * dys).astype(BF)
            rows = pl.ds(b * cap, cap)
            hot_f = hot.astype(F32)
            routes = rt[blk, mb * 2 * TOPK : mb * 2 * TOPK + TOPK, 0:tok]
            total = jnp.zeros((TOPK, tok), F32)
            for l in range(NEXP):
                cut = slice(l * cap, (l + 1) * cap)
                qr[l, unit, rows, :] = qs[cut]
                dots = jnp.sum(dys[cut] * outs[l, unit, rows, :].astype(F32), axis=1, keepdims=True)
                line = jnp.sum(hot_f[cut] * dots, axis=0, keepdims=True)
                total = total + jnp.where(routes == first_id + l, line, 0.0)
            dg[blk, pl.ds(mb * TOPK, TOPK), pl.ds(0, tok)] = total

    def backward(u, between=lambda: None, early=lambda: None):
        back = ndot(qr[0, u], wd[0])
        for l in range(NEXP):
            ahead = ndot(qr[l + 1, u], wd[l + 1]) if l + 1 < NEXP else None
            both = uv[l, u].astype(F32)
            gate_pre, up_pre = both[:, :ff], both[:, ff:]
            sig = jax.nn.sigmoid(gate_pre)
            d_up = (back * gate_pre * sig).astype(BF)
            d_gate = (back * up_pre * sig * (1.0 + gate_pre * (1.0 - sig))).astype(BF)
            d_both = jnp.concatenate([d_gate, d_up], axis=1)
            uv[l, u] = d_both
            d_in = ndot(d_both, wgu[l]).astype(BF)
            for b in range(QUAD):
                pbuf[b, pl.ds(l * cap, cap), :] = d_in[b * cap : (b + 1) * cap]
            back = ahead
            if l == 1:
                early()

        between()

        for b, (mb, mask, c) in enumerate(BLOCKS[u]):
            part[DX * 2 + mb, mask // 2, c] = tdot(disp[u, b], pbuf[b])

    def weight_grads(l):
        rows = 2 * 2 * QUAD * cap
        gd_ref[l] = tdot(hid[l].reshape(rows, ff), qr[l].reshape(rows, dim))
        xs, d_both = xr[l].reshape(rows, dim), uv[l].reshape(rows, 2 * ff)
        grads = tdot(xs, d_both)
        gg_ref[l] = grads[:, :ff]
        gu_ref[l] = grads[:, ff:]

    def dg_copy(mask):
        return remote(dg.at[number(mask)], dg_in.at[me], dg_send.at[0], dg_recv.at[0], mask)

    for kind in range(3):
        rt_copy(kind).start()
    for mb in range(2):
        own[mb][0].wait()
        send_own(mb, 6, 0, 3)
    own[0][1].wait()
    send_own(0, 7, 1)
    own[1][1].wait()
    send_own(1, 7)
    rt_relay(0)
    make_ranks(0)
    for load in weights:
        load.wait()
    await_pair(0, 6)
    dispatch_x(OWN)

    def during():
        rt_relay(1, 3, 4)
        rt_relay(2, 5)

    forward(OWN, lambda: None, during)
    partner_start(Y, OWN)

    relay(0, 0, 5, 8)
    send_own(1, 4)
    relay(0, 3, 10)
    rt_relay(4)
    rt_relay(5)
    make_ranks(2)
    make_ranks(4)
    await_pair(0, 7)
    dispatch_dy(OWN)
    relay(1, 3, 5, 10)
    relay(1, 0, 8)
    send_own(1, 1)
    send_own(0, 4)
    await_pair(0, 8)
    dispatch_x(XY0)
    forward(XY0, lambda: relay(0, 1, 2, 9), lambda: rt_relay(3, 6))
    partner_start(Y, XY0)

    rt_relay(6)
    make_ranks(6)
    relay(0, 5, 12)
    await_pair(1, 8)
    dispatch_x(XY1)

    def during():
        relay(1, 5, 12)
        relay(1, 4, 2, 11)

    forward(XY1, lambda: leave(Y, XY0), during)
    partner_start(Y, XY1)

    await_pair(0, 12)
    dispatch_x(DIAG)
    relay(0, 4, 11)
    relay(1, 1, 9)

    def during():
        leave(Y, XY1)
        relay(0, 2, 13)

    forward(DIAG, lambda: None, during)
    partner_start(Y, DIAG)

    relay(1, 2, 13)
    leave(Y, OWN)
    await_pair(0, 9)
    dispatch_dy(XY0)
    await_pair(1, 9)
    dispatch_dy(XY1)
    leave(Y, DIAG)
    await_pair(0, 13)
    dispatch_dy(DIAG)
    for mask in range(1, NBLK):
        dg_copy(mask).start()
    dg_in[me] = dg[me]
    backward(DIAG)
    partner_start(DX, DIAG)

    backward(XY0, lambda: leave(DX, DIAG))
    partner_start(DX, XY0)

    def during():
        second_send(Y, 0)
        second_send(Y, 1)

    backward(XY1, lambda: leave(DX, XY0), during)
    partner_start(DX, XY1)

    backward(OWN, lambda: leave(DX, XY1))
    partner_start(DX, OWN)
    weight_grads(0)
    second_send(DX, 0)
    second_send(DX, 1)
    leave(DX, OWN)
    weight_grads(1)
    weight_grads(2)
    weight_grads(3)
    finish(Y, 0)
    finish(Y, 1)
    seven = dg_in.at[pl.ds(0, NBLK - 1)]
    others = remote(seven, seven, dg_send.at[0], dg_recv.at[0], 1)
    others.wait_recv()
    others.wait_send()
    grads = jnp.sum(dg_in[...], axis=0)
    for mb in range(2):
        gates_ref[mb] = grads[mb * TOPK : (mb + 1) * TOPK, :tok]
    def sent(ref, sem):
        remote(ref, ref, sem, s_recv.at[0], 1).wait_send()

    sent(rt.at[pl.ds(0, 7)], rt_send.at[0])
    for which in range(2):
        sent(tokens[which].at[:, pl.ds(0, 7)], g_send.at[which])
    sent(near_in, d_send.at[0])
    sent(first_in, f_send.at[0])
    finish(DX, 0)
    finish(DX, 1)
    sent(second_in, s_send.at[0])


def layer(x, grad_y, route_rows, gate_rows, w_gate, w_up, w_down):
    _, tok, dim = x.shape
    ff = w_gate.shape[2]
    cap = tok // 2
    hbm, vmem = pl.BlockSpec(memory_space=pltpu.HBM), pl.BlockSpec(memory_space=pltpu.VMEM)
    dma = pltpu.SemaphoreType.DMA
    unit = QUAD * cap
    shape = jax.ShapeDtypeStruct
    return pl.pallas_call(
        layer_kernel,
        out_shape=(
            shape((2, tok, dim), BF), shape((2, tok, dim), BF), shape((2, TOPK, tok), F32),
            shape(w_gate.shape, F32), shape(w_up.shape, F32), shape(w_down.shape, F32),
        ),
        in_specs=[hbm] * 7,
        out_specs=(vmem,) * 6,
        scratch_shapes=[
            pltpu.VMEM((2, NBLK, tok, dim), BF),
            pltpu.VMEM((2, NBLK, tok, dim), BF),
            pltpu.VMEM((NBLK, 4 * TOPK, LANES), F32),
            pltpu.VMEM((2, TOPK, tok), jnp.int32),
            pltpu.VMEM((2, TOPK, tok), F32),
            pltpu.VMEM((NEXP, dim, 2 * ff), BF),
            pltpu.VMEM((NEXP, ff, dim), BF),
            pltpu.VMEM((4, 4 * NEXP, tok), F32),
            pltpu.VMEM((4, 4 * NEXP, tok), F32),
            pltpu.VMEM((4, QUAD, NEXP * cap, tok), BF),
            pltpu.VMEM((4, QUAD, NEXP * cap, 1), F32),
            pltpu.VMEM((NEXP, 4, unit, 1), F32),
            pltpu.VMEM((NEXP, 4, unit, dim), BF),
            pltpu.VMEM((NEXP, 4, unit, dim), BF),
            pltpu.VMEM((NEXP, 4, unit, 2 * ff), BF),
            pltpu.VMEM((NEXP, 4, unit, ff), BF),
            pltpu.VMEM((NEXP, 4, unit, dim), BF),
            pltpu.VMEM((QUAD, 3 * NEXP * cap, dim), BF),
            pltpu.VMEM((QUAD, NEXP * cap, dim), BF),
            pltpu.VMEM((NBLK, 2 * TOPK, LANES), F32),
            pltpu.VMEM((4, 4, 2, tok, dim), F32),
            pltpu.VMEM((4, 4, tok, dim), F32),
            pltpu.VMEM((4, 4, tok, dim), F32),
            pltpu.VMEM((4, 2, 2, tok // 2, dim), F32),
            pltpu.VMEM((4, 2, tok // 2, dim), F32),
            pltpu.VMEM((NBLK, 2 * TOPK, LANES), F32),
            dma((2,)), dma((2, 2)), dma((3,)), dma((2,)), dma((20,)), dma((1,)), dma((7,)),
            dma((1,)), dma((2, 4)), dma((1,)), dma((4, 2)), dma((1,)), dma((4,)), dma((1,)), dma((1,)),
        ],
        compiler_params=pltpu.CompilerParams(collective_id=0, has_side_effects=True, vmem_limit_bytes=46 << 20),
        name="moe_layer",
    )(x, grad_y, route_rows, gate_rows, w_gate, w_up, w_down)


def flush_kernel(*refs):
    count = (len(refs) - 1) // 2
    sem = refs[-1]
    copies = [pltpu.make_async_copy(refs[i], refs[count + i], sem.at[i]) for i in range(count)]
    for copy in reversed(copies):
        copy.start()
    for copy in copies:
        copy.wait()


def flush(arrays):
    hbm, vmem = pl.BlockSpec(memory_space=pltpu.HBM), pl.BlockSpec(memory_space=pltpu.VMEM)
    return pl.pallas_call(
        flush_kernel,
        out_shape=tuple(jax.ShapeDtypeStruct(arr.shape, arr.dtype) for arr in arrays),
        in_specs=[vmem] * len(arrays),
        out_specs=(hbm,) * len(arrays),
        scratch_shapes=[pltpu.SemaphoreType.DMA((len(arrays),))],
        compiler_params=pltpu.CompilerParams(vmem_limit_bytes=12 << 20),
        name="write_out",
    )(*arrays)


def solution(mesh):
    tok_spec = P(None, ALL_AXES, None)
    w_spec = P(ALL_AXES, None, None)

    def moe_layer(x, route_idx, gates, w_gate, w_up, w_down, grad_y):
        stay = lambda arr: pltpu.with_memory_space_constraint(arr, pltpu.HBM)
        flat = lambda arr: jnp.transpose(arr, (0, 2, 1))
        args = [stay(arr) for arr in (x, grad_y, flat(route_idx), flat(gates), w_gate, w_up, w_down)]
        y, dx, g_gates, g_gate, g_up, g_down = flush(layer(*args))
        return y, dx, flat(g_gates), g_gate, g_up, g_down

    return jax.shard_map(moe_layer, mesh=mesh, in_specs=(tok_spec, tok_spec, tok_spec, w_spec, w_spec, w_spec, tok_spec), out_specs=(tok_spec, tok_spec, tok_spec, w_spec, w_spec, w_spec), check_vma=False)
```

```python
import functools

import jax
import jax.numpy as jnp
from jax import lax
from jax.experimental import pallas as pl
from jax.experimental.pallas import tpu as pltpu
from jax.sharding import PartitionSpec as P

ALL_AXES = ("rep", "row", "col", "core")
MESH = pl.DeviceIdType.MESH
BF = jnp.bfloat16
F32 = jnp.float32
NBLK = 8
QUAD = 4
NEXP = 4
TOPK = 4
LANES = 128
OWN, XY0, XY1, DIAG = 0, 1, 2, 3
Y, DX = 0, 1


def coords():
    return (lax.axis_index("rep"), lax.axis_index("row"), lax.axis_index("col"), lax.axis_index("core"))


def peer(mask):
    rep, row, col, core = coords()
    flip = lambda pos, bit: 1 - pos if mask & bit else pos
    return (rep, flip(row, 4), flip(col, 2), flip(core, 1))


def number(mask=0):
    _, row, col, core = peer(mask)
    return row * 4 + col * 2 + core


def announce():
    barrier = pltpu.get_barrier_semaphore()
    for mask in range(1, NBLK):
        pl.semaphore_signal(barrier, inc=1, device_id=peer(mask), device_id_type=MESH)


def all_entered():
    pl.semaphore_wait(pltpu.get_barrier_semaphore(), NBLK - 1)


def remote(src, dst, send_sem, recv_sem, mask):
    return pltpu.make_async_remote_copy(src_ref=src, dst_ref=dst, send_sem=send_sem, recv_sem=recv_sem, device_id=peer(mask), device_id_type=MESH)


def tdot(lhs, rhs):
    return lax.dot_general(lhs, rhs, (((0,), (0,)), ((), ())), preferred_element_type=F32)


def ndot(lhs, rhs):
    return lax.dot_general(lhs, rhs, (((1,), (1,)), ((), ())), preferred_element_type=F32)


def dot(lhs, rhs):
    return jnp.dot(lhs, rhs, preferred_element_type=F32)


CHIPS = {
    OWN: ((0, 0), (1, 0)),
    XY0: ((0, 2), (0, 4)),
    XY1: ((1, 4), (1, 2)),
    DIAG: ((0, 6), (1, 6)),
}
BLOCKS = {unit: tuple((mb, mask, c) for mb, mask in chips for c in range(2)) for unit, chips in CHIPS.items()}


PAIRS = (
    ((0, 6), (1, 6)), ((0, 7), (1, 7)), ((0, 8), (0, 10)), ((1, 8), (1, 10)),
    ((0, 9), (0, 11)), ((1, 9), (1, 11)), ((0, 12), (1, 12)), ((0, 13), (1, 13)),
)
PAIR = {item: 12 + i for i, pair in enumerate(PAIRS) for item in pair}


def layer_kernel(x_hbm, dy_hbm, route_hbm, gate_hbm, wg_hbm, wu_hbm, wd_hbm,
                 y_ref, dx_ref, gates_ref, gg_ref, gu_ref, gd_ref,
                 xg, dyg, rt, route_tab, gate_tab, wgu, wd, rank, grow, disp, gblk, gcol, xr, qr, uv, hid, outs, zbuf, pbuf, dg,
                 part, near_in, chip_sum, first_in, second_in, dg_in,
                 tab_sem, own_sem, w_sem, g_send, g_recv, rt_send, rt_recv, d_send, d_recv, f_send, f_recv, s_send, s_recv, dg_send, dg_recv):
    tok, dim = xg.shape[2], xg.shape[3]
    ff = wd.shape[1]
    cap = tok // 2
    _, row, col, core = coords()
    me, at_x, at_y, at_d = number(0), number(2), number(4), number(6)
    tokens = (xg, dyg)
    PART = 6

    announce()
    tables = [pltpu.make_async_copy(src, dst, tab_sem.at[i]) for i, (src, dst) in enumerate(((route_hbm, route_tab), (gate_hbm, gate_tab)))]
    own = [[pltpu.make_async_copy(src.at[mb], dst.at[mb, me], own_sem.at[mb, i]) for i, (src, dst) in enumerate(((x_hbm, xg), (dy_hbm, dyg)))] for mb in range(2)]
    weights = [
        pltpu.make_async_copy(wg_hbm, wgu.at[:, :, pl.ds(0, ff)], w_sem.at[0]),
        pltpu.make_async_copy(wu_hbm, wgu.at[:, :, pl.ds(ff, ff)], w_sem.at[1]),
        pltpu.make_async_copy(wd_hbm, wd, w_sem.at[2]),
    ]
    for load in tables + own[0] + own[1] + weights:
        load.start()
    for load in tables:
        load.wait()
    rt[me] = jnp.zeros(rt.shape[1:], F32)
    for mb in range(2):
        rt[me, pl.ds(mb * 2 * TOPK, TOPK), pl.ds(0, tok)] = route_tab[mb].astype(F32)
        rt[me, pl.ds(mb * 2 * TOPK + TOPK, TOPK), pl.ds(0, tok)] = gate_tab[mb]
    all_entered()

    def tok_copy(mb, kind):
        if kind < PART:
            slot, mask = (me, 2) if kind in (0, 1) else (me, 4) if kind in (3, 4) else ((at_x, 4), (at_y, 2))[mb]
            which = int(kind in (1, 2, 4))
        else:
            which, slot, mask = (kind - PART) % 2, (me, at_x, at_y, at_d)[(kind - PART) // 2], 1
        ref = tokens[which].at[mb, slot]
        arrival = mb * PART + kind if kind < PART else PAIR[mb, kind]
        return remote(ref, ref, g_send.at[which], g_recv.at[arrival], mask)

    def await_pair(mb, kind):
        which = (kind - PART) % 2
        two = tokens[which].at[0, pl.ds(0, 2)]
        remote(two, two, g_send.at[which], g_recv.at[PAIR[mb, kind]], 1).wait_recv()

    def send_own(mb, *kinds):
        for kind in kinds:
            tok_copy(mb, kind).start()

    def relay(mb, kind, *then):
        tok_copy(mb, kind).wait_recv()
        for nxt in then:
            tok_copy(mb, nxt).start()

    def rt_copy(kind):
        slot, mask = ((me, 1), (me, 2), (me, 4), (at_x, 4), (at_x, 1), (at_y, 1), (at_d, 1))[kind]
        return remote(rt.at[slot], rt.at[slot], rt_send.at[0], rt_recv.at[kind], mask)

    def rt_relay(kind, *then):
        rt_copy(kind).wait_recv()
        for nxt in then:
            rt_copy(nxt).start()

    FIRST, SECOND = (2, 4), (4, 2)
    half = tok // 2

    def to_partner(q, unit, mb, mask):
        r, i = q * 2 + mb, mask // 2
        return remote(part.at[r, i, 1 - core], near_in.at[r, i], d_send.at[0], d_recv.at[q, unit], 1)

    def partner_start(q, unit):
        for mb, mask in CHIPS[unit]:
            to_partner(q, unit, mb, mask).start()

    def rows_of(h):
        return pl.ds(h * half, half)

    def first(q, mb, h, which):
        r = q * 2 + mb
        src = chip_sum.at[r, (3, FIRST[h] // 2)[which], rows_of(h)]
        return remote(src, first_in.at[r, which, h], f_send.at[0], f_recv.at[r, which], FIRST[h])

    def second(q, mb, h):
        r = q * 2 + mb
        return remote(chip_sum.at[r, SECOND[h] // 2, rows_of(h)], second_in.at[r, h], s_send.at[0], s_recv.at[r], SECOND[h])

    def await_both(ref, sem):
        remote(ref, ref, s_send.at[0], sem, 2).wait_recv()

    def leave(q, unit):
        two = near_in.at[0, pl.ds(0, 2)]
        remote(two, two, d_send.at[0], d_recv.at[q, unit], 1).wait_recv()
        for mb, mask in CHIPS[unit]:
            r, i = q * 2 + mb, mask // 2
            chip_sum[r, i] = part[r, i, core] + near_in[r, i]
            for h in range(2):
                if mask in (6, FIRST[h]):
                    first(q, mb, h, 0 if mask == 6 else 1).start()

    def second_send(q, mb):
        r = q * 2 + mb
        await_both(first_in.at[r, 0], f_recv.at[r, 0])
        for h in range(2):
            chip_sum[r, SECOND[h] // 2, rows_of(h), :] += first_in[r, 0, h]
            second(q, mb, h).start()

    def finish(q, mb):
        r = q * 2 + mb
        await_both(first_in.at[r, 1], f_recv.at[r, 1])
        await_both(second_in.at[r], s_recv.at[r])
        for h in range(2):
            done = chip_sum[r, 0, rows_of(h), :] + first_in[r, 1, h] + second_in[r, h]
            (y_ref, dx_ref)[q][mb, rows_of(h), :] = done.astype(BF)

    first_id = (me * NEXP).astype(F32)
    slot_iota = lax.broadcasted_iota(jnp.int32, (cap, tok), 0).astype(F32)

    def block_of(mask, c):
        return number(mask) - core + c

    before = lax.broadcasted_iota(jnp.int32, (tok, tok), 0) < lax.broadcasted_iota(jnp.int32, (tok, tok), 1)

    def make_ranks(mask):
        tables = rt[pl.ds(number(mask) - core, 2)]
        members, weights_of = [], []
        for mb in range(2):
            at = mb * 2 * TOPK
            routes, gates = tables[:, at : at + TOPK, :tok], tables[:, at + TOPK : at + 2 * TOPK, :tok]
            for l in range(NEXP):
                hit = routes == first_id + l
                members.append(jnp.sum(jnp.where(hit, 1.0, 0.0), axis=1))
                weights_of.append(jnp.sum(jnp.where(hit, gates, 0.0), axis=1))
        member = jnp.concatenate(members, axis=0)
        rank[mask // 2] = jnp.where(member > 0, dot(member.astype(BF), jnp.where(before, 1.0, 0.0).astype(BF)), -1.0)
        grow[mask // 2] = jnp.concatenate(weights_of, axis=0)

    def dispatch_x(unit):
        for b, (mb, mask, c) in enumerate(BLOCKS[unit]):
            lines = [pl.ds((mb * NEXP + l) * 2 + c, 1) for l in range(NEXP)]
            hot = jnp.concatenate([jnp.where(rank[mask // 2, line, :] == slot_iota, 1.0, 0.0) for line in lines], axis=0)
            gs = jnp.concatenate([jnp.broadcast_to(grow[mask // 2, line, :], (cap, tok)) for line in lines], axis=0)
            gate = jnp.sum(hot * gs, axis=1, keepdims=True)
            hot = hot.astype(BF)
            disp[unit, b] = hot
            gblk[unit, b] = gate
            xs = dot(hot, xg[mb, block_of(mask, c)]).astype(BF)
            rows = pl.ds(b * cap, cap)
            for l in range(NEXP):
                xr[l, unit, rows, :] = xs[l * cap : (l + 1) * cap]
                gcol[l, unit, rows, :] = gate[l * cap : (l + 1) * cap]

    def forward(u, between=lambda: None, early=lambda: None):
        def spread(l, out):
            z = gcol[l, u] * out.astype(F32)
            hi = z.astype(BF)
            rest = z - hi.astype(F32)
            mid = rest.astype(BF)
            low = (rest - mid.astype(F32)).astype(BF)
            for b in range(QUAD):
                for i, piece in enumerate((hi, mid, low)):
                    zbuf[b, pl.ds((i * NEXP + l) * cap, cap), :] = piece[b * cap : (b + 1) * cap]

        both, out = dot(xr[0, u], wgu[0]).astype(BF), None
        for l in range(NEXP):
            ahead = dot(xr[l + 1, u], wgu[l + 1]).astype(BF) if l + 1 < NEXP else None
            uv[l, u] = both
            both = both.astype(F32)
            gate_pre, up_pre = both[:, :ff], both[:, ff:]
            hidden = (gate_pre * jax.nn.sigmoid(gate_pre) * up_pre).astype(BF)
            hid[l, u] = hidden
            if out is not None:
                spread(l - 1, out)
            out = dot(hidden, wd[l]).astype(BF)
            outs[l, u] = out
            both = ahead
            if l == 2:
                early()
        spread(NEXP - 1, out)

        between()

        for b, (mb, mask, c) in enumerate(BLOCKS[u]):
            part[Y * 2 + mb, mask // 2, c] = tdot(jnp.concatenate([disp[u, b]] * 3, axis=0), zbuf[b])

    def dispatch_dy(unit):
        for b, (mb, mask, c) in enumerate(BLOCKS[unit]):
            blk = block_of(mask, c)
            hot = disp[unit, b]
            dys = dot(hot, dyg[mb, blk])
            qs = (gblk[unit, b] * dys).astype(BF)
            rows = pl.ds(b * cap, cap)
            hot_f = hot.astype(F32)
            routes = rt[blk, mb * 2 * TOPK : mb * 2 * TOPK + TOPK, 0:tok]
            total = jnp.zeros((TOPK, tok), F32)
            for l in range(NEXP):
                cut = slice(l * cap, (l + 1) * cap)
                qr[l, unit, rows, :] = qs[cut]
                dots = jnp.sum(dys[cut] * outs[l, unit, rows, :].astype(F32), axis=1, keepdims=True)
                line = jnp.sum(hot_f[cut] * dots, axis=0, keepdims=True)
                total = total + jnp.where(routes == first_id + l, line, 0.0)
            dg[blk, pl.ds(mb * TOPK, TOPK), pl.ds(0, tok)] = total

    def backward(u, between=lambda: None, early=lambda: None):
        back = ndot(qr[0, u], wd[0])
        for l in range(NEXP):
            ahead = ndot(qr[l + 1, u], wd[l + 1]) if l + 1 < NEXP else None
            both = uv[l, u].astype(F32)
            gate_pre, up_pre = both[:, :ff], both[:, ff:]
            sig = jax.nn.sigmoid(gate_pre)
            d_up = (back * gate_pre * sig).astype(BF)
            d_gate = (back * up_pre * sig * (1.0 + gate_pre * (1.0 - sig))).astype(BF)
            d_both = jnp.concatenate([d_gate, d_up], axis=1)
            uv[l, u] = d_both
            d_in = ndot(d_both, wgu[l]).astype(BF)
            for b in range(QUAD):
                pbuf[b, pl.ds(l * cap, cap), :] = d_in[b * cap : (b + 1) * cap]
            back = ahead
            if l == 1:
                early()

        between()

        for b, (mb, mask, c) in enumerate(BLOCKS[u]):
            part[DX * 2 + mb, mask // 2, c] = tdot(disp[u, b], pbuf[b])

    def weight_grads(l):
        rows = 2 * 2 * QUAD * cap
        gd_ref[l] = tdot(hid[l].reshape(rows, ff), qr[l].reshape(rows, dim))
        xs, d_both = xr[l].reshape(rows, dim), uv[l].reshape(rows, 2 * ff)
        grads = tdot(xs, d_both)
        gg_ref[l] = grads[:, :ff]
        gu_ref[l] = grads[:, ff:]

    def dg_copy(mask):
        return remote(dg.at[number(mask)], dg_in.at[me], dg_send.at[0], dg_recv.at[0], mask)

    for kind in range(3):
        rt_copy(kind).start()
    for mb in range(2):
        own[mb][0].wait()
        send_own(mb, 6, 0, 3)
    own[0][1].wait()
    send_own(0, 7, 1)
    own[1][1].wait()
    send_own(1, 7)
    rt_relay(0)
    make_ranks(0)
    for load in weights:
        load.wait()
    await_pair(0, 6)
    dispatch_x(OWN)

    def during():
        rt_relay(1, 3, 4)
        rt_relay(2, 5)

    forward(OWN, lambda: None, during)
    partner_start(Y, OWN)

    relay(0, 0, 5, 8)
    send_own(1, 4)
    relay(0, 3, 10)
    rt_relay(4)
    rt_relay(5)
    make_ranks(2)
    make_ranks(4)
    await_pair(0, 7)
    dispatch_dy(OWN)
    relay(1, 3, 5, 10)
    relay(1, 0, 8)
    send_own(1, 1)
    send_own(0, 4)
    await_pair(0, 8)
    dispatch_x(XY0)
    forward(XY0, lambda: relay(0, 1, 2, 9), lambda: rt_relay(3, 6))
    partner_start(Y, XY0)

    rt_relay(6)
    make_ranks(6)
    relay(0, 5, 12)
    await_pair(1, 8)
    dispatch_x(XY1)

    def during():
        relay(1, 5, 12)
        relay(1, 4, 2, 11)

    forward(XY1, lambda: leave(Y, XY0), during)
    partner_start(Y, XY1)

    await_pair(0, 12)
    dispatch_x(DIAG)
    relay(0, 4, 11)
    relay(1, 1, 9)

    def during():
        leave(Y, XY1)
        relay(0, 2, 13)

    forward(DIAG, lambda: None, during)
    partner_start(Y, DIAG)

    relay(1, 2, 13)
    await_pair(0, 9)
    dispatch_dy(XY0)
    leave(Y, DIAG)
    await_pair(0, 13)
    dispatch_dy(DIAG)
    backward(DIAG)
    partner_start(DX, DIAG)

    await_pair(1, 9)
    dispatch_dy(XY1)
    for mask in range(1, NBLK):
        dg_copy(mask).start()
    dg_in[me] = dg[me]
    leave(DX, DIAG)
    backward(XY0, lambda: leave(Y, OWN))
    partner_start(DX, XY0)

    def during():
        second_send(Y, 0)
        second_send(Y, 1)

    backward(XY1, lambda: leave(DX, XY0), during)
    partner_start(DX, XY1)

    backward(OWN, lambda: leave(DX, XY1))
    partner_start(DX, OWN)
    weight_grads(0)
    second_send(DX, 0)
    second_send(DX, 1)
    leave(DX, OWN)
    weight_grads(1)
    weight_grads(2)
    weight_grads(3)
    finish(Y, 0)
    finish(Y, 1)
    seven = dg_in.at[pl.ds(0, NBLK - 1)]
    others = remote(seven, seven, dg_send.at[0], dg_recv.at[0], 1)
    others.wait_recv()
    others.wait_send()
    grads = jnp.sum(dg_in[...], axis=0)
    for mb in range(2):
        gates_ref[mb] = grads[mb * TOPK : (mb + 1) * TOPK, :tok]
    def sent(ref, sem):
        remote(ref, ref, sem, s_recv.at[0], 1).wait_send()

    sent(rt.at[pl.ds(0, 7)], rt_send.at[0])
    for which in range(2):
        sent(tokens[which].at[:, pl.ds(0, 7)], g_send.at[which])
    sent(near_in, d_send.at[0])
    sent(first_in, f_send.at[0])
    finish(DX, 0)
    finish(DX, 1)
    sent(second_in, s_send.at[0])


def layer(x, grad_y, route_rows, gate_rows, w_gate, w_up, w_down):
    _, tok, dim = x.shape
    ff = w_gate.shape[2]
    cap = tok // 2
    hbm, vmem = pl.BlockSpec(memory_space=pltpu.HBM), pl.BlockSpec(memory_space=pltpu.VMEM)
    dma = pltpu.SemaphoreType.DMA
    unit = QUAD * cap
    shape = jax.ShapeDtypeStruct
    return pl.pallas_call(
        layer_kernel,
        out_shape=(
            shape((2, tok, dim), BF), shape((2, tok, dim), BF), shape((2, TOPK, tok), F32),
            shape(w_gate.shape, F32), shape(w_up.shape, F32), shape(w_down.shape, F32),
        ),
        in_specs=[hbm] * 7,
        out_specs=(vmem,) * 6,
        scratch_shapes=[
            pltpu.VMEM((2, NBLK, tok, dim), BF),
            pltpu.VMEM((2, NBLK, tok, dim), BF),
            pltpu.VMEM((NBLK, 4 * TOPK, LANES), F32),
            pltpu.VMEM((2, TOPK, tok), jnp.int32),
            pltpu.VMEM((2, TOPK, tok), F32),
            pltpu.VMEM((NEXP, dim, 2 * ff), BF),
            pltpu.VMEM((NEXP, ff, dim), BF),
            pltpu.VMEM((4, 4 * NEXP, tok), F32),
            pltpu.VMEM((4, 4 * NEXP, tok), F32),
            pltpu.VMEM((4, QUAD, NEXP * cap, tok), BF),
            pltpu.VMEM((4, QUAD, NEXP * cap, 1), F32),
            pltpu.VMEM((NEXP, 4, unit, 1), F32),
            pltpu.VMEM((NEXP, 4, unit, dim), BF),
            pltpu.VMEM((NEXP, 4, unit, dim), BF),
            pltpu.VMEM((NEXP, 4, unit, 2 * ff), BF),
            pltpu.VMEM((NEXP, 4, unit, ff), BF),
            pltpu.VMEM((NEXP, 4, unit, dim), BF),
            pltpu.VMEM((QUAD, 3 * NEXP * cap, dim), BF),
            pltpu.VMEM((QUAD, NEXP * cap, dim), BF),
            pltpu.VMEM((NBLK, 2 * TOPK, LANES), F32),
            pltpu.VMEM((4, 4, 2, tok, dim), F32),
            pltpu.VMEM((4, 4, tok, dim), F32),
            pltpu.VMEM((4, 4, tok, dim), F32),
            pltpu.VMEM((4, 2, 2, tok // 2, dim), F32),
            pltpu.VMEM((4, 2, tok // 2, dim), F32),
            pltpu.VMEM((NBLK, 2 * TOPK, LANES), F32),
            dma((2,)), dma((2, 2)), dma((3,)), dma((2,)), dma((20,)), dma((1,)), dma((7,)),
            dma((1,)), dma((2, 4)), dma((1,)), dma((4, 2)), dma((1,)), dma((4,)), dma((1,)), dma((1,)),
        ],
        compiler_params=pltpu.CompilerParams(collective_id=0, has_side_effects=True, vmem_limit_bytes=46 << 20),
        name="moe_layer",
    )(x, grad_y, route_rows, gate_rows, w_gate, w_up, w_down)


def flush_kernel(*refs):
    count = (len(refs) - 1) // 2
    sem = refs[-1]
    copies = [pltpu.make_async_copy(refs[i], refs[count + i], sem.at[i]) for i in range(count)]
    for copy in reversed(copies):
        copy.start()
    for copy in copies:
        copy.wait()


def flush(arrays):
    hbm, vmem = pl.BlockSpec(memory_space=pltpu.HBM), pl.BlockSpec(memory_space=pltpu.VMEM)
    return pl.pallas_call(
        flush_kernel,
        out_shape=tuple(jax.ShapeDtypeStruct(arr.shape, arr.dtype) for arr in arrays),
        in_specs=[vmem] * len(arrays),
        out_specs=(hbm,) * len(arrays),
        scratch_shapes=[pltpu.SemaphoreType.DMA((len(arrays),))],
        compiler_params=pltpu.CompilerParams(vmem_limit_bytes=12 << 20),
        name="write_out",
    )(*arrays)


def solution(mesh):
    tok_spec = P(None, ALL_AXES, None)
    w_spec = P(ALL_AXES, None, None)

    def moe_layer(x, route_idx, gates, w_gate, w_up, w_down, grad_y):
        stay = lambda arr: pltpu.with_memory_space_constraint(arr, pltpu.HBM)
        flat = lambda arr: jnp.transpose(arr, (0, 2, 1))
        args = [stay(arr) for arr in (x, grad_y, flat(route_idx), flat(gates), w_gate, w_up, w_down)]
        y, dx, g_gates, g_gate, g_up, g_down = flush(layer(*args))
        return y, dx, flat(g_gates), g_gate, g_up, g_down

    return jax.shard_map(moe_layer, mesh=mesh, in_specs=(tok_spec, tok_spec, tok_spec, w_spec, w_spec, w_spec, tok_spec), out_specs=(tok_spec, tok_spec, tok_spec, w_spec, w_spec, w_spec), check_vma=False)
```

```python
import functools

import jax
import jax.numpy as jnp
from jax import lax
from jax.experimental import pallas as pl
from jax.experimental.pallas import tpu as pltpu
from jax.sharding import PartitionSpec as P

ALL_AXES = ("rep", "row", "col", "core")
MESH = pl.DeviceIdType.MESH
BF = jnp.bfloat16
F32 = jnp.float32
NBLK = 8
QUAD = 4
NEXP = 4
TOPK = 4
LANES = 128
OWN, XY0, XY1, DIAG = 0, 1, 2, 3
Y, DX = 0, 1


def coords():
    return (lax.axis_index("rep"), lax.axis_index("row"), lax.axis_index("col"), lax.axis_index("core"))


def peer(mask):
    rep, row, col, core = coords()
    flip = lambda pos, bit: 1 - pos if mask & bit else pos
    return (rep, flip(row, 4), flip(col, 2), flip(core, 1))


def number(mask=0):
    _, row, col, core = peer(mask)
    return row * 4 + col * 2 + core


def announce():
    barrier = pltpu.get_barrier_semaphore()
    for mask in range(1, NBLK):
        pl.semaphore_signal(barrier, inc=1, device_id=peer(mask), device_id_type=MESH)


def all_entered():
    pl.semaphore_wait(pltpu.get_barrier_semaphore(), NBLK - 1)


def remote(src, dst, send_sem, recv_sem, mask):
    return pltpu.make_async_remote_copy(src_ref=src, dst_ref=dst, send_sem=send_sem, recv_sem=recv_sem, device_id=peer(mask), device_id_type=MESH)


def tdot(lhs, rhs):
    return lax.dot_general(lhs, rhs, (((0,), (0,)), ((), ())), preferred_element_type=F32)


def ndot(lhs, rhs):
    return lax.dot_general(lhs, rhs, (((1,), (1,)), ((), ())), preferred_element_type=F32)


def dot(lhs, rhs):
    return jnp.dot(lhs, rhs, preferred_element_type=F32)


CHIPS = {
    OWN: ((0, 0), (1, 0)),
    XY0: ((0, 2), (0, 4)),
    XY1: ((1, 4), (1, 2)),
    DIAG: ((0, 6), (1, 6)),
}
BLOCKS = {unit: tuple((mb, mask, c) for mb, mask in chips for c in range(2)) for unit, chips in CHIPS.items()}


PAIRS = (
    ((0, 6), (1, 6)), ((0, 7), (1, 7)), ((0, 8), (0, 10)), ((1, 8), (1, 10)),
    ((0, 9), (0, 11)), ((1, 9), (1, 11)), ((0, 12), (1, 12)), ((0, 13), (1, 13)),
)
PAIR = {item: 12 + i for i, pair in enumerate(PAIRS) for item in pair}


def layer_kernel(x_hbm, dy_hbm, route_hbm, gate_hbm, wg_hbm, wu_hbm, wd_hbm,
                 y_ref, dx_ref, gates_ref, gg_ref, gu_ref, gd_ref,
                 xg, dyg, rt, route_tab, gate_tab, wgu, wd, rank, grow, disp, gblk, gcol, xr, qr, uv, hid, outs, zbuf, pbuf, dg,
                 part, near_in, chip_sum, first_in, second_in, dg_in,
                 tab_sem, own_sem, w_sem, g_send, g_recv, rt_send, rt_recv, d_send, d_recv, f_send, f_recv, s_send, s_recv, dg_send, dg_recv):
    tok, dim = xg.shape[2], xg.shape[3]
    ff = wd.shape[1]
    cap = tok // 2
    _, row, col, core = coords()
    me, at_x, at_y, at_d = number(0), number(2), number(4), number(6)
    tokens = (xg, dyg)
    PART = 6

    announce()
    tables = [pltpu.make_async_copy(src, dst, tab_sem.at[i]) for i, (src, dst) in enumerate(((route_hbm, route_tab), (gate_hbm, gate_tab)))]
    own = [[pltpu.make_async_copy(src.at[mb], dst.at[mb, me], own_sem.at[mb, i]) for i, (src, dst) in enumerate(((x_hbm, xg), (dy_hbm, dyg)))] for mb in range(2)]
    weights = [
        pltpu.make_async_copy(wg_hbm, wgu.at[:, :, pl.ds(0, ff)], w_sem.at[0]),
        pltpu.make_async_copy(wu_hbm, wgu.at[:, :, pl.ds(ff, ff)], w_sem.at[1]),
        pltpu.make_async_copy(wd_hbm, wd, w_sem.at[2]),
    ]
    for load in tables + own[0] + own[1] + weights:
        load.start()
    for load in tables:
        load.wait()
    rt[me] = jnp.zeros(rt.shape[1:], F32)
    for mb in range(2):
        rt[me, pl.ds(mb * 2 * TOPK, TOPK), pl.ds(0, tok)] = route_tab[mb].astype(F32)
        rt[me, pl.ds(mb * 2 * TOPK + TOPK, TOPK), pl.ds(0, tok)] = gate_tab[mb]
    all_entered()

    def tok_copy(mb, kind):
        if kind < PART:
            slot, mask = (me, 2) if kind in (0, 1) else (me, 4) if kind in (3, 4) else ((at_x, 4), (at_y, 2))[mb]
            which = int(kind in (1, 2, 4))
        else:
            which, slot, mask = (kind - PART) % 2, (me, at_x, at_y, at_d)[(kind - PART) // 2], 1
        ref = tokens[which].at[mb, slot]
        arrival = mb * PART + kind if kind < PART else PAIR[mb, kind]
        return remote(ref, ref, g_send.at[which], g_recv.at[arrival], mask)

    def await_pair(mb, kind):
        which = (kind - PART) % 2
        two = tokens[which].at[0, pl.ds(0, 2)]
        remote(two, two, g_send.at[which], g_recv.at[PAIR[mb, kind]], 1).wait_recv()

    def send_own(mb, *kinds):
        for kind in kinds:
            tok_copy(mb, kind).start()

    def relay(mb, kind, *then):
        tok_copy(mb, kind).wait_recv()
        for nxt in then:
            tok_copy(mb, nxt).start()

    def rt_copy(kind):
        slot, mask = ((me, 1), (me, 2), (me, 4), (at_x, 4), (at_x, 1), (at_y, 1), (at_d, 1))[kind]
        return remote(rt.at[slot], rt.at[slot], rt_send.at[0], rt_recv.at[kind], mask)

    def rt_relay(kind, *then):
        rt_copy(kind).wait_recv()
        for nxt in then:
            rt_copy(nxt).start()

    FIRST, SECOND = (2, 4), (4, 2)
    half = tok // 2

    def to_partner(q, unit, mb, mask):
        r, i = q * 2 + mb, mask // 2
        return remote(part.at[r, i, 1 - core], near_in.at[r, i], d_send.at[0], d_recv.at[q, unit], 1)

    def partner_start(q, unit):
        for mb, mask in CHIPS[unit]:
            to_partner(q, unit, mb, mask).start()

    def rows_of(h):
        return pl.ds(h * half, half)

    def first(q, mb, h, which):
        r = q * 2 + mb
        src = chip_sum.at[r, (3, FIRST[h] // 2)[which], rows_of(h)]
        return remote(src, first_in.at[r, which, h], f_send.at[0], f_recv.at[r, which], FIRST[h])

    def second(q, mb, h):
        r = q * 2 + mb
        return remote(chip_sum.at[r, SECOND[h] // 2, rows_of(h)], second_in.at[r, h], s_send.at[0], s_recv.at[r], SECOND[h])

    def await_both(ref, sem):
        remote(ref, ref, s_send.at[0], sem, 2).wait_recv()

    def leave(q, unit):
        two = near_in.at[0, pl.ds(0, 2)]
        remote(two, two, d_send.at[0], d_recv.at[q, unit], 1).wait_recv()
        for mb, mask in CHIPS[unit]:
            r, i = q * 2 + mb, mask // 2
            chip_sum[r, i] = part[r, i, core] + near_in[r, i]
            for h in range(2):
                if mask in (6, FIRST[h]):
                    first(q, mb, h, 0 if mask == 6 else 1).start()

    def second_send(q, mb):
        r = q * 2 + mb
        await_both(first_in.at[r, 0], f_recv.at[r, 0])
        for h in range(2):
            chip_sum[r, SECOND[h] // 2, rows_of(h), :] += first_in[r, 0, h]
            second(q, mb, h).start()

    def finish(q, mb):
        r = q * 2 + mb
        await_both(first_in.at[r, 1], f_recv.at[r, 1])
        await_both(second_in.at[r], s_recv.at[r])
        for h in range(2):
            done = chip_sum[r, 0, rows_of(h), :] + first_in[r, 1, h] + second_in[r, h]
            (y_ref, dx_ref)[q][mb, rows_of(h), :] = done.astype(BF)

    first_id = (me * NEXP).astype(F32)
    slot_iota = lax.broadcasted_iota(jnp.int32, (cap, tok), 0).astype(F32)

    def block_of(mask, c):
        return number(mask) - core + c

    before = lax.broadcasted_iota(jnp.int32, (tok, tok), 0) < lax.broadcasted_iota(jnp.int32, (tok, tok), 1)

    def make_ranks(mask):
        tables = rt[pl.ds(number(mask) - core, 2)]
        members, weights_of = [], []
        for mb in range(2):
            at = mb * 2 * TOPK
            routes, gates = tables[:, at : at + TOPK, :tok], tables[:, at + TOPK : at + 2 * TOPK, :tok]
            for l in range(NEXP):
                hit = routes == first_id + l
                members.append(jnp.sum(jnp.where(hit, 1.0, 0.0), axis=1))
                weights_of.append(jnp.sum(jnp.where(hit, gates, 0.0), axis=1))
        member = jnp.concatenate(members, axis=0)
        rank[mask // 2] = jnp.where(member > 0, dot(member.astype(BF), jnp.where(before, 1.0, 0.0).astype(BF)), -1.0)
        grow[mask // 2] = jnp.concatenate(weights_of, axis=0)

    def dispatch_x(unit):
        for b, (mb, mask, c) in enumerate(BLOCKS[unit]):
            lines = [pl.ds((mb * NEXP + l) * 2 + c, 1) for l in range(NEXP)]
            hot = jnp.concatenate([jnp.where(rank[mask // 2, line, :] == slot_iota, 1.0, 0.0) for line in lines], axis=0)
            gs = jnp.concatenate([jnp.broadcast_to(grow[mask // 2, line, :], (cap, tok)) for line in lines], axis=0)
            gate = jnp.sum(hot * gs, axis=1, keepdims=True)
            hot = hot.astype(BF)
            disp[unit, b] = hot
            gblk[unit, b] = gate
            xs = dot(hot, xg[mb, block_of(mask, c)]).astype(BF)
            rows = pl.ds(b * cap, cap)
            for l in range(NEXP):
                xr[l, unit, rows, :] = xs[l * cap : (l + 1) * cap]
                gcol[l, unit, rows, :] = gate[l * cap : (l + 1) * cap]

    def forward(u, between=lambda: None, early=lambda: None, at=2):
        def spread(l, out):
            z = gcol[l, u] * out.astype(F32)
            hi = z.astype(BF)
            rest = z - hi.astype(F32)
            mid = rest.astype(BF)
            low = (rest - mid.astype(F32)).astype(BF)
            for b in range(QUAD):
                for i, piece in enumerate((hi, mid, low)):
                    zbuf[b, pl.ds((i * NEXP + l) * cap, cap), :] = piece[b * cap : (b + 1) * cap]

        both, out = dot(xr[0, u], wgu[0]).astype(BF), None
        for l in range(NEXP):
            ahead = dot(xr[l + 1, u], wgu[l + 1]).astype(BF) if l + 1 < NEXP else None
            uv[l, u] = both
            both = both.astype(F32)
            gate_pre, up_pre = both[:, :ff], both[:, ff:]
            hidden = (gate_pre * jax.nn.sigmoid(gate_pre) * up_pre).astype(BF)
            hid[l, u] = hidden
            if out is not None:
                spread(l - 1, out)
            out = dot(hidden, wd[l]).astype(BF)
            outs[l, u] = out
            both = ahead
            if l == at:
                early()
        spread(NEXP - 1, out)

        between()

        for b, (mb, mask, c) in enumerate(BLOCKS[u]):
            part[Y * 2 + mb, mask // 2, c] = tdot(jnp.concatenate([disp[u, b]] * 3, axis=0), zbuf[b])

    def dispatch_dy(unit):
        for b, (mb, mask, c) in enumerate(BLOCKS[unit]):
            blk = block_of(mask, c)
            hot = disp[unit, b]
            dys = dot(hot, dyg[mb, blk])
            qs = (gblk[unit, b] * dys).astype(BF)
            rows = pl.ds(b * cap, cap)
            hot_f = hot.astype(F32)
            routes = rt[blk, mb * 2 * TOPK : mb * 2 * TOPK + TOPK, 0:tok]
            total = jnp.zeros((TOPK, tok), F32)
            for l in range(NEXP):
                cut = slice(l * cap, (l + 1) * cap)
                qr[l, unit, rows, :] = qs[cut]
                dots = jnp.sum(dys[cut] * outs[l, unit, rows, :].astype(F32), axis=1, keepdims=True)
                line = jnp.sum(hot_f[cut] * dots, axis=0, keepdims=True)
                total = total + jnp.where(routes == first_id + l, line, 0.0)
            dg[blk, pl.ds(mb * TOPK, TOPK), pl.ds(0, tok)] = total

    def backward(u, between=lambda: None, early=lambda: None):
        back = ndot(qr[0, u], wd[0])
        for l in range(NEXP):
            ahead = ndot(qr[l + 1, u], wd[l + 1]) if l + 1 < NEXP else None
            both = uv[l, u].astype(F32)
            gate_pre, up_pre = both[:, :ff], both[:, ff:]
            sig = jax.nn.sigmoid(gate_pre)
            d_up = (back * gate_pre * sig).astype(BF)
            d_gate = (back * up_pre * sig * (1.0 + gate_pre * (1.0 - sig))).astype(BF)
            d_both = jnp.concatenate([d_gate, d_up], axis=1)
            uv[l, u] = d_both
            d_in = ndot(d_both, wgu[l]).astype(BF)
            for b in range(QUAD):
                pbuf[b, pl.ds(l * cap, cap), :] = d_in[b * cap : (b + 1) * cap]
            back = ahead
            if l == 1:
                early()

        between()

        for b, (mb, mask, c) in enumerate(BLOCKS[u]):
            part[DX * 2 + mb, mask // 2, c] = tdot(disp[u, b], pbuf[b])

    def weight_grads(l):
        rows = 2 * 2 * QUAD * cap
        gd_ref[l] = tdot(hid[l].reshape(rows, ff), qr[l].reshape(rows, dim))
        xs, d_both = xr[l].reshape(rows, dim), uv[l].reshape(rows, 2 * ff)
        grads = tdot(xs, d_both)
        gg_ref[l] = grads[:, :ff]
        gu_ref[l] = grads[:, ff:]

    def dg_copy(mask):
        return remote(dg.at[number(mask)], dg_in.at[me], dg_send.at[0], dg_recv.at[0], mask)

    for kind in range(3):
        rt_copy(kind).start()
    for mb in range(2):
        own[mb][0].wait()
        send_own(mb, 6, 0, 3)
    own[0][1].wait()
    send_own(0, 7, 1)
    own[1][1].wait()
    send_own(1, 7)
    rt_relay(0)
    make_ranks(0)
    for load in weights:
        load.wait()
    await_pair(0, 6)
    dispatch_x(OWN)

    def during():
        rt_relay(1, 3, 4)
        rt_relay(2, 5)

    forward(OWN, lambda: None, during)
    partner_start(Y, OWN)

    relay(0, 0, 5, 8)
    send_own(1, 4)
    relay(0, 3, 10)
    rt_relay(4)
    rt_relay(5)
    make_ranks(2)
    make_ranks(4)
    await_pair(0, 7)
    dispatch_dy(OWN)
    relay(1, 3, 5, 10)
    relay(1, 0, 8)
    send_own(1, 1)
    send_own(0, 4)
    rt_relay(3, 6)
    await_pair(0, 8)
    dispatch_x(XY0)
    forward(XY0, lambda: relay(0, 1, 2, 9))
    partner_start(Y, XY0)

    rt_relay(6)
    make_ranks(6)
    relay(0, 5, 12)
    await_pair(1, 8)
    dispatch_x(XY1)

    def during():
        relay(1, 5, 12)
        relay(1, 4, 2, 11)
        leave(Y, XY0)

    forward(XY1, lambda: None, during, 1)
    partner_start(Y, XY1)

    await_pair(0, 12)
    dispatch_x(DIAG)
    relay(0, 4, 11)
    relay(1, 1, 9)

    def during():
        leave(Y, XY1)
        relay(0, 2, 13)

    forward(DIAG, lambda: None, during)
    partner_start(Y, DIAG)

    relay(1, 2, 13)
    await_pair(0, 9)
    dispatch_dy(XY0)
    leave(Y, DIAG)
    await_pair(0, 13)
    dispatch_dy(DIAG)
    backward(DIAG)
    partner_start(DX, DIAG)

    await_pair(1, 9)
    dispatch_dy(XY1)
    for mask in range(1, NBLK):
        dg_copy(mask).start()
    dg_in[me] = dg[me]
    leave(DX, DIAG)
    backward(XY0, lambda: leave(Y, OWN))
    partner_start(DX, XY0)

    def during():
        second_send(Y, 0)
        second_send(Y, 1)

    backward(XY1, lambda: leave(DX, XY0), during)
    partner_start(DX, XY1)

    backward(OWN, lambda: leave(DX, XY1))
    partner_start(DX, OWN)
    weight_grads(0)
    second_send(DX, 0)
    second_send(DX, 1)
    leave(DX, OWN)
    weight_grads(1)
    weight_grads(2)
    weight_grads(3)
    finish(Y, 0)
    finish(Y, 1)
    seven = dg_in.at[pl.ds(0, NBLK - 1)]
    others = remote(seven, seven, dg_send.at[0], dg_recv.at[0], 1)
    others.wait_recv()
    others.wait_send()
    grads = jnp.sum(dg_in[...], axis=0)
    for mb in range(2):
        gates_ref[mb] = grads[mb * TOPK : (mb + 1) * TOPK, :tok]
    def sent(ref, sem):
        remote(ref, ref, sem, s_recv.at[0], 1).wait_send()

    sent(rt.at[pl.ds(0, 7)], rt_send.at[0])
    for which in range(2):
        sent(tokens[which].at[:, pl.ds(0, 7)], g_send.at[which])
    sent(near_in, d_send.at[0])
    sent(first_in, f_send.at[0])
    finish(DX, 0)
    finish(DX, 1)
    sent(second_in, s_send.at[0])


def layer(x, grad_y, route_rows, gate_rows, w_gate, w_up, w_down):
    _, tok, dim = x.shape
    ff = w_gate.shape[2]
    cap = tok // 2
    hbm, vmem = pl.BlockSpec(memory_space=pltpu.HBM), pl.BlockSpec(memory_space=pltpu.VMEM)
    dma = pltpu.SemaphoreType.DMA
    unit = QUAD * cap
    shape = jax.ShapeDtypeStruct
    return pl.pallas_call(
        layer_kernel,
        out_shape=(
            shape((2, tok, dim), BF), shape((2, tok, dim), BF), shape((2, TOPK, tok), F32),
            shape(w_gate.shape, F32), shape(w_up.shape, F32), shape(w_down.shape, F32),
        ),
        in_specs=[hbm] * 7,
        out_specs=(vmem,) * 6,
        scratch_shapes=[
            pltpu.VMEM((2, NBLK, tok, dim), BF),
            pltpu.VMEM((2, NBLK, tok, dim), BF),
            pltpu.VMEM((NBLK, 4 * TOPK, LANES), F32),
            pltpu.VMEM((2, TOPK, tok), jnp.int32),
            pltpu.VMEM((2, TOPK, tok), F32),
            pltpu.VMEM((NEXP, dim, 2 * ff), BF),
            pltpu.VMEM((NEXP, ff, dim), BF),
            pltpu.VMEM((4, 4 * NEXP, tok), F32),
            pltpu.VMEM((4, 4 * NEXP, tok), F32),
            pltpu.VMEM((4, QUAD, NEXP * cap, tok), BF),
            pltpu.VMEM((4, QUAD, NEXP * cap, 1), F32),
            pltpu.VMEM((NEXP, 4, unit, 1), F32),
            pltpu.VMEM((NEXP, 4, unit, dim), BF),
            pltpu.VMEM((NEXP, 4, unit, dim), BF),
            pltpu.VMEM((NEXP, 4, unit, 2 * ff), BF),
            pltpu.VMEM((NEXP, 4, unit, ff), BF),
            pltpu.VMEM((NEXP, 4, unit, dim), BF),
            pltpu.VMEM((QUAD, 3 * NEXP * cap, dim), BF),
            pltpu.VMEM((QUAD, NEXP * cap, dim), BF),
            pltpu.VMEM((NBLK, 2 * TOPK, LANES), F32),
            pltpu.VMEM((4, 4, 2, tok, dim), F32),
            pltpu.VMEM((4, 4, tok, dim), F32),
            pltpu.VMEM((4, 4, tok, dim), F32),
            pltpu.VMEM((4, 2, 2, tok // 2, dim), F32),
            pltpu.VMEM((4, 2, tok // 2, dim), F32),
            pltpu.VMEM((NBLK, 2 * TOPK, LANES), F32),
            dma((2,)), dma((2, 2)), dma((3,)), dma((2,)), dma((20,)), dma((1,)), dma((7,)),
            dma((1,)), dma((2, 4)), dma((1,)), dma((4, 2)), dma((1,)), dma((4,)), dma((1,)), dma((1,)),
        ],
        compiler_params=pltpu.CompilerParams(collective_id=0, has_side_effects=True, vmem_limit_bytes=46 << 20),
        name="moe_layer",
    )(x, grad_y, route_rows, gate_rows, w_gate, w_up, w_down)


def flush_kernel(*refs):
    count = (len(refs) - 1) // 2
    sem = refs[-1]
    copies = [pltpu.make_async_copy(refs[i], refs[count + i], sem.at[i]) for i in range(count)]
    for copy in reversed(copies):
        copy.start()
    for copy in copies:
        copy.wait()


def flush(arrays):
    hbm, vmem = pl.BlockSpec(memory_space=pltpu.HBM), pl.BlockSpec(memory_space=pltpu.VMEM)
    return pl.pallas_call(
        flush_kernel,
        out_shape=tuple(jax.ShapeDtypeStruct(arr.shape, arr.dtype) for arr in arrays),
        in_specs=[vmem] * len(arrays),
        out_specs=(hbm,) * len(arrays),
        scratch_shapes=[pltpu.SemaphoreType.DMA((len(arrays),))],
        compiler_params=pltpu.CompilerParams(vmem_limit_bytes=12 << 20),
        name="write_out",
    )(*arrays)


def solution(mesh):
    tok_spec = P(None, ALL_AXES, None)
    w_spec = P(ALL_AXES, None, None)

    def moe_layer(x, route_idx, gates, w_gate, w_up, w_down, grad_y):
        stay = lambda arr: pltpu.with_memory_space_constraint(arr, pltpu.HBM)
        flat = lambda arr: jnp.transpose(arr, (0, 2, 1))
        args = [stay(arr) for arr in (x, grad_y, flat(route_idx), flat(gates), w_gate, w_up, w_down)]
        y, dx, g_gates, g_gate, g_up, g_down = flush(layer(*args))
        return y, dx, flat(g_gates), g_gate, g_up, g_down

    return jax.shard_map(moe_layer, mesh=mesh, in_specs=(tok_spec, tok_spec, tok_spec, w_spec, w_spec, w_spec, tok_spec), out_specs=(tok_spec, tok_spec, tok_spec, w_spec, w_spec, w_spec), check_vma=False)
```

```python
import functools

import jax
import jax.numpy as jnp
from jax import lax
from jax.experimental import pallas as pl
from jax.experimental.pallas import tpu as pltpu
from jax.sharding import PartitionSpec as P

ALL_AXES = ("rep", "row", "col", "core")
MESH = pl.DeviceIdType.MESH
BF = jnp.bfloat16
F32 = jnp.float32
NBLK = 8
QUAD = 4
NEXP = 4
TOPK = 4
LANES = 128
OWN, XY0, XY1, DIAG = 0, 1, 2, 3
Y, DX = 0, 1


def coords():
    return (lax.axis_index("rep"), lax.axis_index("row"), lax.axis_index("col"), lax.axis_index("core"))


def peer(mask):
    rep, row, col, core = coords()
    flip = lambda pos, bit: 1 - pos if mask & bit else pos
    return (rep, flip(row, 4), flip(col, 2), flip(core, 1))


def number(mask=0):
    _, row, col, core = peer(mask)
    return row * 4 + col * 2 + core


def announce():
    barrier = pltpu.get_barrier_semaphore()
    for mask in range(1, NBLK):
        pl.semaphore_signal(barrier, inc=1, device_id=peer(mask), device_id_type=MESH)


def all_entered():
    pl.semaphore_wait(pltpu.get_barrier_semaphore(), NBLK - 1)


def remote(src, dst, send_sem, recv_sem, mask):
    return pltpu.make_async_remote_copy(src_ref=src, dst_ref=dst, send_sem=send_sem, recv_sem=recv_sem, device_id=peer(mask), device_id_type=MESH)


def tdot(lhs, rhs):
    return lax.dot_general(lhs, rhs, (((0,), (0,)), ((), ())), preferred_element_type=F32)


def ndot(lhs, rhs):
    return lax.dot_general(lhs, rhs, (((1,), (1,)), ((), ())), preferred_element_type=F32)


def dot(lhs, rhs):
    return jnp.dot(lhs, rhs, preferred_element_type=F32)


CHIPS = {
    OWN: ((0, 0), (1, 0)),
    XY0: ((0, 2), (0, 4)),
    XY1: ((1, 4), (1, 2)),
    DIAG: ((0, 6), (1, 6)),
}
BLOCKS = {unit: tuple((mb, mask, c) for mb, mask in chips for c in range(2)) for unit, chips in CHIPS.items()}


PAIRS = (
    ((0, 6), (1, 6)), ((0, 7), (1, 7)), ((0, 8), (0, 10)), ((1, 8), (1, 10)),
    ((0, 9), (0, 11)), ((1, 9), (1, 11)), ((0, 12), (1, 12)), ((0, 13), (1, 13)),
)
PAIR = {item: 12 + i for i, pair in enumerate(PAIRS) for item in pair}


def layer_kernel(x_hbm, dy_hbm, route_hbm, gate_hbm, wg_hbm, wu_hbm, wd_hbm,
                 y_ref, dx_ref, gates_ref, gg_ref, gu_ref, gd_ref,
                 xg, dyg, rt, route_tab, gate_tab, wgu, wd, rank, grow, disp, gblk, gcol, xr, qr, uv, hid, outs, zbuf, pbuf, dg,
                 part, near_in, chip_sum, first_in, second_in, dg_in, dg_near, dg_sum,
                 tab_sem, own_sem, w_sem, g_send, g_recv, rt_send, rt_recv, d_send, d_recv, f_send, f_recv, s_send, s_recv, dg_send, dg_recv):
    tok, dim = xg.shape[2], xg.shape[3]
    ff = wd.shape[1]
    cap = tok // 2
    _, row, col, core = coords()
    me, at_x, at_y, at_d = number(0), number(2), number(4), number(6)
    tokens = (xg, dyg)
    PART = 6

    announce()
    tables = [pltpu.make_async_copy(src, dst, tab_sem.at[i]) for i, (src, dst) in enumerate(((route_hbm, route_tab), (gate_hbm, gate_tab)))]
    own = [[pltpu.make_async_copy(src.at[mb], dst.at[mb, me], own_sem.at[mb, i]) for i, (src, dst) in enumerate(((x_hbm, xg), (dy_hbm, dyg)))] for mb in range(2)]
    weights = [
        pltpu.make_async_copy(wg_hbm, wgu.at[:, :, pl.ds(0, ff)], w_sem.at[0]),
        pltpu.make_async_copy(wu_hbm, wgu.at[:, :, pl.ds(ff, ff)], w_sem.at[1]),
        pltpu.make_async_copy(wd_hbm, wd, w_sem.at[2]),
    ]
    for load in tables + own[0] + own[1] + weights:
        load.start()
    for load in tables:
        load.wait()
    rt[me] = jnp.zeros(rt.shape[1:], F32)
    for mb in range(2):
        rt[me, pl.ds(mb * 2 * TOPK, TOPK), pl.ds(0, tok)] = route_tab[mb].astype(F32)
        rt[me, pl.ds(mb * 2 * TOPK + TOPK, TOPK), pl.ds(0, tok)] = gate_tab[mb]
    all_entered()

    def tok_copy(mb, kind):
        if kind < PART:
            slot, mask = (me, 2) if kind in (0, 1) else (me, 4) if kind in (3, 4) else ((at_x, 4), (at_y, 2))[mb]
            which = int(kind in (1, 2, 4))
        else:
            which, slot, mask = (kind - PART) % 2, (me, at_x, at_y, at_d)[(kind - PART) // 2], 1
        ref = tokens[which].at[mb, slot]
        arrival = mb * PART + kind if kind < PART else PAIR[mb, kind]
        return remote(ref, ref, g_send.at[which], g_recv.at[arrival], mask)

    def await_pair(mb, kind):
        which = (kind - PART) % 2
        two = tokens[which].at[0, pl.ds(0, 2)]
        remote(two, two, g_send.at[which], g_recv.at[PAIR[mb, kind]], 1).wait_recv()

    def send_own(mb, *kinds):
        for kind in kinds:
            tok_copy(mb, kind).start()

    def relay(mb, kind, *then):
        tok_copy(mb, kind).wait_recv()
        for nxt in then:
            tok_copy(mb, nxt).start()

    def rt_copy(kind):
        slot, mask = ((me, 1), (me, 2), (me, 4), (at_x, 4), (at_x, 1), (at_y, 1), (at_d, 1))[kind]
        return remote(rt.at[slot], rt.at[slot], rt_send.at[0], rt_recv.at[kind], mask)

    def rt_relay(kind, *then):
        rt_copy(kind).wait_recv()
        for nxt in then:
            rt_copy(nxt).start()

    FIRST, SECOND = (2, 4), (4, 2)
    half = tok // 2

    def to_partner(q, unit, mb, mask):
        r, i = q * 2 + mb, mask // 2
        return remote(part.at[r, i, 1 - core], near_in.at[r, i], d_send.at[0], d_recv.at[q, unit], 1)

    def partner_start(q, unit):
        for mb, mask in CHIPS[unit]:
            to_partner(q, unit, mb, mask).start()

    def rows_of(h):
        return pl.ds(h * half, half)

    def first(q, mb, h, which):
        r = q * 2 + mb
        src = chip_sum.at[r, (3, FIRST[h] // 2)[which], rows_of(h)]
        return remote(src, first_in.at[r, which, h], f_send.at[0], f_recv.at[r, which], FIRST[h])

    def second(q, mb, h):
        r = q * 2 + mb
        return remote(chip_sum.at[r, SECOND[h] // 2, rows_of(h)], second_in.at[r, h], s_send.at[0], s_recv.at[r], SECOND[h])

    def await_both(ref, sem):
        remote(ref, ref, s_send.at[0], sem, 2).wait_recv()

    def leave(q, unit):
        two = near_in.at[0, pl.ds(0, 2)]
        remote(two, two, d_send.at[0], d_recv.at[q, unit], 1).wait_recv()
        for mb, mask in CHIPS[unit]:
            r, i = q * 2 + mb, mask // 2
            chip_sum[r, i] = part[r, i, core] + near_in[r, i]
            for h in range(2):
                if mask in (6, FIRST[h]):
                    first(q, mb, h, 0 if mask == 6 else 1).start()

    def second_send(q, mb):
        r = q * 2 + mb
        await_both(first_in.at[r, 0], f_recv.at[r, 0])
        for h in range(2):
            chip_sum[r, SECOND[h] // 2, rows_of(h), :] += first_in[r, 0, h]
            second(q, mb, h).start()

    def finish(q, mb):
        r = q * 2 + mb
        await_both(first_in.at[r, 1], f_recv.at[r, 1])
        await_both(second_in.at[r], s_recv.at[r])
        for h in range(2):
            done = chip_sum[r, 0, rows_of(h), :] + first_in[r, 1, h] + second_in[r, h]
            (y_ref, dx_ref)[q][mb, rows_of(h), :] = done.astype(BF)

    first_id = (me * NEXP).astype(F32)
    slot_iota = lax.broadcasted_iota(jnp.int32, (cap, tok), 0).astype(F32)

    def block_of(mask, c):
        return number(mask) - core + c

    before = lax.broadcasted_iota(jnp.int32, (tok, tok), 0) < lax.broadcasted_iota(jnp.int32, (tok, tok), 1)

    def make_ranks(mask):
        tables = rt[pl.ds(number(mask) - core, 2)]
        members, weights_of = [], []
        for mb in range(2):
            at = mb * 2 * TOPK
            routes, gates = tables[:, at : at + TOPK, :tok], tables[:, at + TOPK : at + 2 * TOPK, :tok]
            for l in range(NEXP):
                hit = routes == first_id + l
                members.append(jnp.sum(jnp.where(hit, 1.0, 0.0), axis=1))
                weights_of.append(jnp.sum(jnp.where(hit, gates, 0.0), axis=1))
        member = jnp.concatenate(members, axis=0)
        rank[mask // 2] = jnp.where(member > 0, dot(member.astype(BF), jnp.where(before, 1.0, 0.0).astype(BF)), -1.0)
        grow[mask // 2] = jnp.concatenate(weights_of, axis=0)

    def dispatch_x(unit):
        for b, (mb, mask, c) in enumerate(BLOCKS[unit]):
            lines = [pl.ds((mb * NEXP + l) * 2 + c, 1) for l in range(NEXP)]
            hot = jnp.concatenate([jnp.where(rank[mask // 2, line, :] == slot_iota, 1.0, 0.0) for line in lines], axis=0)
            gs = jnp.concatenate([jnp.broadcast_to(grow[mask // 2, line, :], (cap, tok)) for line in lines], axis=0)
            gate = jnp.sum(hot * gs, axis=1, keepdims=True)
            hot = hot.astype(BF)
            disp[unit, b] = hot
            gblk[unit, b] = gate
            xs = dot(hot, xg[mb, block_of(mask, c)]).astype(BF)
            rows = pl.ds(b * cap, cap)
            for l in range(NEXP):
                xr[l, unit, rows, :] = xs[l * cap : (l + 1) * cap]
                gcol[l, unit, rows, :] = gate[l * cap : (l + 1) * cap]

    def forward(u, between=lambda: None, early=lambda: None):
        def spread(l, out):
            z = gcol[l, u] * out.astype(F32)
            hi = z.astype(BF)
            rest = z - hi.astype(F32)
            mid = rest.astype(BF)
            low = (rest - mid.astype(F32)).astype(BF)
            for b in range(QUAD):
                for i, piece in enumerate((hi, mid, low)):
                    zbuf[b, pl.ds((i * NEXP + l) * cap, cap), :] = piece[b * cap : (b + 1) * cap]

        both, out = dot(xr[0, u], wgu[0]).astype(BF), None
        for l in range(NEXP):
            ahead = dot(xr[l + 1, u], wgu[l + 1]).astype(BF) if l + 1 < NEXP else None
            uv[l, u] = both
            both = both.astype(F32)
            gate_pre, up_pre = both[:, :ff], both[:, ff:]
            hidden = (gate_pre * jax.nn.sigmoid(gate_pre) * up_pre).astype(BF)
            hid[l, u] = hidden
            if out is not None:
                spread(l - 1, out)
            out = dot(hidden, wd[l]).astype(BF)
            outs[l, u] = out
            both = ahead
            if l == 2:
                early()
        spread(NEXP - 1, out)

        between()

        for b, (mb, mask, c) in enumerate(BLOCKS[u]):
            part[Y * 2 + mb, mask // 2, c] = tdot(jnp.concatenate([disp[u, b]] * 3, axis=0), zbuf[b])

    def dispatch_dy(unit):
        for b, (mb, mask, c) in enumerate(BLOCKS[unit]):
            blk = block_of(mask, c)
            hot = disp[unit, b]
            dys = dot(hot, dyg[mb, blk])
            qs = (gblk[unit, b] * dys).astype(BF)
            rows = pl.ds(b * cap, cap)
            hot_f = hot.astype(F32)
            routes = rt[blk, mb * 2 * TOPK : mb * 2 * TOPK + TOPK, 0:tok]
            total = jnp.zeros((TOPK, tok), F32)
            for l in range(NEXP):
                cut = slice(l * cap, (l + 1) * cap)
                qr[l, unit, rows, :] = qs[cut]
                dots = jnp.sum(dys[cut] * outs[l, unit, rows, :].astype(F32), axis=1, keepdims=True)
                line = jnp.sum(hot_f[cut] * dots, axis=0, keepdims=True)
                total = total + jnp.where(routes == first_id + l, line, 0.0)
            dg[blk, pl.ds(mb * TOPK, TOPK), pl.ds(0, tok)] = total

    def backward(u, between=lambda: None, early=lambda: None):
        back = ndot(qr[0, u], wd[0])
        for l in range(NEXP):
            ahead = ndot(qr[l + 1, u], wd[l + 1]) if l + 1 < NEXP else None
            both = uv[l, u].astype(F32)
            gate_pre, up_pre = both[:, :ff], both[:, ff:]
            sig = jax.nn.sigmoid(gate_pre)
            d_up = (back * gate_pre * sig).astype(BF)
            d_gate = (back * up_pre * sig * (1.0 + gate_pre * (1.0 - sig))).astype(BF)
            d_both = jnp.concatenate([d_gate, d_up], axis=1)
            uv[l, u] = d_both
            d_in = ndot(d_both, wgu[l]).astype(BF)
            for b in range(QUAD):
                pbuf[b, pl.ds(l * cap, cap), :] = d_in[b * cap : (b + 1) * cap]
            back = ahead
            if l == 1:
                early()

        between()

        for b, (mb, mask, c) in enumerate(BLOCKS[u]):
            part[DX * 2 + mb, mask // 2, c] = tdot(disp[u, b], pbuf[b])

    def weight_grads(l):
        rows = 2 * 2 * QUAD * cap
        gd_ref[l] = tdot(hid[l].reshape(rows, ff), qr[l].reshape(rows, dim))
        xs, d_both = xr[l].reshape(rows, dim), uv[l].reshape(rows, 2 * ff)
        grads = tdot(xs, d_both)
        gg_ref[l] = grads[:, :ff]
        gu_ref[l] = grads[:, ff:]

    def dg_copy(mask):
        return remote(dg_sum.at[mask // 2], dg_in.at[mask // 2], dg_send.at[1], dg_recv.at[1], mask)

    def dg_near_copy(mask):
        return remote(dg.at[number(mask | 1)], dg_near.at[mask // 2], dg_send.at[0], dg_recv.at[0], 1)

    for kind in range(3):
        rt_copy(kind).start()
    for mb in range(2):
        own[mb][0].wait()
        send_own(mb, 6, 0, 3)
    own[0][1].wait()
    send_own(0, 7, 1)
    own[1][1].wait()
    send_own(1, 7)
    rt_relay(0)
    make_ranks(0)
    for load in weights:
        load.wait()
    await_pair(0, 6)
    dispatch_x(OWN)

    def during():
        rt_relay(1, 3, 4)
        rt_relay(2, 5)

    forward(OWN, lambda: None, during)
    partner_start(Y, OWN)

    relay(0, 0, 5, 8)
    send_own(1, 4)
    relay(0, 3, 10)
    rt_relay(4)
    rt_relay(5)
    make_ranks(2)
    make_ranks(4)
    await_pair(0, 7)
    dispatch_dy(OWN)
    relay(1, 3, 5, 10)
    relay(1, 0, 8)
    send_own(1, 1)
    send_own(0, 4)
    await_pair(0, 8)
    dispatch_x(XY0)
    forward(XY0, lambda: relay(0, 1, 2, 9), lambda: rt_relay(3, 6))
    partner_start(Y, XY0)

    rt_relay(6)
    make_ranks(6)
    relay(0, 5, 12)
    await_pair(1, 8)
    dispatch_x(XY1)

    def during():
        relay(1, 5, 12)
        relay(1, 4, 2, 11)

    forward(XY1, lambda: leave(Y, XY0), during)
    partner_start(Y, XY1)

    await_pair(0, 12)
    dispatch_x(DIAG)
    relay(0, 4, 11)
    relay(1, 1, 9)

    def during():
        leave(Y, XY1)
        relay(0, 2, 13)

    forward(DIAG, lambda: None, during)
    partner_start(Y, DIAG)

    relay(1, 2, 13)
    await_pair(0, 9)
    dispatch_dy(XY0)
    leave(Y, DIAG)
    await_pair(0, 13)
    dispatch_dy(DIAG)
    backward(DIAG)
    partner_start(DX, DIAG)

    await_pair(1, 9)
    dispatch_dy(XY1)
    for mask in (0, 2, 4, 6):
        dg_near_copy(mask).start()
    leave(DX, DIAG)
    remote(dg_near, dg_near, dg_send.at[0], dg_recv.at[0], 1).wait_recv()
    for mask in (0, 2, 4, 6):
        dg_sum[mask // 2] = dg[number(mask)] + dg_near[mask // 2]
    for mask in (6, 2, 4):
        dg_copy(mask).start()
    backward(XY0, lambda: leave(Y, OWN))
    partner_start(DX, XY0)

    def during():
        second_send(Y, 0)
        second_send(Y, 1)

    backward(XY1, lambda: leave(DX, XY0), during)
    partner_start(DX, XY1)

    backward(OWN, lambda: leave(DX, XY1))
    partner_start(DX, OWN)
    weight_grads(0)
    second_send(DX, 0)
    second_send(DX, 1)
    leave(DX, OWN)
    weight_grads(1)
    weight_grads(2)
    weight_grads(3)
    finish(Y, 0)
    finish(Y, 1)
    remote(dg_near, dg_near, dg_send.at[0], dg_recv.at[0], 1).wait_send()
    three = dg_in.at[pl.ds(1, 3)]
    remote(three, three, dg_send.at[1], dg_recv.at[1], 2).wait()
    grads = dg_sum[0] + dg_in[1] + dg_in[2] + dg_in[3]
    for mb in range(2):
        gates_ref[mb] = grads[mb * TOPK : (mb + 1) * TOPK, :tok]
    def sent(ref, sem):
        remote(ref, ref, sem, s_recv.at[0], 1).wait_send()

    sent(rt.at[pl.ds(0, 7)], rt_send.at[0])
    for which in range(2):
        sent(tokens[which].at[:, pl.ds(0, 7)], g_send.at[which])
    sent(near_in, d_send.at[0])
    sent(first_in, f_send.at[0])
    finish(DX, 0)
    finish(DX, 1)
    sent(second_in, s_send.at[0])


def layer(x, grad_y, route_rows, gate_rows, w_gate, w_up, w_down):
    _, tok, dim = x.shape
    ff = w_gate.shape[2]
    cap = tok // 2
    hbm, vmem = pl.BlockSpec(memory_space=pltpu.HBM), pl.BlockSpec(memory_space=pltpu.VMEM)
    dma = pltpu.SemaphoreType.DMA
    unit = QUAD * cap
    shape = jax.ShapeDtypeStruct
    return pl.pallas_call(
        layer_kernel,
        out_shape=(
            shape((2, tok, dim), BF), shape((2, tok, dim), BF), shape((2, TOPK, tok), F32),
            shape(w_gate.shape, F32), shape(w_up.shape, F32), shape(w_down.shape, F32),
        ),
        in_specs=[hbm] * 7,
        out_specs=(vmem,) * 6,
        scratch_shapes=[
            pltpu.VMEM((2, NBLK, tok, dim), BF),
            pltpu.VMEM((2, NBLK, tok, dim), BF),
            pltpu.VMEM((NBLK, 4 * TOPK, LANES), F32),
            pltpu.VMEM((2, TOPK, tok), jnp.int32),
            pltpu.VMEM((2, TOPK, tok), F32),
            pltpu.VMEM((NEXP, dim, 2 * ff), BF),
            pltpu.VMEM((NEXP, ff, dim), BF),
            pltpu.VMEM((4, 4 * NEXP, tok), F32),
            pltpu.VMEM((4, 4 * NEXP, tok), F32),
            pltpu.VMEM((4, QUAD, NEXP * cap, tok), BF),
            pltpu.VMEM((4, QUAD, NEXP * cap, 1), F32),
            pltpu.VMEM((NEXP, 4, unit, 1), F32),
            pltpu.VMEM((NEXP, 4, unit, dim), BF),
            pltpu.VMEM((NEXP, 4, unit, dim), BF),
            pltpu.VMEM((NEXP, 4, unit, 2 * ff), BF),
            pltpu.VMEM((NEXP, 4, unit, ff), BF),
            pltpu.VMEM((NEXP, 4, unit, dim), BF),
            pltpu.VMEM((QUAD, 3 * NEXP * cap, dim), BF),
            pltpu.VMEM((QUAD, NEXP * cap, dim), BF),
            pltpu.VMEM((NBLK, 2 * TOPK, LANES), F32),
            pltpu.VMEM((4, 4, 2, tok, dim), F32),
            pltpu.VMEM((4, 4, tok, dim), F32),
            pltpu.VMEM((4, 4, tok, dim), F32),
            pltpu.VMEM((4, 2, 2, tok // 2, dim), F32),
            pltpu.VMEM((4, 2, tok // 2, dim), F32),
            pltpu.VMEM((4, 2 * TOPK, LANES), F32),
            pltpu.VMEM((4, 2 * TOPK, LANES), F32),
            pltpu.VMEM((4, 2 * TOPK, LANES), F32),
            dma((2,)), dma((2, 2)), dma((3,)), dma((2,)), dma((20,)), dma((1,)), dma((7,)),
            dma((1,)), dma((2, 4)), dma((1,)), dma((4, 2)), dma((1,)), dma((4,)), dma((2,)), dma((2,)),
        ],
        compiler_params=pltpu.CompilerParams(collective_id=0, has_side_effects=True, vmem_limit_bytes=46 << 20),
        name="moe_layer",
    )(x, grad_y, route_rows, gate_rows, w_gate, w_up, w_down)


def flush_kernel(*refs):
    count = (len(refs) - 1) // 2
    sem = refs[-1]
    copies = [pltpu.make_async_copy(refs[i], refs[count + i], sem.at[i]) for i in range(count)]
    for copy in reversed(copies):
        copy.start()
    for copy in copies:
        copy.wait()


def flush(arrays):
    hbm, vmem = pl.BlockSpec(memory_space=pltpu.HBM), pl.BlockSpec(memory_space=pltpu.VMEM)
    return pl.pallas_call(
        flush_kernel,
        out_shape=tuple(jax.ShapeDtypeStruct(arr.shape, arr.dtype) for arr in arrays),
        in_specs=[vmem] * len(arrays),
        out_specs=(hbm,) * len(arrays),
        scratch_shapes=[pltpu.SemaphoreType.DMA((len(arrays),))],
        compiler_params=pltpu.CompilerParams(vmem_limit_bytes=12 << 20),
        name="write_out",
    )(*arrays)


def solution(mesh):
    tok_spec = P(None, ALL_AXES, None)
    w_spec = P(ALL_AXES, None, None)

    def moe_layer(x, route_idx, gates, w_gate, w_up, w_down, grad_y):
        stay = lambda arr: pltpu.with_memory_space_constraint(arr, pltpu.HBM)
        flat = lambda arr: jnp.transpose(arr, (0, 2, 1))
        args = [stay(arr) for arr in (x, grad_y, flat(route_idx), flat(gates), w_gate, w_up, w_down)]
        y, dx, g_gates, g_gate, g_up, g_down = flush(layer(*args))
        return y, dx, flat(g_gates), g_gate, g_up, g_down

    return jax.shard_map(moe_layer, mesh=mesh, in_specs=(tok_spec, tok_spec, tok_spec, w_spec, w_spec, w_spec, tok_spec), out_specs=(tok_spec, tok_spec, tok_spec, w_spec, w_spec, w_spec), check_vma=False)
```

```python
import functools

import jax
import jax.numpy as jnp
from jax import lax
from jax.experimental import pallas as pl
from jax.experimental.pallas import tpu as pltpu
from jax.sharding import PartitionSpec as P

ALL_AXES = ("rep", "row", "col", "core")
MESH = pl.DeviceIdType.MESH
BF = jnp.bfloat16
F32 = jnp.float32
NBLK = 8
QUAD = 4
NEXP = 4
TOPK = 4
LANES = 128
OWN, XY0, XY1, DIAG = 0, 1, 2, 3
Y, DX = 0, 1


def coords():
    return (lax.axis_index("rep"), lax.axis_index("row"), lax.axis_index("col"), lax.axis_index("core"))


def peer(mask):
    rep, row, col, core = coords()
    flip = lambda pos, bit: 1 - pos if mask & bit else pos
    return (rep, flip(row, 4), flip(col, 2), flip(core, 1))


def number(mask=0):
    _, row, col, core = peer(mask)
    return row * 4 + col * 2 + core


def announce():
    barrier = pltpu.get_barrier_semaphore()
    for mask in range(1, NBLK):
        pl.semaphore_signal(barrier, inc=1, device_id=peer(mask), device_id_type=MESH)


def all_entered():
    pl.semaphore_wait(pltpu.get_barrier_semaphore(), NBLK - 1)


def remote(src, dst, send_sem, recv_sem, mask):
    return pltpu.make_async_remote_copy(src_ref=src, dst_ref=dst, send_sem=send_sem, recv_sem=recv_sem, device_id=peer(mask), device_id_type=MESH)


def tdot(lhs, rhs):
    return lax.dot_general(lhs, rhs, (((0,), (0,)), ((), ())), preferred_element_type=F32)


def ndot(lhs, rhs):
    return lax.dot_general(lhs, rhs, (((1,), (1,)), ((), ())), preferred_element_type=F32)


def dot(lhs, rhs):
    return jnp.dot(lhs, rhs, preferred_element_type=F32)


CHIPS = {
    OWN: ((0, 0), (1, 0)),
    XY0: ((0, 2), (0, 4)),
    XY1: ((1, 4), (1, 2)),
    DIAG: ((0, 6), (1, 6)),
}
BLOCKS = {unit: tuple((mb, mask, c) for mb, mask in chips for c in range(2)) for unit, chips in CHIPS.items()}


PAIRS = (
    ((0, 6), (1, 6)), ((0, 7), (1, 7)), ((0, 8), (0, 10)), ((1, 8), (1, 10)),
    ((0, 9), (0, 11)), ((1, 9), (1, 11)), ((0, 12), (1, 12)), ((0, 13), (1, 13)),
)
PAIR = {item: 12 + i for i, pair in enumerate(PAIRS) for item in pair}


def layer_kernel(x_hbm, dy_hbm, route_hbm, gate_hbm, wg_hbm, wu_hbm, wd_hbm,
                 y_ref, dx_ref, gates_ref, gg_ref, gu_ref, gd_ref,
                 xg, dyg, rt, route_tab, gate_tab, wgu, wd, rank, grow, disp, gblk, gcol, xr, qr, uv, hid, outs, zbuf, pbuf, dg,
                 part, near_in, chip_sum, first_in, second_in, dg_in, dg_near, dg_sum,
                 tab_sem, own_sem, w_sem, g_send, g_recv, rt_send, rt_recv, d_send, d_recv, f_send, f_recv, s_send, dg_send, dg_recv):
    tok, dim = xg.shape[2], xg.shape[3]
    ff = wd.shape[1]
    cap = tok // 2
    _, row, col, core = coords()
    me, at_x, at_y, at_d = number(0), number(2), number(4), number(6)
    tokens = (xg, dyg)
    PART = 6

    announce()
    tables = [pltpu.make_async_copy(src, dst, tab_sem.at[i]) for i, (src, dst) in enumerate(((route_hbm, route_tab), (gate_hbm, gate_tab)))]
    own = [[pltpu.make_async_copy(src.at[mb], dst.at[mb, me], own_sem.at[mb, i]) for i, (src, dst) in enumerate(((x_hbm, xg), (dy_hbm, dyg)))] for mb in range(2)]
    weights = [
        pltpu.make_async_copy(wg_hbm, wgu.at[:, :, pl.ds(0, ff)], w_sem.at[0]),
        pltpu.make_async_copy(wu_hbm, wgu.at[:, :, pl.ds(ff, ff)], w_sem.at[1]),
        pltpu.make_async_copy(wd_hbm, wd, w_sem.at[2]),
    ]
    for load in tables + own[0] + own[1] + weights:
        load.start()
    for load in tables:
        load.wait()
    rt[me] = jnp.zeros(rt.shape[1:], F32)
    for mb in range(2):
        rt[me, pl.ds(mb * 2 * TOPK, TOPK), pl.ds(0, tok)] = route_tab[mb].astype(F32)
        rt[me, pl.ds(mb * 2 * TOPK + TOPK, TOPK), pl.ds(0, tok)] = gate_tab[mb]
    all_entered()

    def tok_copy(mb, kind):
        if kind < PART:
            slot, mask = (me, 2) if kind in (0, 1) else (me, 4) if kind in (3, 4) else ((at_x, 4), (at_y, 2))[mb]
            which = int(kind in (1, 2, 4))
        else:
            which, slot, mask = (kind - PART) % 2, (me, at_x, at_y, at_d)[(kind - PART) // 2], 1
        ref = tokens[which].at[mb, slot]
        arrival = mb * PART + kind if kind < PART else PAIR[mb, kind]
        return remote(ref, ref, g_send.at[which], g_recv.at[arrival], mask)

    def await_pair(mb, kind):
        which = (kind - PART) % 2
        two = tokens[which].at[0, pl.ds(0, 2)]
        remote(two, two, g_send.at[which], g_recv.at[PAIR[mb, kind]], 1).wait_recv()

    def send_own(mb, *kinds):
        for kind in kinds:
            tok_copy(mb, kind).start()

    def relay(mb, kind, *then):
        tok_copy(mb, kind).wait_recv()
        for nxt in then:
            tok_copy(mb, nxt).start()

    def rt_copy(kind):
        slot, mask = ((me, 1), (me, 2), (me, 4), (at_x, 4), (at_x, 1), (at_y, 1), (at_d, 1))[kind]
        return remote(rt.at[slot], rt.at[slot], rt_send.at[0], rt_recv.at[kind], mask)

    def rt_relay(kind, *then):
        rt_copy(kind).wait_recv()
        for nxt in then:
            rt_copy(nxt).start()

    FIRST, SECOND = (2, 4), (4, 2)
    half = tok // 2

    def to_partner(q, unit, mb, mask):
        r, i = q * 2 + mb, mask // 2
        return remote(part.at[r, i, 1 - core], near_in.at[r, i], d_send.at[0], d_recv.at[q, unit], 1)

    def partner_start(q, unit):
        for mb, mask in CHIPS[unit]:
            to_partner(q, unit, mb, mask).start()

    def rows_of(h):
        return pl.ds(h * half, half)

    def first(q, mb, h, which):
        r = q * 2 + mb
        src = chip_sum.at[r, (3, FIRST[h] // 2)[which], rows_of(h)]
        return remote(src, first_in.at[r, which, h], f_send.at[0], f_recv.at[r, which], FIRST[h])

    def second(q, mb, h):
        r = q * 2 + mb
        return remote(chip_sum.at[r, SECOND[h] // 2, rows_of(h)], second_in.at[r, h], s_send.at[0], f_recv.at[r, 1], SECOND[h])

    def await_both(ref, sem):
        remote(ref, ref, s_send.at[0], sem, 2).wait_recv()

    def leave(q, unit):
        two = near_in.at[0, pl.ds(0, 2)]
        remote(two, two, d_send.at[0], d_recv.at[q, unit], 1).wait_recv()
        for mb, mask in CHIPS[unit]:
            r, i = q * 2 + mb, mask // 2
            chip_sum[r, i] = part[r, i, core] + near_in[r, i]
            for h in range(2):
                if mask in (6, FIRST[h]):
                    first(q, mb, h, 0 if mask == 6 else 1).start()

    def second_send(q, mb):
        r = q * 2 + mb
        await_both(first_in.at[r, 0], f_recv.at[r, 0])
        for h in range(2):
            chip_sum[r, SECOND[h] // 2, rows_of(h), :] += first_in[r, 0, h]
            second(q, mb, h).start()

    def finish(q, mb):
        r = q * 2 + mb
        await_both(first_in.at[r], f_recv.at[r, 1])
        for h in range(2):
            done = chip_sum[r, 0, rows_of(h), :] + first_in[r, 1, h] + second_in[r, h]
            (y_ref, dx_ref)[q][mb, rows_of(h), :] = done.astype(BF)

    first_id = (me * NEXP).astype(F32)
    slot_iota = lax.broadcasted_iota(jnp.int32, (cap, tok), 0).astype(F32)

    def block_of(mask, c):
        return number(mask) - core + c

    before = lax.broadcasted_iota(jnp.int32, (tok, tok), 0) < lax.broadcasted_iota(jnp.int32, (tok, tok), 1)

    def make_ranks(mask):
        tables = rt[pl.ds(number(mask) - core, 2)]
        members, weights_of = [], []
        for mb in range(2):
            at = mb * 2 * TOPK
            routes, gates = tables[:, at : at + TOPK, :tok], tables[:, at + TOPK : at + 2 * TOPK, :tok]
            for l in range(NEXP):
                hit = routes == first_id + l
                members.append(jnp.sum(jnp.where(hit, 1.0, 0.0), axis=1))
                weights_of.append(jnp.sum(jnp.where(hit, gates, 0.0), axis=1))
        member = jnp.concatenate(members, axis=0)
        rank[mask // 2] = jnp.where(member > 0, dot(member.astype(BF), jnp.where(before, 1.0, 0.0).astype(BF)), -1.0)
        grow[mask // 2] = jnp.concatenate(weights_of, axis=0)

    def dispatch_x(unit):
        for b, (mb, mask, c) in enumerate(BLOCKS[unit]):
            lines = [pl.ds((mb * NEXP + l) * 2 + c, 1) for l in range(NEXP)]
            hot = jnp.concatenate([jnp.where(rank[mask // 2, line, :] == slot_iota, 1.0, 0.0) for line in lines], axis=0)
            gs = jnp.concatenate([jnp.broadcast_to(grow[mask // 2, line, :], (cap, tok)) for line in lines], axis=0)
            gate = jnp.sum(hot * gs, axis=1, keepdims=True)
            hot = hot.astype(BF)
            disp[unit, b] = hot
            gblk[unit, b] = gate
            xs = dot(hot, xg[mb, block_of(mask, c)]).astype(BF)
            rows = pl.ds(b * cap, cap)
            for l in range(NEXP):
                xr[l, unit, rows, :] = xs[l * cap : (l + 1) * cap]
                gcol[l, unit, rows, :] = gate[l * cap : (l + 1) * cap]

    def forward(u, between=lambda: None, early=lambda: None):
        def spread(l, out):
            z = gcol[l, u] * out.astype(F32)
            hi = z.astype(BF)
            rest = z - hi.astype(F32)
            mid = rest.astype(BF)
            low = (rest - mid.astype(F32)).astype(BF)
            for b in range(QUAD):
                for i, piece in enumerate((hi, mid, low)):
                    zbuf[b, pl.ds((i * NEXP + l) * cap, cap), :] = piece[b * cap : (b + 1) * cap]

        both, out = dot(xr[0, u], wgu[0]).astype(BF), None
        for l in range(NEXP):
            ahead = dot(xr[l + 1, u], wgu[l + 1]).astype(BF) if l + 1 < NEXP else None
            uv[l, u] = both
            both = both.astype(F32)
            gate_pre, up_pre = both[:, :ff], both[:, ff:]
            hidden = (gate_pre * jax.nn.sigmoid(gate_pre) * up_pre).astype(BF)
            hid[l, u] = hidden
            if out is not None:
                spread(l - 1, out)
            out = dot(hidden, wd[l]).astype(BF)
            outs[l, u] = out
            both = ahead
            if l == 2:
                early()
        spread(NEXP - 1, out)

        between()

        for b, (mb, mask, c) in enumerate(BLOCKS[u]):
            part[Y * 2 + mb, mask // 2, c] = tdot(jnp.concatenate([disp[u, b]] * 3, axis=0), zbuf[b])

    def dispatch_dy(unit):
        for b, (mb, mask, c) in enumerate(BLOCKS[unit]):
            blk = block_of(mask, c)
            hot = disp[unit, b]
            dys = dot(hot, dyg[mb, blk])
            qs = (gblk[unit, b] * dys).astype(BF)
            rows = pl.ds(b * cap, cap)
            hot_f = hot.astype(F32)
            routes = rt[blk, mb * 2 * TOPK : mb * 2 * TOPK + TOPK, 0:tok]
            total = jnp.zeros((TOPK, tok), F32)
            for l in range(NEXP):
                cut = slice(l * cap, (l + 1) * cap)
                qr[l, unit, rows, :] = qs[cut]
                dots = jnp.sum(dys[cut] * outs[l, unit, rows, :].astype(F32), axis=1, keepdims=True)
                line = jnp.sum(hot_f[cut] * dots, axis=0, keepdims=True)
                total = total + jnp.where(routes == first_id + l, line, 0.0)
            dg[blk, pl.ds(mb * TOPK, TOPK), pl.ds(0, tok)] = total

    def backward(u, between=lambda: None, early=lambda: None):
        back = ndot(qr[0, u], wd[0])
        for l in range(NEXP):
            ahead = ndot(qr[l + 1, u], wd[l + 1]) if l + 1 < NEXP else None
            both = uv[l, u].astype(F32)
            gate_pre, up_pre = both[:, :ff], both[:, ff:]
            sig = jax.nn.sigmoid(gate_pre)
            d_up = (back * gate_pre * sig).astype(BF)
            d_gate = (back * up_pre * sig * (1.0 + gate_pre * (1.0 - sig))).astype(BF)
            d_both = jnp.concatenate([d_gate, d_up], axis=1)
            uv[l, u] = d_both
            d_in = ndot(d_both, wgu[l]).astype(BF)
            for b in range(QUAD):
                pbuf[b, pl.ds(l * cap, cap), :] = d_in[b * cap : (b + 1) * cap]
            back = ahead
            if l == 1:
                early()

        between()

        for b, (mb, mask, c) in enumerate(BLOCKS[u]):
            part[DX * 2 + mb, mask // 2, c] = tdot(disp[u, b], pbuf[b])

    def weight_grads(l):
        rows = 2 * 2 * QUAD * cap
        gd_ref[l] = tdot(hid[l].reshape(rows, ff), qr[l].reshape(rows, dim))
        xs, d_both = xr[l].reshape(rows, dim), uv[l].reshape(rows, 2 * ff)
        grads = tdot(xs, d_both)
        gg_ref[l] = grads[:, :ff]
        gu_ref[l] = grads[:, ff:]

    def dg_copy(mask):
        return remote(dg_sum.at[mask // 2], dg_in.at[mask // 2], dg_send.at[1], dg_recv.at[1], mask)

    def dg_near_copy(mask):
        return remote(dg.at[number(mask | 1)], dg_near.at[mask // 2], dg_send.at[0], dg_recv.at[0], 1)

    for kind in range(3):
        rt_copy(kind).start()
    for mb in range(2):
        own[mb][0].wait()
        send_own(mb, 6, 0, 3)
    own[0][1].wait()
    send_own(0, 7, 1)
    own[1][1].wait()
    send_own(1, 7)
    rt_relay(0)
    make_ranks(0)
    for load in weights:
        load.wait()
    await_pair(0, 6)
    dispatch_x(OWN)

    def during():
        rt_relay(1, 3, 4)
        rt_relay(2, 5)

    forward(OWN, lambda: None, during)
    partner_start(Y, OWN)

    relay(0, 0, 5, 8)
    send_own(1, 4)
    relay(0, 3, 10)
    rt_relay(4)
    rt_relay(5)
    make_ranks(2)
    make_ranks(4)
    await_pair(0, 7)
    dispatch_dy(OWN)
    relay(1, 3, 5, 10)
    relay(1, 0, 8)
    send_own(1, 1)
    send_own(0, 4)
    await_pair(0, 8)
    dispatch_x(XY0)
    forward(XY0, lambda: relay(0, 1, 2, 9), lambda: rt_relay(3, 6))
    partner_start(Y, XY0)

    rt_relay(6)
    make_ranks(6)
    relay(0, 5, 12)
    await_pair(1, 8)
    dispatch_x(XY1)

    def during():
        relay(1, 5, 12)
        relay(1, 4, 2, 11)

    forward(XY1, lambda: leave(Y, XY0), during)
    partner_start(Y, XY1)

    await_pair(0, 12)
    dispatch_x(DIAG)
    relay(0, 4, 11)
    relay(1, 1, 9)

    def during():
        leave(Y, XY1)
        relay(0, 2, 13)

    forward(DIAG, lambda: None, during)
    partner_start(Y, DIAG)

    relay(1, 2, 13)
    await_pair(0, 9)
    dispatch_dy(XY0)
    leave(Y, DIAG)
    await_pair(0, 13)
    dispatch_dy(DIAG)
    backward(DIAG)
    partner_start(DX, DIAG)

    await_pair(1, 9)
    dispatch_dy(XY1)
    for mask in (0, 2, 4, 6):
        dg_near_copy(mask).start()
    leave(DX, DIAG)
    remote(dg_near, dg_near, dg_send.at[0], dg_recv.at[0], 1).wait_recv()
    for mask in (0, 2, 4, 6):
        dg_sum[mask // 2] = dg[number(mask)] + dg_near[mask // 2]
    for mask in (6, 2, 4):
        dg_copy(mask).start()
    backward(XY0, lambda: leave(Y, OWN))
    partner_start(DX, XY0)

    def during():
        second_send(Y, 0)
        second_send(Y, 1)

    backward(XY1, lambda: leave(DX, XY0), during)
    partner_start(DX, XY1)

    backward(OWN, lambda: leave(DX, XY1))
    partner_start(DX, OWN)
    weight_grads(0)
    second_send(DX, 0)
    second_send(DX, 1)
    leave(DX, OWN)
    weight_grads(1)
    weight_grads(2)
    weight_grads(3)
    finish(Y, 0)
    finish(Y, 1)
    remote(dg_near, dg_near, dg_send.at[0], dg_recv.at[0], 1).wait_send()
    three = dg_in.at[pl.ds(1, 3)]
    remote(three, three, dg_send.at[1], dg_recv.at[1], 2).wait()
    grads = dg_sum[0] + dg_in[1] + dg_in[2] + dg_in[3]
    for mb in range(2):
        gates_ref[mb] = grads[mb * TOPK : (mb + 1) * TOPK, :tok]
    def sent(ref, sem):
        remote(ref, ref, sem, f_recv.at[0, 0], 1).wait_send()

    sent(rt.at[pl.ds(0, 7)], rt_send.at[0])
    for which in range(2):
        sent(tokens[which].at[:, pl.ds(0, 7)], g_send.at[which])
    sent(near_in, d_send.at[0])
    sent(first_in, f_send.at[0])
    finish(DX, 0)
    finish(DX, 1)
    sent(second_in, s_send.at[0])


def layer(x, grad_y, route_rows, gate_rows, w_gate, w_up, w_down):
    _, tok, dim = x.shape
    ff = w_gate.shape[2]
    cap = tok // 2
    hbm, vmem = pl.BlockSpec(memory_space=pltpu.HBM), pl.BlockSpec(memory_space=pltpu.VMEM)
    dma = pltpu.SemaphoreType.DMA
    unit = QUAD * cap
    shape = jax.ShapeDtypeStruct
    return pl.pallas_call(
        layer_kernel,
        out_shape=(
            shape((2, tok, dim), BF), shape((2, tok, dim), BF), shape((2, TOPK, tok), F32),
            shape(w_gate.shape, F32), shape(w_up.shape, F32), shape(w_down.shape, F32),
        ),
        in_specs=[hbm] * 7,
        out_specs=(vmem,) * 6,
        scratch_shapes=[
            pltpu.VMEM((2, NBLK, tok, dim), BF),
            pltpu.VMEM((2, NBLK, tok, dim), BF),
            pltpu.VMEM((NBLK, 4 * TOPK, LANES), F32),
            pltpu.VMEM((2, TOPK, tok), jnp.int32),
            pltpu.VMEM((2, TOPK, tok), F32),
            pltpu.VMEM((NEXP, dim, 2 * ff), BF),
            pltpu.VMEM((NEXP, ff, dim), BF),
            pltpu.VMEM((4, 4 * NEXP, tok), F32),
            pltpu.VMEM((4, 4 * NEXP, tok), F32),
            pltpu.VMEM((4, QUAD, NEXP * cap, tok), BF),
            pltpu.VMEM((4, QUAD, NEXP * cap, 1), F32),
            pltpu.VMEM((NEXP, 4, unit, 1), F32),
            pltpu.VMEM((NEXP, 4, unit, dim), BF),
            pltpu.VMEM((NEXP, 4, unit, dim), BF),
            pltpu.VMEM((NEXP, 4, unit, 2 * ff), BF),
            pltpu.VMEM((NEXP, 4, unit, ff), BF),
            pltpu.VMEM((NEXP, 4, unit, dim), BF),
            pltpu.VMEM((QUAD, 3 * NEXP * cap, dim), BF),
            pltpu.VMEM((QUAD, NEXP * cap, dim), BF),
            pltpu.VMEM((NBLK, 2 * TOPK, LANES), F32),
            pltpu.VMEM((4, 4, 2, tok, dim), F32),
            pltpu.VMEM((4, 4, tok, dim), F32),
            pltpu.VMEM((4, 4, tok, dim), F32),
            pltpu.VMEM((4, 2, 2, tok // 2, dim), F32),
            pltpu.VMEM((4, 2, tok // 2, dim), F32),
            pltpu.VMEM((4, 2 * TOPK, LANES), F32),
            pltpu.VMEM((4, 2 * TOPK, LANES), F32),
            pltpu.VMEM((4, 2 * TOPK, LANES), F32),
            dma((2,)), dma((2, 2)), dma((3,)), dma((2,)), dma((20,)), dma((1,)), dma((7,)),
            dma((1,)), dma((2, 4)), dma((1,)), dma((4, 2)), dma((1,)), dma((2,)), dma((2,)),
        ],
        compiler_params=pltpu.CompilerParams(collective_id=0, has_side_effects=True, vmem_limit_bytes=46 << 20),
        name="moe_layer",
    )(x, grad_y, route_rows, gate_rows, w_gate, w_up, w_down)


def flush_kernel(*refs):
    count = (len(refs) - 1) // 2
    sem = refs[-1]
    copies = [pltpu.make_async_copy(refs[i], refs[count + i], sem.at[i]) for i in range(count)]
    for copy in reversed(copies):
        copy.start()
    for copy in copies:
        copy.wait()


def flush(arrays):
    hbm, vmem = pl.BlockSpec(memory_space=pltpu.HBM), pl.BlockSpec(memory_space=pltpu.VMEM)
    return pl.pallas_call(
        flush_kernel,
        out_shape=tuple(jax.ShapeDtypeStruct(arr.shape, arr.dtype) for arr in arrays),
        in_specs=[vmem] * len(arrays),
        out_specs=(hbm,) * len(arrays),
        scratch_shapes=[pltpu.SemaphoreType.DMA((len(arrays),))],
        compiler_params=pltpu.CompilerParams(vmem_limit_bytes=12 << 20),
        name="write_out",
    )(*arrays)


def solution(mesh):
    tok_spec = P(None, ALL_AXES, None)
    w_spec = P(ALL_AXES, None, None)

    def moe_layer(x, route_idx, gates, w_gate, w_up, w_down, grad_y):
        stay = lambda arr: pltpu.with_memory_space_constraint(arr, pltpu.HBM)
        flat = lambda arr: jnp.transpose(arr, (0, 2, 1))
        args = [stay(arr) for arr in (x, grad_y, flat(route_idx), flat(gates), w_gate, w_up, w_down)]
        y, dx, g_gates, g_gate, g_up, g_down = flush(layer(*args))
        return y, dx, flat(g_gates), g_gate, g_up, g_down

    return jax.shard_map(moe_layer, mesh=mesh, in_specs=(tok_spec, tok_spec, tok_spec, w_spec, w_spec, w_spec, tok_spec), out_specs=(tok_spec, tok_spec, tok_spec, w_spec, w_spec, w_spec), check_vma=False)
```

```python
import functools

import jax
import jax.numpy as jnp
from jax import lax
from jax.experimental import pallas as pl
from jax.experimental.pallas import tpu as pltpu
from jax.sharding import PartitionSpec as P

ALL_AXES = ("rep", "row", "col", "core")
MESH = pl.DeviceIdType.MESH
BF = jnp.bfloat16
F32 = jnp.float32
NBLK = 8
QUAD = 4
NEXP = 4
TOPK = 4
LANES = 128
OWN, XY0, XY1, DIAG = 0, 1, 2, 3
Y, DX = 0, 1


def coords():
    return (lax.axis_index("rep"), lax.axis_index("row"), lax.axis_index("col"), lax.axis_index("core"))


def peer(mask):
    rep, row, col, core = coords()
    flip = lambda pos, bit: 1 - pos if mask & bit else pos
    return (rep, flip(row, 4), flip(col, 2), flip(core, 1))


def number(mask=0):
    _, row, col, core = peer(mask)
    return row * 4 + col * 2 + core


def announce():
    barrier = pltpu.get_barrier_semaphore()
    for mask in range(1, NBLK):
        pl.semaphore_signal(barrier, inc=1, device_id=peer(mask), device_id_type=MESH)


def all_entered():
    pl.semaphore_wait(pltpu.get_barrier_semaphore(), NBLK - 1)


def remote(src, dst, send_sem, recv_sem, mask):
    return pltpu.make_async_remote_copy(src_ref=src, dst_ref=dst, send_sem=send_sem, recv_sem=recv_sem, device_id=peer(mask), device_id_type=MESH)


def tdot(lhs, rhs):
    return lax.dot_general(lhs, rhs, (((0,), (0,)), ((), ())), preferred_element_type=F32)


def ndot(lhs, rhs):
    return lax.dot_general(lhs, rhs, (((1,), (1,)), ((), ())), preferred_element_type=F32)


def dot(lhs, rhs):
    return jnp.dot(lhs, rhs, preferred_element_type=F32)


CHIPS = {
    OWN: ((0, 0), (1, 0)),
    XY0: ((0, 2), (0, 4)),
    XY1: ((1, 4), (1, 2)),
    DIAG: ((0, 6), (1, 6)),
}
BLOCKS = {unit: tuple((mb, mask, c) for mb, mask in chips for c in range(2)) for unit, chips in CHIPS.items()}


PAIRS = (
    ((0, 6), (1, 6)), ((0, 7), (1, 7)), ((0, 8), (0, 10)), ((1, 8), (1, 10)),
    ((0, 9), (0, 11)), ((1, 9), (1, 11)), ((0, 12), (1, 12)), ((0, 13), (1, 13)),
)
PAIR = {item: 12 + i for i, pair in enumerate(PAIRS) for item in pair}


def layer_kernel(x_hbm, dy_hbm, route_hbm, gate_hbm, wg_hbm, wu_hbm, wd_hbm,
                 y_ref, dx_ref, gates_ref, gg_ref, gu_ref, gd_ref,
                 xg, dyg, rt, route_tab, gate_tab, wgu, wd, rank, grow, disp, gblk, gcol, xr, qr, uv, hid, outs, zbuf, pbuf, dg,
                 part, near_in, chip_sum, first_in, second_in, dg_in, dg_near, dg_sum,
                 tab_sem, own_sem, w_sem, g_send, g_recv, rt_send, rt_recv, d_send, d_recv, f_send, f_recv, s_send, dg_send, dg_recv):
    tok, dim = xg.shape[2], xg.shape[3]
    ff = wd.shape[1]
    cap = tok // 2
    _, row, col, core = coords()
    me, at_x, at_y, at_d = number(0), number(2), number(4), number(6)
    tokens = (xg, dyg)
    PART = 6

    announce()
    tables = [pltpu.make_async_copy(src, dst, tab_sem.at[i]) for i, (src, dst) in enumerate(((route_hbm, route_tab), (gate_hbm, gate_tab)))]
    own = [[pltpu.make_async_copy(src.at[mb], dst.at[mb, me], own_sem.at[mb, i]) for i, (src, dst) in enumerate(((x_hbm, xg), (dy_hbm, dyg)))] for mb in range(2)]
    weights = [
        pltpu.make_async_copy(wg_hbm, wgu.at[:, :, pl.ds(0, ff)], w_sem.at[0]),
        pltpu.make_async_copy(wu_hbm, wgu.at[:, :, pl.ds(ff, ff)], w_sem.at[1]),
        pltpu.make_async_copy(wd_hbm, wd, w_sem.at[2]),
    ]
    for load in tables + own[0] + own[1] + weights:
        load.start()
    for load in tables:
        load.wait()
    rt[me] = jnp.zeros(rt.shape[1:], F32)
    for mb in range(2):
        rt[me, pl.ds(mb * 2 * TOPK, TOPK), pl.ds(0, tok)] = route_tab[mb].astype(F32)
        rt[me, pl.ds(mb * 2 * TOPK + TOPK, TOPK), pl.ds(0, tok)] = gate_tab[mb]
    all_entered()

    def tok_copy(mb, kind):
        if kind < PART:
            slot, mask = (me, 2) if kind in (0, 1) else (me, 4) if kind in (3, 4) else ((at_x, 4), (at_y, 2))[mb]
            which = int(kind in (1, 2, 4))
        else:
            which, slot, mask = (kind - PART) % 2, (me, at_x, at_y, at_d)[(kind - PART) // 2], 1
        ref = tokens[which].at[mb, slot]
        arrival = mb * PART + kind if kind < PART else PAIR[mb, kind]
        return remote(ref, ref, g_send.at[which], g_recv.at[arrival], mask)

    def await_pair(mb, kind):
        which = (kind - PART) % 2
        two = tokens[which].at[0, pl.ds(0, 2)]
        remote(two, two, g_send.at[which], g_recv.at[PAIR[mb, kind]], 1).wait_recv()

    def send_own(mb, *kinds):
        for kind in kinds:
            tok_copy(mb, kind).start()

    def relay(mb, kind, *then):
        tok_copy(mb, kind).wait_recv()
        for nxt in then:
            tok_copy(mb, nxt).start()

    def rt_copy(kind):
        slot, mask = ((me, 1), (me, 2), (me, 4), (at_x, 4), (at_x, 1), (at_y, 1), (at_d, 1))[kind]
        return remote(rt.at[slot], rt.at[slot], rt_send.at[0], rt_recv.at[4 if kind == 5 else kind], mask)

    def rt_relay(kind, *then):
        rt_copy(kind).wait_recv()
        for nxt in then:
            rt_copy(nxt).start()

    FIRST, SECOND = (2, 4), (4, 2)
    half = tok // 2

    def to_partner(q, unit, mb, mask):
        r, i = q * 2 + mb, mask // 2
        return remote(part.at[r, i, 1 - core], near_in.at[r, i], d_send.at[0], d_recv.at[q, unit], 1)

    def partner_start(q, unit):
        for mb, mask in CHIPS[unit]:
            to_partner(q, unit, mb, mask).start()

    def rows_of(h):
        return pl.ds(h * half, half)

    def first(q, mb, h, which):
        r = q * 2 + mb
        src = chip_sum.at[r, (3, FIRST[h] // 2)[which], rows_of(h)]
        return remote(src, first_in.at[r, which, h], f_send.at[0], f_recv.at[r, which], FIRST[h])

    def second(q, mb, h):
        r = q * 2 + mb
        return remote(chip_sum.at[r, SECOND[h] // 2, rows_of(h)], second_in.at[r, h], s_send.at[0], f_recv.at[r, 1], SECOND[h])

    def await_both(ref, sem):
        remote(ref, ref, s_send.at[0], sem, 2).wait_recv()

    def leave(q, unit):
        two = near_in.at[0, pl.ds(0, 2)]
        remote(two, two, d_send.at[0], d_recv.at[q, unit], 1).wait_recv()
        for mb, mask in CHIPS[unit]:
            r, i = q * 2 + mb, mask // 2
            chip_sum[r, i] = part[r, i, core] + near_in[r, i]
            for h in range(2):
                if mask in (6, FIRST[h]):
                    first(q, mb, h, 0 if mask == 6 else 1).start()

    def second_send(q, mb):
        r = q * 2 + mb
        await_both(first_in.at[r, 0], f_recv.at[r, 0])
        for h in range(2):
            chip_sum[r, SECOND[h] // 2, rows_of(h), :] += first_in[r, 0, h]
            second(q, mb, h).start()

    def finish(q, mb):
        r = q * 2 + mb
        await_both(first_in.at[r], f_recv.at[r, 1])
        for h in range(2):
            done = chip_sum[r, 0, rows_of(h), :] + first_in[r, 1, h] + second_in[r, h]
            (y_ref, dx_ref)[q][mb, rows_of(h), :] = done.astype(BF)

    first_id = (me * NEXP).astype(F32)
    slot_iota = lax.broadcasted_iota(jnp.int32, (cap, tok), 0).astype(F32)

    def block_of(mask, c):
        return number(mask) - core + c

    before = lax.broadcasted_iota(jnp.int32, (tok, tok), 0) < lax.broadcasted_iota(jnp.int32, (tok, tok), 1)

    def make_ranks(mask):
        tables = rt[pl.ds(number(mask) - core, 2)]
        members, weights_of = [], []
        for mb in range(2):
            at = mb * 2 * TOPK
            routes, gates = tables[:, at : at + TOPK, :tok], tables[:, at + TOPK : at + 2 * TOPK, :tok]
            for l in range(NEXP):
                hit = routes == first_id + l
                members.append(jnp.sum(jnp.where(hit, 1.0, 0.0), axis=1))
                weights_of.append(jnp.sum(jnp.where(hit, gates, 0.0), axis=1))
        member = jnp.concatenate(members, axis=0)
        rank[mask // 2] = jnp.where(member > 0, dot(member.astype(BF), jnp.where(before, 1.0, 0.0).astype(BF)), -1.0)
        grow[mask // 2] = jnp.concatenate(weights_of, axis=0)

    def dispatch_x(unit):
        for b, (mb, mask, c) in enumerate(BLOCKS[unit]):
            lines = [pl.ds((mb * NEXP + l) * 2 + c, 1) for l in range(NEXP)]
            hot = jnp.concatenate([jnp.where(rank[mask // 2, line, :] == slot_iota, 1.0, 0.0) for line in lines], axis=0)
            gs = jnp.concatenate([jnp.broadcast_to(grow[mask // 2, line, :], (cap, tok)) for line in lines], axis=0)
            gate = jnp.sum(hot * gs, axis=1, keepdims=True)
            hot = hot.astype(BF)
            disp[unit, b] = hot
            gblk[unit, b] = gate
            xs = dot(hot, xg[mb, block_of(mask, c)]).astype(BF)
            rows = pl.ds(b * cap, cap)
            for l in range(NEXP):
                xr[l, unit, rows, :] = xs[l * cap : (l + 1) * cap]
                gcol[l, unit, rows, :] = gate[l * cap : (l + 1) * cap]

    def forward(u, between=lambda: None, early=lambda: None):
        def spread(l, out):
            z = gcol[l, u] * out.astype(F32)
            hi = z.astype(BF)
            rest = z - hi.astype(F32)
            mid = rest.astype(BF)
            low = (rest - mid.astype(F32)).astype(BF)
            for b in range(QUAD):
                for i, piece in enumerate((hi, mid, low)):
                    zbuf[b, pl.ds((i * NEXP + l) * cap, cap), :] = piece[b * cap : (b + 1) * cap]

        both, out = dot(xr[0, u], wgu[0]).astype(BF), None
        for l in range(NEXP):
            ahead = dot(xr[l + 1, u], wgu[l + 1]).astype(BF) if l + 1 < NEXP else None
            uv[l, u] = both
            both = both.astype(F32)
            gate_pre, up_pre = both[:, :ff], both[:, ff:]
            hidden = (gate_pre * jax.nn.sigmoid(gate_pre) * up_pre).astype(BF)
            hid[l, u] = hidden
            if out is not None:
                spread(l - 1, out)
            out = dot(hidden, wd[l]).astype(BF)
            outs[l, u] = out
            both = ahead
            if l == 2:
                early()
        spread(NEXP - 1, out)

        between()

        for b, (mb, mask, c) in enumerate(BLOCKS[u]):
            part[Y * 2 + mb, mask // 2, c] = tdot(jnp.concatenate([disp[u, b]] * 3, axis=0), zbuf[b])

    def dispatch_dy(unit):
        for b, (mb, mask, c) in enumerate(BLOCKS[unit]):
            blk = block_of(mask, c)
            hot = disp[unit, b]
            dys = dot(hot, dyg[mb, blk])
            qs = (gblk[unit, b] * dys).astype(BF)
            rows = pl.ds(b * cap, cap)
            hot_f = hot.astype(F32)
            routes = rt[blk, mb * 2 * TOPK : mb * 2 * TOPK + TOPK, 0:tok]
            total = jnp.zeros((TOPK, tok), F32)
            for l in range(NEXP):
                cut = slice(l * cap, (l + 1) * cap)
                qr[l, unit, rows, :] = qs[cut]
                dots = jnp.sum(dys[cut] * outs[l, unit, rows, :].astype(F32), axis=1, keepdims=True)
                line = jnp.sum(hot_f[cut] * dots, axis=0, keepdims=True)
                total = total + jnp.where(routes == first_id + l, line, 0.0)
            dg[blk, pl.ds(mb * TOPK, TOPK), pl.ds(0, tok)] = total

    def backward(u, between=lambda: None, early=lambda: None):
        back = ndot(qr[0, u], wd[0])
        for l in range(NEXP):
            ahead = ndot(qr[l + 1, u], wd[l + 1]) if l + 1 < NEXP else None
            both = uv[l, u].astype(F32)
            gate_pre, up_pre = both[:, :ff], both[:, ff:]
            sig = jax.nn.sigmoid(gate_pre)
            d_up = (back * gate_pre * sig).astype(BF)
            d_gate = (back * up_pre * sig * (1.0 + gate_pre * (1.0 - sig))).astype(BF)
            d_both = jnp.concatenate([d_gate, d_up], axis=1)
            uv[l, u] = d_both
            d_in = ndot(d_both, wgu[l]).astype(BF)
            for b in range(QUAD):
                pbuf[b, pl.ds(l * cap, cap), :] = d_in[b * cap : (b + 1) * cap]
            back = ahead
            if l == 1:
                early()

        between()

        for b, (mb, mask, c) in enumerate(BLOCKS[u]):
            part[DX * 2 + mb, mask // 2, c] = tdot(disp[u, b], pbuf[b])

    def weight_grads(l):
        rows = 2 * 2 * QUAD * cap
        gd_ref[l] = tdot(hid[l].reshape(rows, ff), qr[l].reshape(rows, dim))
        xs, d_both = xr[l].reshape(rows, dim), uv[l].reshape(rows, 2 * ff)
        grads = tdot(xs, d_both)
        gg_ref[l] = grads[:, :ff]
        gu_ref[l] = grads[:, ff:]

    def dg_copy(mask):
        return remote(dg_sum.at[mask // 2], dg_in.at[mask // 2], dg_send.at[1], dg_recv.at[1], mask)

    def dg_near_copy(mask):
        return remote(dg.at[number(mask | 1)], dg_near.at[mask // 2], dg_send.at[0], dg_recv.at[0], 1)

    for kind in range(3):
        rt_copy(kind).start()
    for mb in range(2):
        own[mb][0].wait()
        send_own(mb, 6, 0, 3)
    own[0][1].wait()
    send_own(0, 7, 1)
    own[1][1].wait()
    send_own(1, 7)
    rt_relay(0)
    make_ranks(0)
    for load in weights:
        load.wait()
    await_pair(0, 6)
    dispatch_x(OWN)

    def during():
        rt_relay(1, 3, 4)
        rt_relay(2, 5)

    forward(OWN, lambda: None, during)
    partner_start(Y, OWN)

    relay(0, 0, 5, 8)
    send_own(1, 4)
    relay(0, 3, 10)
    two = rt.at[pl.ds(0, 2)]
    remote(two, two, rt_send.at[0], rt_recv.at[4], 1).wait_recv()
    make_ranks(2)
    make_ranks(4)
    await_pair(0, 7)
    dispatch_dy(OWN)
    relay(1, 3, 5, 10)
    relay(1, 0, 8)
    send_own(1, 1)
    send_own(0, 4)
    await_pair(0, 8)
    dispatch_x(XY0)
    forward(XY0, lambda: relay(0, 1, 2, 9), lambda: rt_relay(3, 6))
    partner_start(Y, XY0)

    rt_relay(6)
    make_ranks(6)
    relay(0, 5, 12)
    await_pair(1, 8)
    dispatch_x(XY1)

    def during():
        relay(1, 5, 12)
        relay(1, 4, 2, 11)

    forward(XY1, lambda: leave(Y, XY0), during)
    partner_start(Y, XY1)

    await_pair(0, 12)
    dispatch_x(DIAG)
    relay(0, 4, 11)
    relay(1, 1, 9)

    def during():
        leave(Y, XY1)
        relay(0, 2, 13)

    forward(DIAG, lambda: None, during)
    partner_start(Y, DIAG)

    relay(1, 2, 13)
    await_pair(0, 9)
    dispatch_dy(XY0)
    leave(Y, DIAG)
    await_pair(0, 13)
    dispatch_dy(DIAG)
    backward(DIAG)
    partner_start(DX, DIAG)

    await_pair(1, 9)
    dispatch_dy(XY1)
    for mask in (0, 2, 4, 6):
        dg_near_copy(mask).start()
    leave(DX, DIAG)
    remote(dg_near, dg_near, dg_send.at[0], dg_recv.at[0], 1).wait_recv()
    for mask in (0, 2, 4, 6):
        dg_sum[mask // 2] = dg[number(mask)] + dg_near[mask // 2]
    for mask in (6, 2, 4):
        dg_copy(mask).start()
    backward(XY0, lambda: leave(Y, OWN))
    partner_start(DX, XY0)

    def during():
        second_send(Y, 0)
        second_send(Y, 1)

    backward(XY1, lambda: leave(DX, XY0), during)
    partner_start(DX, XY1)

    backward(OWN, lambda: leave(DX, XY1))
    partner_start(DX, OWN)
    weight_grads(0)
    second_send(DX, 0)
    second_send(DX, 1)
    leave(DX, OWN)
    weight_grads(1)
    weight_grads(2)
    weight_grads(3)
    finish(Y, 0)
    finish(Y, 1)
    remote(dg_near, dg_near, dg_send.at[0], dg_recv.at[0], 1).wait_send()
    three = dg_in.at[pl.ds(1, 3)]
    remote(three, three, dg_send.at[1], dg_recv.at[1], 2).wait()
    grads = dg_sum[0] + dg_in[1] + dg_in[2] + dg_in[3]
    for mb in range(2):
        gates_ref[mb] = grads[mb * TOPK : (mb + 1) * TOPK, :tok]
    def sent(ref, sem):
        remote(ref, ref, sem, f_recv.at[0, 0], 1).wait_send()

    sent(rt.at[pl.ds(0, 7)], rt_send.at[0])
    for which in range(2):
        sent(tokens[which].at[:, pl.ds(0, 7)], g_send.at[which])
    sent(near_in, d_send.at[0])
    sent(first_in, f_send.at[0])
    finish(DX, 0)
    finish(DX, 1)
    sent(second_in, s_send.at[0])


def layer(x, grad_y, route_rows, gate_rows, w_gate, w_up, w_down):
    _, tok, dim = x.shape
    ff = w_gate.shape[2]
    cap = tok // 2
    hbm, vmem = pl.BlockSpec(memory_space=pltpu.HBM), pl.BlockSpec(memory_space=pltpu.VMEM)
    dma = pltpu.SemaphoreType.DMA
    unit = QUAD * cap
    shape = jax.ShapeDtypeStruct
    return pl.pallas_call(
        layer_kernel,
        out_shape=(
            shape((2, tok, dim), BF), shape((2, tok, dim), BF), shape((2, TOPK, tok), F32),
            shape(w_gate.shape, F32), shape(w_up.shape, F32), shape(w_down.shape, F32),
        ),
        in_specs=[hbm] * 7,
        out_specs=(vmem,) * 6,
        scratch_shapes=[
            pltpu.VMEM((2, NBLK, tok, dim), BF),
            pltpu.VMEM((2, NBLK, tok, dim), BF),
            pltpu.VMEM((NBLK, 4 * TOPK, LANES), F32),
            pltpu.VMEM((2, TOPK, tok), jnp.int32),
            pltpu.VMEM((2, TOPK, tok), F32),
            pltpu.VMEM((NEXP, dim, 2 * ff), BF),
            pltpu.VMEM((NEXP, ff, dim), BF),
            pltpu.VMEM((4, 4 * NEXP, tok), F32),
            pltpu.VMEM((4, 4 * NEXP, tok), F32),
            pltpu.VMEM((4, QUAD, NEXP * cap, tok), BF),
            pltpu.VMEM((4, QUAD, NEXP * cap, 1), F32),
            pltpu.VMEM((NEXP, 4, unit, 1), F32),
            pltpu.VMEM((NEXP, 4, unit, dim), BF),
            pltpu.VMEM((NEXP, 4, unit, dim), BF),
            pltpu.VMEM((NEXP, 4, unit, 2 * ff), BF),
            pltpu.VMEM((NEXP, 4, unit, ff), BF),
            pltpu.VMEM((NEXP, 4, unit, dim), BF),
            pltpu.VMEM((QUAD, 3 * NEXP * cap, dim), BF),
            pltpu.VMEM((QUAD, NEXP * cap, dim), BF),
            pltpu.VMEM((NBLK, 2 * TOPK, LANES), F32),
            pltpu.VMEM((4, 4, 2, tok, dim), F32),
            pltpu.VMEM((4, 4, tok, dim), F32),
            pltpu.VMEM((4, 4, tok, dim), F32),
            pltpu.VMEM((4, 2, 2, tok // 2, dim), F32),
            pltpu.VMEM((4, 2, tok // 2, dim), F32),
            pltpu.VMEM((4, 2 * TOPK, LANES), F32),
            pltpu.VMEM((4, 2 * TOPK, LANES), F32),
            pltpu.VMEM((4, 2 * TOPK, LANES), F32),
            dma((2,)), dma((2, 2)), dma((3,)), dma((2,)), dma((20,)), dma((1,)), dma((7,)),
            dma((1,)), dma((2, 4)), dma((1,)), dma((4, 2)), dma((1,)), dma((2,)), dma((2,)),
        ],
        compiler_params=pltpu.CompilerParams(collective_id=0, has_side_effects=True, vmem_limit_bytes=46 << 20),
        name="moe_layer",
    )(x, grad_y, route_rows, gate_rows, w_gate, w_up, w_down)


def flush_kernel(*refs):
    count = (len(refs) - 1) // 2
    sem = refs[-1]
    copies = [pltpu.make_async_copy(refs[i], refs[count + i], sem.at[i]) for i in range(count)]
    for copy in reversed(copies):
        copy.start()
    for copy in copies:
        copy.wait()


def flush(arrays):
    hbm, vmem = pl.BlockSpec(memory_space=pltpu.HBM), pl.BlockSpec(memory_space=pltpu.VMEM)
    return pl.pallas_call(
        flush_kernel,
        out_shape=tuple(jax.ShapeDtypeStruct(arr.shape, arr.dtype) for arr in arrays),
        in_specs=[vmem] * len(arrays),
        out_specs=(hbm,) * len(arrays),
        scratch_shapes=[pltpu.SemaphoreType.DMA((len(arrays),))],
        compiler_params=pltpu.CompilerParams(vmem_limit_bytes=12 << 20),
        name="write_out",
    )(*arrays)


def solution(mesh):
    tok_spec = P(None, ALL_AXES, None)
    w_spec = P(ALL_AXES, None, None)

    def moe_layer(x, route_idx, gates, w_gate, w_up, w_down, grad_y):
        stay = lambda arr: pltpu.with_memory_space_constraint(arr, pltpu.HBM)
        flat = lambda arr: jnp.transpose(arr, (0, 2, 1))
        args = [stay(arr) for arr in (x, grad_y, flat(route_idx), flat(gates), w_gate, w_up, w_down)]
        y, dx, g_gates, g_gate, g_up, g_down = flush(layer(*args))
        return y, dx, flat(g_gates), g_gate, g_up, g_down

    return jax.shard_map(moe_layer, mesh=mesh, in_specs=(tok_spec, tok_spec, tok_spec, w_spec, w_spec, w_spec, tok_spec), out_specs=(tok_spec, tok_spec, tok_spec, w_spec, w_spec, w_spec), check_vma=False)
```
